32 devices in a mesh: rep: 2 (over x), kv2: 4 (over z), kv: 4 (over y, core).
Axes of the slice: x: 2, y: 2, z: 4, core: 2. Of those that a mesh axis runs over, the one named last changes fastest.
Arguments:
- x_embed: bfloat16 [2, 384, 3072], P(None, ('rep', 'kv2', 'kv')), parts along dimension 1
- w_query: bfloat16 [2, 3072, 3072], replicated
- w_key: bfloat16 [2, 3072, 1024], replicated
- w_value: bfloat16 [2, 3072, 1024], replicated
- w_out: bfloat16 [2, 3072, 3072], replicated
- w_up: bfloat16 [2, 3072, 8192], replicated
- w_down: bfloat16 [2, 8192, 3072], replicated
- k_pool: bfloat16 [1920, 2, 32, 8, 128], P(('rep', 'kv2', 'kv')), parts along dimension 0
- v_pool: bfloat16 [1920, 2, 32, 8, 128], P(('rep', 'kv2', 'kv')), parts along dimension 0
- old_table: int32 [384, 2], P(('rep', 'kv2', 'kv')), parts along dimension 0
- seq_len: int32 [384], P(('rep', 'kv2', 'kv')), parts along dimension 0
- src_slot: int32 [384], P(('rep', 'kv2', 'kv')), parts along dimension 0
- dst_slot: int32 [384], P(('rep', 'kv2', 'kv')), parts along dimension 0
Outputs:
- output 1: bfloat16 [2, 384, 3072], P(None, ('rep', 'kv2', 'kv')), parts along dimension 1
- output 2: bfloat16 [1920, 2, 32, 8, 128], P(('rep', 'kv2', 'kv')), parts along dimension 0
- output 3: bfloat16 [1920, 2, 32, 8, 128], P(('rep', 'kv2', 'kv')), parts along dimension 0
There are 2 independent parts. The reference program is written for one: setup_inputs(seed, part) draws one part's arguments, and reference() takes and returns one part's arrays. A program takes and returns all parts, laid end to end along the dimension named above; an argument that names none is the same for every part.
All inputs are finite; a program needn't handle non-finite values.
Results may differ from the reference program's by a relative error of at most 0.0137214.
Values are sent between devices in bfloat16 or wider.
A program may use at most 1.25 GiB of HBM per device.

```python
import jax
import jax.numpy as jnp
from jax import lax

MESH_ROWS = 4
MESH_COLS = 4
SEQ_DEV = 12
PAGES = 2
MIG_DEV = 12
D = 3072
HEADS = 24
KV_HEADS = 8
HEAD = 128
FF = 8192
PAGE = 32
LAYERS = 2
DEVICES_PART = MESH_ROWS * MESH_COLS
ROW_SEQS = MESH_COLS * SEQ_DEV
BATCH = DEVICES_PART * SEQ_DEV
SLOTS = 2 * SEQ_DEV * PAGES + MIG_DEV
MOVES = DEVICES_PART * MIG_DEV
ALL_SLOTS = DEVICES_PART * SLOTS


def draw_layout(key):
    keys_list = jax.random.split(key, 7)
    n_pages = jax.random.randint(keys_list[0], (BATCH,), 2, PAGES + 1).at[0].set(PAGES)
    fill_len = jax.random.randint(keys_list[1], (BATCH,), 0, PAGE - 1).at[0].set(PAGE - 2)
    seq_len = (n_pages - 1) * PAGE + fill_len
    dev_ids = jnp.arange(DEVICES_PART, dtype=jnp.int32)
    local_ids = jnp.arange(SLOTS, dtype=jnp.int32)
    slot_caps = jnp.where(dev_ids % MESH_COLS % 2 == 0, SLOTS - MIG_DEV, (SLOTS - MIG_DEV) // 4)
    move_ids = jnp.arange(MOVES, dtype=jnp.int32)
    src_dev = move_ids // MIG_DEV
    target = 2 * (jax.random.permutation(keys_list[2], MOVES) // (2 * MIG_DEV))
    target = jnp.where(target == src_dev, (target + 2) % DEVICES_PART, target)
    order_t = jnp.argsort(target * MOVES + move_ids)
    group_start = jnp.searchsorted(target[order_t], target)
    rank_in = jnp.argsort(order_t) - group_start
    outside = (local_ids[None, :] >= slot_caps[:, None]).astype(jnp.int32)
    prio_dst = jax.random.permutation(keys_list[3], ALL_SLOTS).reshape(DEVICES_PART, SLOTS) + outside * ALL_SLOTS
    dst_slot = target * SLOTS + jnp.argsort(prio_dst, axis=1)[target, rank_in]
    prio_src = jax.random.permutation(keys_list[4], ALL_SLOTS).reshape(DEVICES_PART, SLOTS) + (1 - outside) * ALL_SLOTS
    src_slot = (dev_ids[:, None] * SLOTS + jnp.argsort(prio_src, axis=1)[:, :MIG_DEV]).reshape(MOVES)
    marked = jnp.zeros((ALL_SLOTS,), jnp.int32).at[dst_slot].set(1).reshape(MESH_ROWS, MESH_COLS * SLOTS)
    inside = (1 - outside).reshape(MESH_ROWS, MESH_COLS * SLOTS)
    prio_new = jax.random.permutation(keys_list[5], ALL_SLOTS).reshape(MESH_ROWS, MESH_COLS * SLOTS) + jnp.where(marked == 1, 0, jnp.where(inside == 1, ALL_SLOTS, 2 * ALL_SLOTS))
    slot_order = jnp.argsort(prio_new, axis=1)
    pages_row = n_pages.reshape(MESH_ROWS, ROW_SEQS, 1)
    page_ids = jnp.arange(PAGES, dtype=jnp.int32)[None, None, :]
    is_valid = (page_ids < pages_row).reshape(MESH_ROWS, ROW_SEQS * PAGES)
    is_last = (page_ids == pages_row - 1).reshape(MESH_ROWS, ROW_SEQS * PAGES)
    n_cells = BATCH * PAGES
    cell_key = jax.random.permutation(keys_list[6], n_cells).reshape(MESH_ROWS, ROW_SEQS * PAGES) + jnp.where(is_last, 0, jnp.where(is_valid, n_cells, 2 * n_cells))
    cell_rank = jnp.argsort(jnp.argsort(cell_key, axis=1), axis=1)
    row_base = jnp.arange(MESH_ROWS, dtype=jnp.int32)[:, None] * (MESH_COLS * SLOTS)
    new_slot = jnp.take_along_axis(slot_order, cell_rank, axis=1) + row_base
    new_table = jnp.where(is_valid, new_slot, -1).reshape(BATCH, PAGES)
    slot_move = jnp.full((ALL_SLOTS,), -1, jnp.int32).at[dst_slot].set(move_ids)
    move_idx = slot_move[jnp.maximum(new_table, 0)]
    old_table = jnp.where((new_table >= 0) & (move_idx >= 0), src_slot[jnp.maximum(move_idx, 0)], new_table)
    return old_table.astype(jnp.int32), seq_len.astype(jnp.int32), src_slot.astype(jnp.int32), dst_slot.astype(jnp.int32)


def weight_draw(key, shape):
    return (jax.random.normal(key, shape, jnp.float32) * shape[1] ** -0.5).astype(jnp.bfloat16)


def setup_inputs(seed: int = 0, part: int = 0) -> dict:
    root = jax.random.key(seed)
    shared = jax.random.split(root, 6)
    own = jax.random.split(jax.random.fold_in(root, part), 4)
    pool_shape = (ALL_SLOTS, LAYERS, PAGE, KV_HEADS, HEAD)
    old_table, seq_len, src_slot, dst_slot = draw_layout(own[3])
    return dict(
        x_embed=jax.random.normal(own[0], (2, BATCH, D), jnp.float32).astype(jnp.bfloat16),
        w_query=weight_draw(shared[0], (LAYERS, D, HEADS * HEAD)),
        w_key=weight_draw(shared[1], (LAYERS, D, KV_HEADS * HEAD)),
        w_value=weight_draw(shared[2], (LAYERS, D, KV_HEADS * HEAD)),
        w_out=weight_draw(shared[3], (LAYERS, HEADS * HEAD, D)),
        w_up=weight_draw(shared[4], (LAYERS, D, FF)),
        w_down=weight_draw(shared[5], (LAYERS, FF, D)),
        k_pool=jax.random.normal(own[1], pool_shape, jnp.float32).astype(jnp.bfloat16),
        v_pool=jax.random.normal(own[2], pool_shape, jnp.float32).astype(jnp.bfloat16),
        old_table=old_table,
        seq_len=seq_len,
        src_slot=src_slot,
        dst_slot=dst_slot,
    )


def reference(x_embed, w_query, w_key, w_value, w_out, w_up, w_down, k_pool, v_pool, old_table, seq_len, src_slot, dst_slot):
    move_ids = jnp.arange(MOVES, dtype=jnp.int32)
    slot_move = jnp.full((ALL_SLOTS,), -1, jnp.int32).at[src_slot].set(move_ids)
    move_idx = slot_move[jnp.maximum(old_table, 0)]
    new_table = jnp.where((old_table >= 0) & (move_idx >= 0), dst_slot[jnp.maximum(move_idx, 0)], old_table)
    k_pool = k_pool.at[dst_slot].set(k_pool[src_slot])
    v_pool = v_pool.at[dst_slot].set(v_pool[src_slot])
    seq_ids = jnp.arange(BATCH)
    tok_pos = jnp.arange(PAGES * PAGE)
    q_group = HEADS // KV_HEADS
    step_outs = []
    for step_idx in range(2):
        cur_pos = seq_len + step_idx
        w_slot = new_table[seq_ids, cur_pos // PAGE]
        w_off = cur_pos % PAGE

        def layer_body(layer_state, layer_in):
            hidden, k_cache, v_cache = layer_state
            layer_idx, wq_l, wk_l, wv_l, wo_l, up_l, down_l = layer_in
            query = jnp.dot(hidden, wq_l, preferred_element_type=jnp.float32).astype(jnp.bfloat16)
            k_new = jnp.dot(hidden, wk_l, preferred_element_type=jnp.float32).astype(jnp.bfloat16).reshape(BATCH, KV_HEADS, HEAD)
            v_new = jnp.dot(hidden, wv_l, preferred_element_type=jnp.float32).astype(jnp.bfloat16).reshape(BATCH, KV_HEADS, HEAD)
            k_cache = k_cache.at[w_slot, layer_idx, w_off].set(k_new)
            v_cache = v_cache.at[w_slot, layer_idx, w_off].set(v_new)

            def attend(seq_in):
                q_row, table_row, limit_pos = seq_in
                page_sel = jnp.maximum(table_row, 0)
                page_keys = k_cache[page_sel, layer_idx].reshape(PAGES * PAGE, KV_HEADS, HEAD).astype(jnp.float32)
                page_vals = v_cache[page_sel, layer_idx].reshape(PAGES * PAGE, KV_HEADS, HEAD).astype(jnp.float32)
                q_heads = q_row.reshape(KV_HEADS, q_group, HEAD).astype(jnp.float32)
                scores = jnp.einsum('grd,tgd->grt', q_heads, page_keys) * HEAD ** -0.5
                scores = jnp.where(tok_pos <= limit_pos, scores, -1e30)
                attn_w = jax.nn.softmax(scores, axis=-1)
                return jnp.einsum('grt,tgd->grd', attn_w, page_vals).reshape(HEADS * HEAD).astype(jnp.bfloat16)

            attn_out = lax.map(attend, (query, new_table, cur_pos))
            hidden = (hidden.astype(jnp.float32) + jnp.dot(attn_out, wo_l, preferred_element_type=jnp.float32)).astype(jnp.bfloat16)
            up_act = jax.nn.gelu(jnp.dot(hidden, up_l, preferred_element_type=jnp.float32)).astype(jnp.bfloat16)
            hidden = (hidden.astype(jnp.float32) + jnp.dot(up_act, down_l, preferred_element_type=jnp.float32)).astype(jnp.bfloat16)
            return (hidden, k_cache, v_cache), None

        layer_xs = (jnp.arange(LAYERS), w_query, w_key, w_value, w_out, w_up, w_down)
        (hidden, k_pool, v_pool), _ = lax.scan(layer_body, (x_embed[step_idx], k_pool, v_pool), layer_xs)
        step_outs.append(hidden)
    return jnp.stack(step_outs), k_pool, v_pool
```

```python
import functools

import jax
import jax.numpy as jnp
from jax import lax
from jax.experimental import pallas as pl
from jax.experimental.pallas import tpu as pltpu
from jax.sharding import PartitionSpec as P

MESH_ID = pl.DeviceIdType.MESH
NEG = -1e30
UNROLL = 4


def take_pages(rows, k_rows, v_rows, layers):
    m = rows.shape[0]
    tail = k_rows.shape[1:]

    def body(rows_ref, k_in, v_in, *rest):
        outs, (buf, isem, osem) = rest[:layers], rest[layers:]
        ins, puts = [], []
        for layer in range(layers):
            for i in range(m):
                for which, ref in enumerate((k_in, v_in)):
                    j = 2 * i + which
                    cp = pltpu.make_async_copy(ref.at[rows_ref[i] + layer], buf.at[layer, j], isem.at[layer, j])
                    cp.start()
                    ins.append(cp)
        for layer in range(layers):
            for cp in ins[layer * 2 * m:(layer + 1) * 2 * m]:
                cp.wait()
            cp = pltpu.make_async_copy(buf.at[layer], outs[layer], osem.at[layer])
            cp.start()
            puts.append(cp)
        for cp in puts:
            cp.wait()

    any_spec = pl.BlockSpec(memory_space=pl.ANY)
    return pl.pallas_call(
        body,
        out_shape=[jax.ShapeDtypeStruct((2 * m,) + tail, k_rows.dtype)] * layers,
        in_specs=[pl.BlockSpec(memory_space=pltpu.SMEM), any_spec, any_spec],
        out_specs=[any_spec] * layers,
        scratch_shapes=[pltpu.VMEM((layers, 2 * m) + tail, k_rows.dtype),
                        pltpu.SemaphoreType.DMA((layers, 2 * m)), pltpu.SemaphoreType.DMA((layers,))],
        name="take_pages",
    )(rows, k_rows, v_rows)


def enter(axis, n, me):
    barrier = pltpu.get_barrier_semaphore()
    for d in range(1, n):
        pl.semaphore_signal(barrier, inc=1, device_id={axis: lax.rem(me + d, n)}, device_id_type=MESH_ID)
    pl.semaphore_wait(barrier, n - 1)


def gather_rows(x, axis, n, cid):
    def body(x_ref, o_ref, send_sem, recv_sem):
        me = lax.axis_index(axis)
        enter(axis, n, me)
        copies = []
        for d in range(1, n):
            cp = pltpu.make_async_remote_copy(
                src_ref=x_ref, dst_ref=o_ref.at[me], send_sem=send_sem.at[d], recv_sem=recv_sem.at[d],
                device_id={axis: lax.rem(me + d, n)}, device_id_type=MESH_ID)
            cp.start()
            copies.append(cp)
        o_ref[me] = x_ref[...]
        for cp in copies:
            cp.wait()

    return pl.pallas_call(
        body,
        out_shape=jax.ShapeDtypeStruct((n,) + x.shape, x.dtype),
        in_specs=[pl.BlockSpec(memory_space=pltpu.VMEM)],
        out_specs=pl.BlockSpec(memory_space=pltpu.VMEM),
        scratch_shapes=[pltpu.SemaphoreType.DMA((n,)), pltpu.SemaphoreType.DMA((n,))],
        compiler_params=pltpu.CompilerParams(collective_id=cid, has_side_effects=True),
        name="gather_rows",
    )(x)


def combine(acc, ml, axis, n, cid):
    rows, r, hd = acc.shape
    b = rows // n

    def body(acc_ref, ml_ref, o_ref, acc_in, ml_in, send_sem, recv_sem, send_ml, recv_ml):
        me = lax.axis_index(axis)
        enter(axis, n, me)
        copies = []
        for d in range(1, n):
            peer = lax.rem(me + d, n)
            for src, dst, ss, rs in (
                (acc_ref.at[pl.ds(peer * b, b)], acc_in.at[d], send_sem, recv_sem),
                (ml_ref, ml_in.at[d], send_ml, recv_ml),
            ):
                cp = pltpu.make_async_remote_copy(
                    src_ref=src, dst_ref=dst, send_sem=ss.at[d], recv_sem=rs.at[d],
                    device_id={axis: peer}, device_id_type=MESH_ID)
                cp.start()
                copies.append(cp)
        for cp in copies:
            cp.wait()
        lane = lax.broadcasted_iota(jnp.int32, (r, ml_ref.shape[2]), 1)
        for i in range(b):
            sel = lane == me * b + i
            pick = lambda t: jnp.sum(jnp.where(sel, t, 0.0), axis=1, keepdims=True)
            ms = [pick(ml_ref[0])] + [pick(ml_in[d, 0]) for d in range(1, n)]
            ls = [pick(ml_ref[1])] + [pick(ml_in[d, 1]) for d in range(1, n)]
            top = functools.reduce(jnp.maximum, ms)
            ws = [jnp.exp(m - top) for m in ms]
            den = sum(w * l for w, l in zip(ws, ls))
            num = ws[0] * acc_ref[me * b + i]
            for d in range(1, n):
                num += ws[d] * acc_in[d, i]
            o_ref[i] = (num / den).astype(o_ref.dtype)

    return pl.pallas_call(
        body,
        out_shape=jax.ShapeDtypeStruct((b, r, hd), jnp.bfloat16),
        in_specs=[pl.BlockSpec(memory_space=pltpu.VMEM)] * 2,
        out_specs=pl.BlockSpec(memory_space=pltpu.VMEM),
        scratch_shapes=[
            pltpu.VMEM((n, b, r, hd), jnp.float32),
            pltpu.VMEM((n,) + ml.shape, jnp.float32),
            pltpu.SemaphoreType.DMA((n,)), pltpu.SemaphoreType.DMA((n,)),
            pltpu.SemaphoreType.DMA((n,)), pltpu.SemaphoreType.DMA((n,)),
        ],
        compiler_params=pltpu.CompilerParams(collective_id=cid, has_side_effects=True),
        name="combine",
    )(acc, ml)


def attend(info, counts, qkv, k_src, v_src, prev_pools, state, layer, part, n_slots, layers, page, kvh, q_group, hd):
    prow = page * kvh
    qr = 2 * kvh * q_group
    n_seq = qkv.shape[0]
    scale = hd ** -0.5
    aliased = prev_pools is not None
    carried = state is not None

    def body(info_ref, cnt_ref, qkv_ref, k_in, v_in, *rest):
        if aliased:
            rest = rest[2:]
        if carried:
            acc_prev, ml_prev = rest[:2]
            rest = rest[2:]
        k_out, v_out, acc_ref, ml_ref, kbuf, vbuf, isem, osem = rest
        lo = cnt_ref[2 * part - 1] if part else 0
        mid = cnt_ref[2 * part]
        hi = cnt_ref[2 * part + 1]

        def loads(i):
            if part:
                k_at, v_at = info_ref[3, i] * 2, info_ref[3, i] * 2 + 1
            else:
                k_at = v_at = info_ref[0, i] * layers + layer
            return (pltpu.make_async_copy(k_in.at[k_at], kbuf.at[i], isem.at[0, i]),
                    pltpu.make_async_copy(v_in.at[v_at], vbuf.at[i], isem.at[1, i]))

        def stores(i):
            slot = info_ref[0, i]
            return (pltpu.make_async_copy(kbuf.at[i], k_out.at[slot * layers + layer], osem.at[0, i]),
                    pltpu.make_async_copy(vbuf.at[i], v_out.at[slot * layers + layer], osem.at[1, i]))

        @pl.loop(lo, hi)
        def _(i):
            for cp in loads(i):
                cp.start()

        if carried:
            acc_ref[...] = acc_prev[...]
            ml_ref[...] = ml_prev[...]
        else:
            acc_ref[...] = jnp.zeros_like(acc_ref)
            ml_ref[0] = jnp.full(ml_ref.shape[1:], NEG, jnp.float32)
            ml_ref[1] = jnp.zeros(ml_ref.shape[1:], jnp.float32)

        col = lax.broadcasted_iota(jnp.int32, (qr, prow), 1)
        row = lax.broadcasted_iota(jnp.int32, (qr, prow), 0)
        late = (row >= kvh * q_group).astype(jnp.int32)
        head_ok = lax.rem(col, kvh) == (row - late * (kvh * q_group)) // q_group
        need = col // kvh - late
        need = jnp.where(head_ok, need, 1 << 20)
        lane = lax.broadcasted_iota(jnp.int32, ml_ref.shape[1:], 1)
        wrow = lax.broadcasted_iota(jnp.int32, (4 * kvh, hd), 0) // kvh

        @pl.loop(0, (mid - lo + UNROLL - 1) // UNROLL)
        def _(g):
            base = lo + g * UNROLL
            idx, seqs, offs = [], [], []
            for u in range(UNROLL):
                i = base + u
                live = i < mid
                j = jnp.minimum(i, mid - 1)
                idx.append(j)
                seqs.append(jnp.where(live, info_ref[1, j], n_seq))
                offs.append(info_ref[2, j])

                @pl.when(live)
                def _():
                    for cp in loads(j):
                        cp.wait()

                    @pl.when(info_ref[2, j] < page)
                    def _():
                        off = info_ref[2, j]
                        w = jnp.minimum(off // 2, page // 2 - 2)
                        at = pl.ds(pl.multiple_of(w * (2 * kvh), 2 * kvh), 4 * kvh)
                        for buf, r0 in ((kbuf, qr), (vbuf, qr + 2 * kvh)):
                            new = qkv_ref[info_ref[1, j], r0:r0 + 2 * kvh, :].astype(jnp.float32)
                            first = jnp.concatenate([new[:kvh]] * 4, axis=0)
                            second = jnp.concatenate([new[kvh:]] * 4, axis=0)
                            old = buf[j, at, :].astype(jnp.float32)
                            tok = wrow + 2 * w
                            old = jnp.where(tok == off, first, jnp.where(tok == off + 1, second, old))
                            buf[j, at, :] = old.astype(jnp.bfloat16)

            res = []
            for u in range(UNROLL):
                q = qkv_ref[jnp.minimum(seqs[u], n_seq - 1), :qr, :]
                s = lax.dot_general(q, kbuf[idx[u]], (((1,), (1,)), ((), ())), preferred_element_type=jnp.float32) * scale
                s = jnp.where(need <= offs[u], s, NEG)
                m = jnp.max(s, axis=1, keepdims=True)
                p = jnp.exp(s - m)
                l = jnp.sum(p, axis=1, keepdims=True)
                o = jnp.dot(p.astype(jnp.bfloat16), vbuf[idx[u]], preferred_element_type=jnp.float32)
                res.append((m, l, o))
            for u in range(UNROLL):
                m, l, o = res[u]
                sel = lane == seqs[u]
                m_all, l_all = ml_ref[0], ml_ref[1]
                m_old = jnp.max(jnp.where(sel, m_all, NEG), axis=1, keepdims=True)
                m_new = jnp.maximum(m_old, m)
                alpha = jnp.exp(m_old - m_new)
                beta = jnp.exp(m - m_new)
                acc_ref[seqs[u]] = acc_ref[seqs[u]] * alpha + o * beta
                ml_ref[0] = jnp.where(sel, m_new, m_all)
                ml_ref[1] = jnp.where(sel, l_all * alpha + l * beta, l_all)
            for u in range(UNROLL):
                @pl.when(base + u < mid)
                def _():
                    for cp in stores(base + u):
                        cp.start()

        @pl.loop(mid, hi)
        def _(i):
            for cp in loads(i):
                cp.wait()
            for cp in stores(i):
                cp.start()

        @pl.loop(lo, hi)
        def _(i):
            for cp in stores(i):
                cp.wait()

    any_spec = pl.BlockSpec(memory_space=pl.ANY)
    vmem = pl.BlockSpec(memory_space=pltpu.VMEM)
    smem = pl.BlockSpec(memory_space=pltpu.SMEM)
    operands = [info, counts, qkv, k_src, v_src]
    specs = [smem, smem, vmem, any_spec, any_spec]
    alias = {}
    if aliased:
        alias = {5: 0, 6: 1}
        operands += list(prev_pools)
        specs += [any_spec, any_spec]
    if carried:
        operands += list(state)
        specs += [vmem, vmem]
    pool = jax.ShapeDtypeStruct((n_slots * layers, prow, hd), jnp.bfloat16)
    return pl.pallas_call(
        body,
        out_shape=[pool, pool,
                   jax.ShapeDtypeStruct((n_seq + 1, qr, hd), jnp.float32),
                   jax.ShapeDtypeStruct((2, qr, 128), jnp.float32)],
        in_specs=specs,
        out_specs=[any_spec, any_spec, vmem, vmem],
        scratch_shapes=[
            pltpu.VMEM((n_slots, prow, hd), jnp.bfloat16),
            pltpu.VMEM((n_slots, prow, hd), jnp.bfloat16),
            pltpu.SemaphoreType.DMA((2, n_slots)),
            pltpu.SemaphoreType.DMA((2, n_slots)),
        ],
        input_output_aliases=alias,
        cost_estimate=pl.CostEstimate(flops=400_000_000, bytes_accessed=16_000_000, transcendentals=0),
        name=f"attend_{layer}_{part}",
    )(*operands)


def solution(mesh):
    n_rows = mesh.shape['kv2']
    n_cols = mesh.shape['kv']
    dev_axes = ('rep', 'kv2', 'kv')
    seq_spec = P(None, dev_axes, None)
    pool_spec = P(dev_axes, None, None, None, None)
    table_spec = P(dev_axes, None)
    vec_spec = P(dev_axes)
    full_spec = P()

    def per_device(x_embed, w_query, w_key, w_value, w_out, w_up, w_down, k_pool, v_pool, old_table, seq_len, src_slot, dst_slot):
        n_slots, layers, page, kv_heads, head_dim = k_pool.shape
        heads = w_query.shape[2] // head_dim
        q_group = heads // kv_heads
        seq_dev = x_embed.shape[1]
        n_pages = old_table.shape[1]
        n_mig = src_slot.shape[0]
        n_dev = n_rows * n_cols
        row_seqs = seq_dev * n_cols
        prow = page * kv_heads
        width = x_embed.shape[2]
        me_row, me_col = lax.axis_index('kv2'), lax.axis_index('kv')
        me = me_row * n_cols + me_col
        base = me * n_slots

        meta = jnp.concatenate([src_slot, dst_slot, old_table.reshape(-1), seq_len])
        meta = lax.all_gather(meta, ('kv2', 'kv'))
        src_all = meta[:, :n_mig].reshape(-1)
        dst_all = meta[:, n_mig:2 * n_mig].reshape(-1)
        row_meta = lax.dynamic_slice_in_dim(meta, me_row * n_cols, n_cols, axis=0)
        row_table = row_meta[:, 2 * n_mig:2 * n_mig + seq_dev * n_pages].reshape(-1)
        row_len = row_meta[:, 2 * n_mig + seq_dev * n_pages:].reshape(-1)

        k_rows = k_pool.reshape(n_slots * layers, prow, head_dim)
        v_rows = v_pool.reshape(n_slots * layers, prow, head_dim)
        leaving = take_pages((src_slot - base) * layers, k_rows, v_rows, layers)
        moved = [lax.all_gather(t, ('kv2', 'kv'), tiled=True) for t in leaving]

        same = row_table[:, None] == src_all[None, :]
        new_table = jnp.where(same.any(axis=1), jnp.sum(jnp.where(same, dst_all[None, :], 0), axis=1), row_table)
        slots = jnp.arange(n_slots, dtype=jnp.int32)
        cells = jnp.arange(row_seqs * n_pages, dtype=jnp.int32)
        slot_cell = jnp.max(jnp.where(new_table[None, :] == (slots + base)[:, None], cells[None, :], -1), axis=1)
        moves = jnp.arange(n_dev * n_mig, dtype=jnp.int32)
        move_of = jnp.max(jnp.where(dst_all[None, :] == (slots + base)[:, None], moves[None, :], -1), axis=1)
        is_mig = move_of >= 0
        used = slot_cell >= 0
        seq_of = jnp.where(used, slot_cell // n_pages, row_seqs)
        seq_one = seq_of[:, None] == jnp.arange(row_seqs, dtype=jnp.int32)[None, :]
        len_of = jnp.sum(jnp.where(seq_one, row_len[None, :], 0), axis=1)
        off_of = len_of - (slot_cell % n_pages) * page
        off_of = jnp.where(used & (off_of >= 0) & (off_of < page), off_of, 2 * page)
        key = is_mig.astype(jnp.int32) * 2 + (~used).astype(jnp.int32)
        order = key * n_slots + slots
        pos = jnp.sum((order[None, :] < order[:, None]).astype(jnp.int32), axis=1)
        place = pos[None, :] == jnp.arange(64, dtype=jnp.int32)[:, None]
        info = jnp.stack([jnp.sum(jnp.where(place, t[None, :], 0), axis=1) for t in (slots, seq_of, off_of, move_of)])
        counts = jnp.sum((key[None, :] <= jnp.arange(4, dtype=jnp.int32)[:, None]).astype(jnp.int32), axis=1)

        hidden = x_embed.reshape(2 * seq_dev, width)
        pools = None
        for layer in range(layers):
            dot = lambda a, w: jnp.dot(a, w[layer], preferred_element_type=jnp.float32)
            query = dot(hidden, w_query).astype(jnp.bfloat16).reshape(2, seq_dev, heads, head_dim)
            k_new = dot(hidden, w_key).astype(jnp.bfloat16).reshape(2, seq_dev, kv_heads, head_dim)
            v_new = dot(hidden, w_value).astype(jnp.bfloat16).reshape(2, seq_dev, kv_heads, head_dim)
            per_seq = lambda t: jnp.swapaxes(t, 0, 1).reshape(seq_dev, -1, head_dim)
            qkv = jnp.concatenate([per_seq(query), per_seq(k_new), per_seq(v_new)], axis=1)
            qkv = gather_rows(qkv, 'kv', n_cols, 0).reshape(row_seqs, -1, head_dim)
            dims = dict(layer=layer, n_slots=n_slots, layers=layers, page=page, kvh=kv_heads, q_group=q_group, hd=head_dim)
            *pools, acc, ml = attend(info, counts, qkv, k_rows, v_rows, pools, None, part=0, **dims)
            *pools, acc, ml = attend(info, counts, qkv, moved[layer], moved[layer], pools, (acc, ml), part=1, **dims)
            o = combine(acc[:row_seqs], ml, 'kv', n_cols, 1)
            attn_out = jnp.swapaxes(o.reshape(seq_dev, 2, heads * head_dim), 0, 1).reshape(2 * seq_dev, heads * head_dim)
            hidden = (hidden.astype(jnp.float32) + dot(attn_out, w_out)).astype(jnp.bfloat16)
            up_act = jax.nn.gelu(dot(hidden, w_up)).astype(jnp.bfloat16)
            hidden = (hidden.astype(jnp.float32) + dot(up_act, w_down)).astype(jnp.bfloat16)
        k_out, v_out = (p.reshape(k_pool.shape) for p in pools)
        return hidden.reshape(2, seq_dev, width), k_out, v_out

    return jax.shard_map(per_device, mesh=mesh, in_specs=(seq_spec, full_spec, full_spec, full_spec, full_spec, full_spec, full_spec, pool_spec, pool_spec, table_spec, vec_spec, vec_spec, vec_spec), out_specs=(seq_spec, pool_spec, pool_spec), check_vma=False)
```

```python
import functools

import jax
import jax.numpy as jnp
from jax import lax
from jax.experimental import pallas as pl
from jax.experimental.pallas import tpu as pltpu
from jax.sharding import PartitionSpec as P


MESH_ID = pl.DeviceIdType.MESH
NEG = -1e30
UNROLL = 4
Z_CORE = 6
Y_CORE = 10


def uninit(shape, dtype):
    def body(o_ref):
        pass

    return pl.pallas_call(
        body, out_shape=jax.ShapeDtypeStruct(shape, dtype), out_specs=pl.BlockSpec(memory_space=pl.ANY), name="uninit")()


def take_pages(rows, k_rows, v_rows, layers):
    m = rows.shape[0]
    prow, hd = k_rows.shape[1:]

    def body(rows_ref, k_in, v_in, *rest):
        outs, (buf, isem, osem) = rest[:layers], rest[layers:]
        ins, puts = [], []
        for layer in range(layers):
            for i in range(m):
                for which, ref in enumerate((k_in, v_in)):
                    cp = pltpu.make_async_copy(
                        ref.at[rows_ref[i] + layer], buf.at[layer, i, pl.ds(which * prow, prow)], isem.at[layer, 2 * i + which])
                    cp.start()
                    ins.append(cp)
        for layer in range(layers):
            for cp in ins[layer * 2 * m:(layer + 1) * 2 * m]:
                cp.wait()
            cp = pltpu.make_async_copy(buf.at[layer], outs[layer], osem.at[layer])
            cp.start()
            puts.append(cp)
        for cp in puts:
            cp.wait()

    any_spec = pl.BlockSpec(memory_space=pl.ANY)
    return pl.pallas_call(
        body,
        out_shape=[jax.ShapeDtypeStruct((m, 2 * prow, hd), k_rows.dtype)] * layers,
        in_specs=[pl.BlockSpec(memory_space=pltpu.SMEM), any_spec, any_spec],
        out_specs=[any_spec] * layers,
        scratch_shapes=[pltpu.VMEM((layers, m, 2 * prow, hd), k_rows.dtype),
                        pltpu.SemaphoreType.DMA((layers, 2 * m)), pltpu.SemaphoreType.DMA((layers,))],
        cost_estimate=pl.CostEstimate(flops=100_000_000, bytes_accessed=12_000_000, transcendentals=0),
        name="take_pages",
    )(rows, k_rows, v_rows)


def pick(lists, sources, splits):
    n = sum(splits)
    tail, dtype = sources[0].shape[1:], sources[0].dtype

    def body(idx_ref, *rest):
        ins, outs, (buf, isem, osem) = rest[:len(sources)], rest[len(sources):-3], rest[-3:]

        @pl.loop(0, n)
        def _(i):
            at, lo = idx_ref[i], 0
            for ref in ins:
                hi = lo + ref.shape[0]

                @pl.when((at >= lo) & (at < hi))
                def _():
                    pltpu.make_async_copy(ref.at[at - lo], buf.at[i], isem.at[i]).start()

                lo = hi

        @pl.loop(0, n)
        def _(i):
            pltpu.make_async_copy(ins[0].at[0], buf.at[i], isem.at[i]).wait()

        puts, lo = [], 0
        for j, size in enumerate(splits):
            cp = pltpu.make_async_copy(buf.at[pl.ds(lo, size)], outs[j], osem.at[j])
            cp.start()
            puts.append(cp)
            lo += size
        for cp in puts:
            cp.wait()

    any_spec = pl.BlockSpec(memory_space=pl.ANY)
    return pl.pallas_call(
        body,
        out_shape=[jax.ShapeDtypeStruct((size,) + tail, dtype) for size in splits],
        in_specs=[pl.BlockSpec(memory_space=pltpu.SMEM)] + [any_spec] * len(sources),
        out_specs=[any_spec] * len(splits),
        scratch_shapes=[pltpu.VMEM((n,) + tail, dtype), pltpu.SemaphoreType.DMA((n,)), pltpu.SemaphoreType.DMA((len(splits),))],
        cost_estimate=pl.CostEstimate(flops=100_000_000, bytes_accessed=5_000_000, transcendentals=0),
    )(lists, *sources)


def share_plan(x, mesh_shape, cid):
    nx, ny, nz = mesh_shape
    n = nx * ny * nz

    def body(x_ref, o_ref, send_sem, recv_sem):
        me = (lax.axis_index('rep') * ny + lax.axis_index('kv2')) * nz + lax.axis_index('kv')

        def coords(d):
            p = lax.rem(me + d, n)
            return (p // (ny * nz), lax.rem(p // nz, ny), lax.rem(p, nz))

        barrier = pltpu.get_barrier_semaphore()
        for d in range(1, n):
            pl.semaphore_signal(barrier, inc=1, device_id=coords(d), device_id_type=MESH_ID)
        pl.semaphore_wait(barrier, n - 1)
        copies = []
        for d in range(1, n):
            cp = pltpu.make_async_remote_copy(
                src_ref=x_ref, dst_ref=o_ref.at[me], send_sem=send_sem.at[d], recv_sem=recv_sem.at[d],
                device_id=coords(d), device_id_type=MESH_ID)
            cp.start()
            copies.append(cp)
        o_ref[me] = x_ref[...]
        for cp in copies:
            cp.wait()

    return pl.pallas_call(
        body,
        out_shape=jax.ShapeDtypeStruct((n,) + x.shape, x.dtype),
        in_specs=[pl.BlockSpec(memory_space=pltpu.VMEM)],
        out_specs=pl.BlockSpec(memory_space=pltpu.VMEM),
        scratch_shapes=[pltpu.SemaphoreType.DMA((n,)), pltpu.SemaphoreType.DMA((n,))],
        compiler_params=pltpu.CompilerParams(collective_id=cid, has_side_effects=True),
        name="share_plan",
    )(x)


def route(dst, dev, pos, n_mig, n_slots):
    n_dev = dev.shape[0] // n_mig
    z_at, y_at = 2 * n_mig, 2 * n_mig + 2 * 3 * Z_CORE

    def body(dst_ref, dev_ref, pos_ref, z_ref, y_ref, s_ref, cnt, cnt2):
        row, colm = pos_ref[0], pos_ref[1]
        half, core = colm >> 1, colm & 1
        me = row * 4 + colm

        @pl.loop(0, 64)
        def _(i):
            z_ref[i] = 0
            y_ref[i] = 0
            s_ref[i] = -1
            cnt[i] = 0

        @pl.loop(0, 8)
        def _(i):
            cnt2[i] = 0

        @pl.loop(0, n_dev)
        def _(d):
            si, sy, sc = d >> 2, (d >> 1) & 1, d & 1

            @pl.loop(0, n_mig)
            def _(e):
                dd = dev_ref[d * n_mig + e]
                di, dy = dd >> 2, (dd >> 1) & 1
                c1 = (d >> 1) * 4 + di
                k = cnt[c1]
                cnt[c1] = k + 1
                cross = (dy != sy).astype(jnp.int32)
                c2 = di * 2 + sy
                k2 = cnt2[c2]
                cnt2[c2] = k2 + cross
                shift = (di - si) & 3
                at = jnp.where(sc == core, e, n_mig + e)
                z_slot = (shift - 1) * Z_CORE + (k >> 1)
                here = jnp.where(shift == 0, at, z_at + z_slot + jnp.where((k & 1) == core, 0, 3 * Z_CORE))

                @pl.when((si == row) & (sy == half) & (shift != 0) & ((k & 1) == core) & (k < 2 * Z_CORE))
                def _():
                    z_ref[z_slot] = at

                @pl.when((di == row) & (sy == half) & (cross == 1) & ((k2 & 1) == core) & (k2 < 2 * Y_CORE))
                def _():
                    y_ref[k2 >> 1] = jnp.minimum(here, y_at - 1)

                @pl.when(dd == me)
                def _():
                    by_y = y_at + (k2 >> 1) + jnp.where((k2 & 1) == core, 0, Y_CORE)
                    s_ref[dst_ref[d * n_mig + e] - me * n_slots] = jnp.where(cross == 1, by_y, here)

    smem = pl.BlockSpec(memory_space=pltpu.SMEM)
    return pl.pallas_call(
        body,
        out_shape=[jax.ShapeDtypeStruct((64,), jnp.int32)] * 3,
        in_specs=[smem] * 3,
        out_specs=[smem] * 3,
        scratch_shapes=[pltpu.SMEM((64,), jnp.int32), pltpu.SMEM((8,), jnp.int32)],
        cost_estimate=pl.CostEstimate(flops=100_000_000, bytes_accessed=1_000_000, transcendentals=0),
        name="route",
    )(dst, dev, pos)


def enter(axis, n, me):
    barrier = pltpu.get_barrier_semaphore()
    for d in range(1, n):
        pl.semaphore_signal(barrier, inc=1, device_id={axis: lax.rem(me + d, n)}, device_id_type=MESH_ID)
    pl.semaphore_wait(barrier, n - 1)


def gather_rows(x, axis, n, cid):
    def body(x_ref, o_ref, send_sem, recv_sem):
        me = lax.axis_index(axis)
        enter(axis, n, me)
        copies = []
        for d in range(1, n):
            cp = pltpu.make_async_remote_copy(
                src_ref=x_ref, dst_ref=o_ref.at[me], send_sem=send_sem.at[d], recv_sem=recv_sem.at[d],
                device_id={axis: lax.rem(me + d, n)}, device_id_type=MESH_ID)
            cp.start()
            copies.append(cp)
        o_ref[me] = x_ref[...]
        for cp in copies:
            cp.wait()

    return pl.pallas_call(
        body,
        out_shape=jax.ShapeDtypeStruct((n,) + x.shape, x.dtype),
        in_specs=[pl.BlockSpec(memory_space=pltpu.VMEM)],
        out_specs=pl.BlockSpec(memory_space=pltpu.VMEM),
        scratch_shapes=[pltpu.SemaphoreType.DMA((n,)), pltpu.SemaphoreType.DMA((n,))],
        compiler_params=pltpu.CompilerParams(collective_id=cid, has_side_effects=True),
        name="gather_rows",
    )(x)


def combine(acc, ml, axis, n, cid):
    rows, r, hd = acc.shape
    b = rows // n

    def body(acc_ref, ml_ref, o_ref, acc_in, ml_in, send_sem, recv_sem, send_ml, recv_ml):
        me = lax.axis_index(axis)
        enter(axis, n, me)
        copies = []
        for d in range(1, n):
            peer = lax.rem(me + d, n)
            for src, dst, ss, rs in (
                (acc_ref.at[pl.ds(peer * b, b)], acc_in.at[d], send_sem, recv_sem),
                (ml_ref, ml_in.at[d], send_ml, recv_ml),
            ):
                cp = pltpu.make_async_remote_copy(
                    src_ref=src, dst_ref=dst, send_sem=ss.at[d], recv_sem=rs.at[d],
                    device_id={axis: peer}, device_id_type=MESH_ID)
                cp.start()
                copies.append(cp)
        for cp in copies:
            cp.wait()
        lane = lax.broadcasted_iota(jnp.int32, (r, ml_ref.shape[2]), 1)
        for i in range(b):
            sel = lane == me * b + i
            pick = lambda t: jnp.sum(jnp.where(sel, t, 0.0), axis=1, keepdims=True)
            ms = [pick(ml_ref[0])] + [pick(ml_in[d, 0]) for d in range(1, n)]
            ls = [pick(ml_ref[1])] + [pick(ml_in[d, 1]) for d in range(1, n)]
            top = functools.reduce(jnp.maximum, ms)
            ws = [jnp.exp(m - top) for m in ms]
            den = sum(w * l for w, l in zip(ws, ls))
            num = ws[0] * acc_ref[me * b + i]
            for d in range(1, n):
                num += ws[d] * acc_in[d, i]
            o_ref[i] = (num / den).astype(o_ref.dtype)

    return pl.pallas_call(
        body,
        out_shape=jax.ShapeDtypeStruct((b, r, hd), jnp.bfloat16),
        in_specs=[pl.BlockSpec(memory_space=pltpu.VMEM)] * 2,
        out_specs=pl.BlockSpec(memory_space=pltpu.VMEM),
        scratch_shapes=[
            pltpu.VMEM((n, b, r, hd), jnp.float32),
            pltpu.VMEM((n,) + ml.shape, jnp.float32),
            pltpu.SemaphoreType.DMA((n,)), pltpu.SemaphoreType.DMA((n,)),
            pltpu.SemaphoreType.DMA((n,)), pltpu.SemaphoreType.DMA((n,)),
        ],
        compiler_params=pltpu.CompilerParams(collective_id=cid, has_side_effects=True),
        name="combine",
    )(acc, ml)


def mlp_pair(attn, hidden, w_out, w_up, w_down, layer, cid):
    rows, d = attn.shape
    ff = w_up.shape[2]
    r = -(-rows // 32) * 32
    tile = 512
    d_half, f_half = d // 2, ff // 2
    n_o, n_f = d_half // tile, f_half // tile
    ring_c, ring_r = min(8, n_o + n_f), min(6, n_f)
    attn, hidden = (jnp.pad(t, ((0, r - rows), (0, 0))) for t in (attn, hidden))

    def body(attn_ref, hid_ref, wo_ref, wu_ref, wd_ref, o_ref, x_all, h_all, hm, act, acc, rx, wc, wr, csem, rsem, ssem, qsem):
        me = lax.axis_index('kv')
        core = lax.rem(me, 2)
        peer = me + 1 - 2 * core
        mine, other = pl.ds(core * r, r), pl.ds((1 - core) * r, r)

        def col(c, is_out):
            if is_out:
                src = wo_ref.at[layer, :, pl.ds(pl.multiple_of(core * d_half + c * tile, tile), tile)]
            else:
                src = wu_ref.at[layer, :, pl.ds(pl.multiple_of(core * f_half + (c - n_o) * tile, tile), tile)]
            slot = lax.rem(c, ring_c)
            return pltpu.make_async_copy(src, wc.at[slot], csem.at[slot])

        def row(j):
            slot = lax.rem(j, ring_r)
            src = wd_ref.at[layer, pl.ds(pl.multiple_of(core * f_half + j * tile, tile), tile), :]
            return pltpu.make_async_copy(src, wr.at[slot], rsem.at[slot])

        for c in range(ring_c):
            col(c, c < n_o).start()

        barrier = pltpu.get_barrier_semaphore()
        pl.semaphore_signal(barrier, inc=1, device_id={'kv': peer}, device_id_type=MESH_ID)
        pl.semaphore_wait(barrier, 1)

        def send(src, dst, i):
            return pltpu.make_async_remote_copy(
                src_ref=src, dst_ref=dst, send_sem=ssem.at[i], recv_sem=qsem.at[i],
                device_id={'kv': peer}, device_id_type=MESH_ID)

        swaps = [send(attn_ref, x_all.at[mine], 0), send(hid_ref, h_all.at[mine], 1)]
        for cp in swaps:
            cp.start()
        x_all[mine] = attn_ref[...]
        h_all[mine] = hid_ref[...]
        for cp in swaps:
            cp.wait()

        @pl.loop(0, n_o)
        def _(c):
            col(c, True).wait()
            at = pl.ds(pl.multiple_of(core * d_half + c * tile, tile), tile)
            part = jnp.dot(x_all[...], wc[lax.rem(c, ring_c)], preferred_element_type=jnp.float32)
            hm[:, at] = (h_all[:, at].astype(jnp.float32) + part).astype(jnp.bfloat16)

            @pl.when(c + ring_c < n_o + n_f)
            def _():
                col(c + ring_c, False).start()

        own_cols = pl.ds(pl.multiple_of(core * d_half, tile), d_half)
        cp = send(hm.at[:, own_cols], hm.at[:, own_cols], 2)
        cp.start()
        acc[...] = jnp.zeros_like(acc)
        cp.wait()

        @pl.loop(0, n_f)
        def _(j):
            c = j + n_o
            col(c, False).wait()
            up = jnp.dot(hm[...], wc[lax.rem(c, ring_c)], preferred_element_type=jnp.float32)
            act[:, pl.ds(pl.multiple_of(j * tile, tile), tile)] = jax.nn.gelu(up).astype(jnp.bfloat16)

            @pl.when(c + ring_c < n_o + n_f)
            def _():
                col(c + ring_c, False).start()

            @pl.when(j < ring_r)
            def _():
                row(j).start()

        @pl.loop(0, n_f)
        def _(j):
            row(j).wait()
            acc[...] += jnp.dot(act[:, pl.ds(pl.multiple_of(j * tile, tile), tile)], wr[lax.rem(j, ring_r)],
                                preferred_element_type=jnp.float32)

            @pl.when(j + ring_r < n_f)
            def _():
                row(j + ring_r).start()

        cp = send(acc.at[other], rx, 3)
        cp.start()
        cp.wait()
        o_ref[...] = (hm[mine].astype(jnp.float32) + (acc[mine] + rx[...])).astype(o_ref.dtype)

    vmem, any_spec = pl.BlockSpec(memory_space=pltpu.VMEM), pl.BlockSpec(memory_space=pl.ANY)
    out = pl.pallas_call(
        body,
        out_shape=jax.ShapeDtypeStruct((r, d), jnp.bfloat16),
        in_specs=[vmem, vmem, any_spec, any_spec, any_spec],
        out_specs=vmem,
        scratch_shapes=[
            pltpu.VMEM((2 * r, d), jnp.bfloat16), pltpu.VMEM((2 * r, d), jnp.bfloat16), pltpu.VMEM((2 * r, d), jnp.bfloat16),
            pltpu.VMEM((2 * r, f_half), jnp.bfloat16), pltpu.VMEM((2 * r, d), jnp.float32), pltpu.VMEM((r, d), jnp.float32),
            pltpu.VMEM((ring_c, d, tile), jnp.bfloat16), pltpu.VMEM((ring_r, tile, d), jnp.bfloat16),
            pltpu.SemaphoreType.DMA((ring_c,)), pltpu.SemaphoreType.DMA((ring_r,)),
            pltpu.SemaphoreType.DMA((4,)), pltpu.SemaphoreType.DMA((4,)),
        ],
        compiler_params=pltpu.CompilerParams(collective_id=cid, has_side_effects=True, vmem_limit_bytes=58 * 1024 * 1024),
        cost_estimate=pl.CostEstimate(flops=6_000_000_000, bytes_accessed=60_000_000, transcendentals=0),
    )(attn, hidden, w_out, w_up, w_down)
    return out[:rows]


def attend(info, counts, qkv, sources, prev_pools, state, layer, part, n_slots, layers, page, kvh, q_group, hd):
    prow = page * kvh
    qr = 2 * kvh * q_group
    n_seq = qkv.shape[0]
    scale = hd ** -0.5
    aliased = prev_pools is not None
    carried = state is not None

    def body(info_ref, cnt_ref, qkv_ref, *rest):
        ins, rest = rest[:len(sources)], rest[len(sources):]
        if aliased:
            rest = rest[2:]
        if carried:
            acc_prev, ml_prev = rest[:2]
            rest = rest[2:]
        k_out, v_out, acc_ref, ml_ref, kbuf, vbuf, isem, osem = rest
        lo = cnt_ref[2 * part - 1] if part else 0
        mid = cnt_ref[2 * part]
        hi = cnt_ref[2 * part + 1]

        def load_from(k_page, v_page, i):
            return (pltpu.make_async_copy(k_page, kbuf.at[i], isem.at[0, i]),
                    pltpu.make_async_copy(v_page, vbuf.at[i], isem.at[1, i]))

        def loads(i):
            if part:
                return load_from(ins[0].at[0, pl.ds(0, prow)], ins[0].at[0, pl.ds(prow, prow)], i)
            at = info_ref[0, i] * layers + layer
            return load_from(ins[0].at[at], ins[1].at[at], i)

        def start_loads(i):
            if not part:
                for cp in loads(i):
                    cp.start()
                return
            at, first = info_ref[3, i], 0
            for ref in ins:
                last = first + ref.shape[0]

                @pl.when((at >= first) & (at < last))
                def _():
                    u = at - first
                    for cp in load_from(ref.at[u, pl.ds(0, prow)], ref.at[u, pl.ds(prow, prow)], i):
                        cp.start()

                first = last

        def stores(i):
            slot = info_ref[0, i]
            return (pltpu.make_async_copy(kbuf.at[i], k_out.at[slot * layers + layer], osem.at[0, i]),
                    pltpu.make_async_copy(vbuf.at[i], v_out.at[slot * layers + layer], osem.at[1, i]))

        @pl.loop(lo, hi)
        def _(i):
            start_loads(i)

        if carried:
            acc_ref[...] = acc_prev[...]
            ml_ref[...] = ml_prev[...]
        else:
            acc_ref[...] = jnp.zeros_like(acc_ref)
            ml_ref[0] = jnp.full(ml_ref.shape[1:], NEG, jnp.float32)
            ml_ref[1] = jnp.zeros(ml_ref.shape[1:], jnp.float32)

        col = lax.broadcasted_iota(jnp.int32, (qr, prow), 1)
        row = lax.broadcasted_iota(jnp.int32, (qr, prow), 0)
        late = (row >= kvh * q_group).astype(jnp.int32)
        head_ok = lax.rem(col, kvh) == (row - late * (kvh * q_group)) // q_group
        need = col // kvh - late
        need = jnp.where(head_ok, need, 1 << 20)
        lane = lax.broadcasted_iota(jnp.int32, ml_ref.shape[1:], 1)
        wrow = lax.broadcasted_iota(jnp.int32, (4 * kvh, hd), 0) // kvh

        @pl.loop(0, (mid - lo + UNROLL - 1) // UNROLL)
        def _(g):
            base = lo + g * UNROLL
            idx, seqs, offs = [], [], []
            for u in range(UNROLL):
                i = base + u
                live = i < mid
                j = jnp.minimum(i, mid - 1)
                idx.append(j)
                seqs.append(jnp.where(live, info_ref[1, j], n_seq))
                offs.append(info_ref[2, j])

                @pl.when(live)
                def _():
                    for cp in loads(j):
                        cp.wait()

                    @pl.when(info_ref[2, j] < page)
                    def _():
                        off = info_ref[2, j]
                        w = jnp.minimum(off // 2, page // 2 - 2)
                        at = pl.ds(pl.multiple_of(w * (2 * kvh), 2 * kvh), 4 * kvh)
                        for buf, r0 in ((kbuf, qr), (vbuf, qr + 2 * kvh)):
                            new = qkv_ref[info_ref[1, j], r0:r0 + 2 * kvh, :].astype(jnp.float32)
                            first = jnp.concatenate([new[:kvh]] * 4, axis=0)
                            second = jnp.concatenate([new[kvh:]] * 4, axis=0)
                            old = buf[j, at, :].astype(jnp.float32)
                            tok = wrow + 2 * w
                            old = jnp.where(tok == off, first, jnp.where(tok == off + 1, second, old))
                            buf[j, at, :] = old.astype(jnp.bfloat16)

            res = []
            for u in range(UNROLL):
                q = qkv_ref[jnp.minimum(seqs[u], n_seq - 1), :qr, :]
                s = lax.dot_general(q, kbuf[idx[u]], (((1,), (1,)), ((), ())), preferred_element_type=jnp.float32) * scale
                s = jnp.where(need <= offs[u], s, NEG)
                m = jnp.max(s, axis=1, keepdims=True)
                p = jnp.exp(s - m)
                l = jnp.sum(p, axis=1, keepdims=True)
                o = jnp.dot(p.astype(jnp.bfloat16), vbuf[idx[u]], preferred_element_type=jnp.float32)
                res.append((m, l, o))
            for u in range(UNROLL):
                m, l, o = res[u]
                sel = lane == seqs[u]
                m_all, l_all = ml_ref[0], ml_ref[1]
                m_old = jnp.max(jnp.where(sel, m_all, NEG), axis=1, keepdims=True)
                m_new = jnp.maximum(m_old, m)
                alpha = jnp.exp(m_old - m_new)
                beta = jnp.exp(m - m_new)
                acc_ref[seqs[u]] = acc_ref[seqs[u]] * alpha + o * beta
                ml_ref[0] = jnp.where(sel, m_new, m_all)
                ml_ref[1] = jnp.where(sel, l_all * alpha + l * beta, l_all)
            for u in range(UNROLL):
                @pl.when(base + u < mid)
                def _():
                    for cp in stores(base + u):
                        cp.start()

        @pl.loop(mid, hi)
        def _(i):
            for cp in loads(i):
                cp.wait()
            for cp in stores(i):
                cp.start()

        @pl.loop(lo, hi)
        def _(i):
            for cp in stores(i):
                cp.wait()

    any_spec = pl.BlockSpec(memory_space=pl.ANY)
    vmem = pl.BlockSpec(memory_space=pltpu.VMEM)
    smem = pl.BlockSpec(memory_space=pltpu.SMEM)
    operands = [info, counts, qkv, *sources]
    specs = [smem, smem, vmem] + [any_spec] * len(sources)
    alias = {}
    if aliased:
        alias = {len(operands): 0, len(operands) + 1: 1}
        operands += list(prev_pools)
        specs += [any_spec, any_spec]
    if carried:
        operands += list(state)
        specs += [vmem, vmem]
    pool = jax.ShapeDtypeStruct((n_slots * layers, prow, hd), jnp.bfloat16)
    return pl.pallas_call(
        body,
        out_shape=[pool, pool,
                   jax.ShapeDtypeStruct((n_seq + 1, qr, hd), jnp.float32),
                   jax.ShapeDtypeStruct((2, qr, 128), jnp.float32)],
        in_specs=specs,
        out_specs=[any_spec, any_spec, vmem, vmem],
        scratch_shapes=[
            pltpu.VMEM((n_slots, prow, hd), jnp.bfloat16),
            pltpu.VMEM((n_slots, prow, hd), jnp.bfloat16),
            pltpu.SemaphoreType.DMA((2, n_slots)),
            pltpu.SemaphoreType.DMA((2, n_slots)),
        ],
        input_output_aliases=alias,
        cost_estimate=pl.CostEstimate(flops=400_000_000, bytes_accessed=16_000_000, transcendentals=0),
    )(*operands)


def solution(mesh):
    n_rows = mesh.shape['kv2']
    n_cols = mesh.shape['kv']
    dev_axes = ('rep', 'kv2', 'kv')
    seq_spec = P(None, dev_axes, None)
    pool_spec = P(dev_axes, None, None, None, None)
    table_spec = P(dev_axes, None)
    vec_spec = P(dev_axes)
    full_spec = P()

    def per_device(x_embed, w_query, w_key, w_value, w_out, w_up, w_down, k_pool, v_pool, old_table, seq_len, src_slot, dst_slot):
        n_slots, layers, page, kv_heads, head_dim = k_pool.shape
        heads = w_query.shape[2] // head_dim
        q_group = heads // kv_heads
        seq_dev = x_embed.shape[1]
        n_pages = old_table.shape[1]
        n_mig = src_slot.shape[0]
        n_dev = n_rows * n_cols
        row_seqs = seq_dev * n_cols
        prow = page * kv_heads
        width = x_embed.shape[2]
        me_row, me_col = lax.axis_index('kv2'), lax.axis_index('kv')
        me = me_row * n_cols + me_col
        base = me * n_slots

        n_rep = mesh.shape['rep']
        words = [src_slot, dst_slot, dst_slot // n_slots, old_table.reshape(-1), seq_len]
        cuts = [0]
        for w in words:
            cuts.append(cuts[-1] + w.shape[0])
        meta = jnp.pad(jnp.concatenate(words), (0, 128 - cuts[-1])).reshape(1, 128)
        meta_all = share_plan(meta, (n_rep, n_rows, n_cols), 2).reshape(n_rep, n_dev, 128)
        meta = lax.dynamic_index_in_dim(meta_all, lax.axis_index('rep'), 0, keepdims=False)
        src_all, dst_all, dev_all = (meta[:, cuts[t]:cuts[t + 1]].reshape(-1) for t in range(3))
        row_meta = lax.dynamic_slice_in_dim(meta, me_row * n_cols, n_cols, axis=0)
        row_table = row_meta[:, cuts[3]:cuts[4]].reshape(-1)
        row_len = row_meta[:, cuts[4]:cuts[5]].reshape(-1)

        dev_by = meta_all[:, :, cuts[2]:cuts[3]]
        to_row = dev_by // n_cols
        rows4 = jnp.arange(n_rows, dtype=jnp.int32)
        goes = (to_row[..., None] == rows4).astype(jnp.int32).sum(axis=2)
        per_chip = goes.reshape(n_rep, n_rows, n_cols // 2, 2, n_rows).sum(axis=3)
        leaves = rows4[:, None] != rows4[None, :]
        z_full = ((per_chip > 2 * Z_CORE) & leaves[None, :, None, :]).any()
        side = (jnp.arange(n_dev, dtype=jnp.int32) // 2 % 2)[None, :, None]
        crosses = dev_by // 2 % 2 != side
        per_side = ((to_row[..., None] == rows4) & crosses[..., None]).astype(jnp.int32).sum(axis=2)
        y_full = (per_side.reshape(n_rep, n_rows, n_cols // 2, 2, n_rows).sum(axis=(1, 3)) > 2 * Y_CORE).any()
        full = z_full | y_full

        k_rows = k_pool.reshape(n_slots * layers, prow, head_dim)
        v_rows = v_pool.reshape(n_slots * layers, prow, head_dim)
        leaving = take_pages((src_slot - base) * layers, k_rows, v_rows, layers)
        pos = jnp.stack([me_row, me_col]).astype(jnp.int32)
        z_list, y_list, unit_of = route(dst_all, dev_all, pos, n_mig, n_slots)
        pair = [(c, c ^ 1) for c in range(n_cols)]
        over = [(c, c ^ 2) for c in range(n_cols)]
        z_hops = [[(r, (r + s) % n_rows) for r in range(n_rows)] for s in range(1, n_rows)]

        def along_z(hops):
            got = []
            for h, z in zip(hops, z_hops):
                got.append(lax.ppermute(h, 'kv2', z))
            return got

        def to_y(units, got):
            units = units + got + [lax.ppermute(g, 'kv', pair) for g in got]
            hop, = pick(y_list, units, [Y_CORE])
            return units, hop

        def along_y(units, hop):
            got = lax.ppermute(hop, 'kv', over)
            return units + [got, lax.ppermute(got, 'kv', pair)]

        same = row_table[:, None] == src_all[None, :]
        new_table = jnp.where(same.any(axis=1), jnp.sum(jnp.where(same, dst_all[None, :], 0), axis=1), row_table)
        slots = jnp.arange(n_slots, dtype=jnp.int32)
        cells = jnp.arange(row_seqs * n_pages, dtype=jnp.int32)
        slot_cell = jnp.max(jnp.where(new_table[None, :] == (slots + base)[:, None], cells[None, :], -1), axis=1)
        moves = jnp.arange(n_dev * n_mig, dtype=jnp.int32)
        move_of = jnp.max(jnp.where(dst_all[None, :] == (slots + base)[:, None], moves[None, :], -1), axis=1)
        is_mig = move_of >= 0
        used = slot_cell >= 0
        seq_of = jnp.where(used, slot_cell // n_pages, row_seqs)
        seq_one = seq_of[:, None] == jnp.arange(row_seqs, dtype=jnp.int32)[None, :]
        len_of = jnp.sum(jnp.where(seq_one, row_len[None, :], 0), axis=1)
        off_of = len_of - (slot_cell % n_pages) * page
        off_of = jnp.where(used & (off_of >= 0) & (off_of < page), off_of, 2 * page)
        key = is_mig.astype(jnp.int32) * 2 + (~used).astype(jnp.int32)
        order = key * n_slots + slots
        pos = jnp.sum((order[None, :] < order[:, None]).astype(jnp.int32), axis=1)
        place = pos[None, :] == jnp.arange(64, dtype=jnp.int32)[:, None]
        fast_units = 2 * n_mig + 2 * (n_rows - 1) * Z_CORE + 2 * Y_CORE
        unit = jnp.where(full, slots + fast_units, unit_of[:n_slots])
        info = jnp.stack([jnp.sum(jnp.where(place, t[None, :], 0), axis=1) for t in (slots, seq_of, off_of, unit)])
        counts = jnp.sum((key[None, :] <= jnp.arange(4, dtype=jnp.int32)[:, None]).astype(jnp.int32), axis=1)

        def all_pages(layer):
            def collect():
                every = lax.all_gather(leaving[layer], ('kv2', 'kv'), tiled=True)
                return pick(jnp.maximum(move_of, 0), [every], [n_slots])[0]

            return lax.cond(full, collect, lambda: uninit((n_slots, 2 * prow, head_dim), jnp.bfloat16))

        hidden = x_embed.reshape(2 * seq_dev, width)
        pools = None
        units = [[own, lax.ppermute(own, 'kv', pair)] for own in leaving]
        hops = pick(z_list, units[0], [Z_CORE] * (n_rows - 1))
        *hops, z_list, hidden = lax.optimization_barrier((*hops, z_list, hidden))
        got = along_z(hops)
        for layer in range(layers):
            dot = lambda a, w: jnp.dot(a, w[layer], preferred_element_type=jnp.float32)
            query = dot(hidden, w_query).astype(jnp.bfloat16).reshape(2, seq_dev, heads, head_dim)
            k_new = dot(hidden, w_key).astype(jnp.bfloat16).reshape(2, seq_dev, kv_heads, head_dim)
            v_new = dot(hidden, w_value).astype(jnp.bfloat16).reshape(2, seq_dev, kv_heads, head_dim)
            per_seq = lambda t: jnp.swapaxes(t, 0, 1).reshape(seq_dev, -1, head_dim)
            qkv = jnp.concatenate([per_seq(query), per_seq(k_new), per_seq(v_new)], axis=1)
            qkv = gather_rows(qkv, 'kv', n_cols, 0).reshape(row_seqs, -1, head_dim)
            dims = dict(layer=layer, n_slots=n_slots, layers=layers, page=page, kvh=kv_heads, q_group=q_group, hd=head_dim)
            *pools, acc, ml = attend(info, counts, qkv, [k_rows, v_rows], pools, None, part=0, **dims)
            if layer == 0:
                next_hops = pick(z_list, units[1], [Z_CORE] * (n_rows - 1))
                got, acc, next_hops = lax.optimization_barrier((got, acc, next_hops))
                next_got = along_z(next_hops)
                all_units, hop = to_y(units[0], got)
            all_units = along_y(all_units, hop)
            *pools, acc, ml = attend(info, counts, qkv, all_units + [all_pages(layer)], pools, (acc, ml), part=1, **dims)
            o = combine(acc, ml, 'kv', n_cols, 1)
            if layer + 1 < layers:
                next_got, o = lax.optimization_barrier((next_got, o))
                all_units, hop = to_y(units[1], next_got)
            attn_out = jnp.swapaxes(o.reshape(seq_dev, 2, heads * head_dim), 0, 1).reshape(2 * seq_dev, heads * head_dim)
            hidden = mlp_pair(attn_out, hidden, w_out, w_up, w_down, layer, 3 + layer)
        k_out, v_out = (p.reshape(k_pool.shape) for p in pools)
        return hidden.reshape(2, seq_dev, width), k_out, v_out

    return jax.shard_map(per_device, mesh=mesh, in_specs=(seq_spec, full_spec, full_spec, full_spec, full_spec, full_spec, full_spec, pool_spec, pool_spec, table_spec, vec_spec, vec_spec, vec_spec), out_specs=(seq_spec, pool_spec, pool_spec), check_vma=False)
```

```python
import functools

import jax
import jax.numpy as jnp
from jax import lax
from jax.experimental import pallas as pl
from jax.experimental.pallas import tpu as pltpu
from jax.sharding import PartitionSpec as P


MESH_ID = pl.DeviceIdType.MESH
NEG = -1e30
UNROLL = 4
Z_CORE = 6
Y_CORE = 10


def uninit(shape, dtype):
    def body(o_ref):
        pass

    return pl.pallas_call(
        body, out_shape=jax.ShapeDtypeStruct(shape, dtype), out_specs=pl.BlockSpec(memory_space=pl.ANY), name="uninit")()


def take_pages(rows, k_rows, v_rows, layers):
    m = rows.shape[0]
    prow, hd = k_rows.shape[1:]

    def body(rows_ref, k_in, v_in, *rest):
        outs, (buf, isem, osem) = rest[:layers], rest[layers:]
        ins, puts = [], []
        for layer in range(layers):
            for i in range(m):
                for which, ref in enumerate((k_in, v_in)):
                    cp = pltpu.make_async_copy(
                        ref.at[rows_ref[i] + layer], buf.at[layer, i, pl.ds(which * prow, prow)], isem.at[layer, 2 * i + which])
                    cp.start()
                    ins.append(cp)
        for layer in range(layers):
            for cp in ins[layer * 2 * m:(layer + 1) * 2 * m]:
                cp.wait()
            cp = pltpu.make_async_copy(buf.at[layer], outs[layer], osem.at[layer])
            cp.start()
            puts.append(cp)
        for cp in puts:
            cp.wait()

    any_spec = pl.BlockSpec(memory_space=pl.ANY)
    return pl.pallas_call(
        body,
        out_shape=[jax.ShapeDtypeStruct((m, 2 * prow, hd), k_rows.dtype)] * layers,
        in_specs=[pl.BlockSpec(memory_space=pltpu.SMEM), any_spec, any_spec],
        out_specs=[any_spec] * layers,
        scratch_shapes=[pltpu.VMEM((layers, m, 2 * prow, hd), k_rows.dtype),
                        pltpu.SemaphoreType.DMA((layers, 2 * m)), pltpu.SemaphoreType.DMA((layers,))],
        cost_estimate=pl.CostEstimate(flops=100_000_000, bytes_accessed=12_000_000, transcendentals=0),
        name="take_pages",
    )(rows, k_rows, v_rows)


def pick(lists, sources, splits):
    n = sum(splits)
    tail, dtype = sources[0].shape[1:], sources[0].dtype

    def body(idx_ref, *rest):
        ins, outs, (buf, isem, osem) = rest[:len(sources)], rest[len(sources):-3], rest[-3:]

        @pl.loop(0, n)
        def _(i):
            at, lo = idx_ref[i], 0
            for ref in ins:
                hi = lo + ref.shape[0]

                @pl.when((at >= lo) & (at < hi))
                def _():
                    pltpu.make_async_copy(ref.at[at - lo], buf.at[i], isem.at[i]).start()

                lo = hi

        @pl.loop(0, n)
        def _(i):
            pltpu.make_async_copy(ins[0].at[0], buf.at[i], isem.at[i]).wait()

        puts, lo = [], 0
        for j, size in enumerate(splits):
            cp = pltpu.make_async_copy(buf.at[pl.ds(lo, size)], outs[j], osem.at[j])
            cp.start()
            puts.append(cp)
            lo += size
        for cp in puts:
            cp.wait()

    any_spec = pl.BlockSpec(memory_space=pl.ANY)
    return pl.pallas_call(
        body,
        out_shape=[jax.ShapeDtypeStruct((size,) + tail, dtype) for size in splits],
        in_specs=[pl.BlockSpec(memory_space=pltpu.SMEM)] + [any_spec] * len(sources),
        out_specs=[any_spec] * len(splits),
        scratch_shapes=[pltpu.VMEM((n,) + tail, dtype), pltpu.SemaphoreType.DMA((n,)), pltpu.SemaphoreType.DMA((len(splits),))],
        cost_estimate=pl.CostEstimate(flops=100_000_000, bytes_accessed=5_000_000, transcendentals=0),
    )(lists, *sources)


def share_plan(x, mesh_shape, cid):
    nx, ny, nz = mesh_shape
    n = nx * ny * nz

    def body(x_ref, o_ref, send_sem, recv_sem):
        me = (lax.axis_index('rep') * ny + lax.axis_index('kv2')) * nz + lax.axis_index('kv')

        def coords(d):
            p = lax.rem(me + d, n)
            return (p // (ny * nz), lax.rem(p // nz, ny), lax.rem(p, nz))

        barrier = pltpu.get_barrier_semaphore()
        for d in range(1, n):
            pl.semaphore_signal(barrier, inc=1, device_id=coords(d), device_id_type=MESH_ID)
        pl.semaphore_wait(barrier, n - 1)
        copies = []
        for d in range(1, n):
            cp = pltpu.make_async_remote_copy(
                src_ref=x_ref, dst_ref=o_ref.at[me], send_sem=send_sem.at[d], recv_sem=recv_sem.at[d],
                device_id=coords(d), device_id_type=MESH_ID)
            cp.start()
            copies.append(cp)
        o_ref[me] = x_ref[...]
        for cp in copies:
            cp.wait()

    return pl.pallas_call(
        body,
        out_shape=jax.ShapeDtypeStruct((n,) + x.shape, x.dtype),
        in_specs=[pl.BlockSpec(memory_space=pltpu.VMEM)],
        out_specs=pl.BlockSpec(memory_space=pltpu.VMEM),
        scratch_shapes=[pltpu.SemaphoreType.DMA((n,)), pltpu.SemaphoreType.DMA((n,))],
        compiler_params=pltpu.CompilerParams(collective_id=cid, has_side_effects=True),
        name="share_plan",
    )(x)


def route_z(own, pair, pos):
    n_mig = own.shape[0]

    def body(own_ref, pair_ref, pos_ref, z_ref, cnt):
        row, core = pos_ref[0], pos_ref[1] & 1

        @pl.loop(0, 3 * Z_CORE)
        def _(i):
            z_ref[i] = 0

        for i in range(4):
            cnt[i] = 0

        @pl.loop(0, 2 * n_mig)
        def _(i):
            second = (i >= n_mig).astype(jnp.int32)
            e = i - second * n_mig
            mine = second == core
            dd = jnp.where(mine, own_ref[e], pair_ref[e])
            di = dd >> 2
            k = cnt[di]
            cnt[di] = k + 1
            shift = (di - row) & 3

            @pl.when((shift != 0) & ((k & 1) == core) & (k < 2 * Z_CORE))
            def _():
                z_ref[(shift - 1) * Z_CORE + (k >> 1)] = jnp.where(mine, e, n_mig + e)

    smem = pl.BlockSpec(memory_space=pltpu.SMEM)
    return pl.pallas_call(
        body,
        out_shape=jax.ShapeDtypeStruct((64,), jnp.int32),
        in_specs=[smem] * 3,
        out_specs=smem,
        scratch_shapes=[pltpu.SMEM((4,), jnp.int32)],
        name="route_z",
    )(own, pair, pos)


def route(dst, dev, pos, n_mig, n_slots):
    n_dev = dev.shape[0] // n_mig
    z_at, y_at = 2 * n_mig, 2 * n_mig + 2 * 3 * Z_CORE

    def body(dst_ref, dev_ref, pos_ref, y_ref, s_ref, cnt, cnt2):
        row, colm = pos_ref[0], pos_ref[1]
        half, core = colm >> 1, colm & 1
        me = row * 4 + colm

        @pl.loop(0, 64)
        def _(i):
            y_ref[i] = 0
            s_ref[i] = -1
            cnt[i] = 0

        @pl.loop(0, 8)
        def _(i):
            cnt2[i] = 0

        @pl.loop(0, n_dev)
        def _(d):
            si, sy, sc = d >> 2, (d >> 1) & 1, d & 1

            @pl.loop(0, n_mig)
            def _(e):
                dd = dev_ref[d * n_mig + e]
                di, dy = dd >> 2, (dd >> 1) & 1
                c1 = (d >> 1) * 4 + di
                k = cnt[c1]
                cnt[c1] = k + 1
                cross = (dy != sy).astype(jnp.int32)
                c2 = di * 2 + sy
                k2 = cnt2[c2]
                cnt2[c2] = k2 + cross

                @pl.when(di == row)
                def _():
                    shift = (di - si) & 3
                    at = jnp.where(sc == core, e, n_mig + e)
                    z_slot = (shift - 1) * Z_CORE + (k >> 1)
                    here = jnp.where(shift == 0, at, z_at + z_slot + jnp.where((k & 1) == core, 0, 3 * Z_CORE))

                    @pl.when((sy == half) & (cross == 1) & ((k2 & 1) == core) & (k2 < 2 * Y_CORE))
                    def _():
                        y_ref[k2 >> 1] = jnp.minimum(here, y_at - 1)

                    @pl.when(dd == me)
                    def _():
                        by_y = y_at + (k2 >> 1) + jnp.where((k2 & 1) == core, 0, Y_CORE)
                        s_ref[dst_ref[d * n_mig + e] - me * n_slots] = jnp.where(cross == 1, by_y, here)

    smem = pl.BlockSpec(memory_space=pltpu.SMEM)
    return pl.pallas_call(
        body,
        out_shape=[jax.ShapeDtypeStruct((64,), jnp.int32)] * 2,
        in_specs=[smem] * 3,
        out_specs=[smem] * 2,
        scratch_shapes=[pltpu.SMEM((64,), jnp.int32), pltpu.SMEM((8,), jnp.int32)],
        cost_estimate=pl.CostEstimate(flops=100_000_000, bytes_accessed=1_000_000, transcendentals=0),
        name="route",
    )(dst, dev, pos)


def enter(axis, n, me):
    barrier = pltpu.get_barrier_semaphore()
    for d in range(1, n):
        pl.semaphore_signal(barrier, inc=1, device_id={axis: lax.rem(me + d, n)}, device_id_type=MESH_ID)
    pl.semaphore_wait(barrier, n - 1)


def gather_rows(x, axis, n, cid):
    def body(x_ref, o_ref, send_sem, recv_sem):
        me = lax.axis_index(axis)
        enter(axis, n, me)
        copies = []
        for d in range(1, n):
            cp = pltpu.make_async_remote_copy(
                src_ref=x_ref, dst_ref=o_ref.at[me], send_sem=send_sem.at[d], recv_sem=recv_sem.at[d],
                device_id={axis: lax.rem(me + d, n)}, device_id_type=MESH_ID)
            cp.start()
            copies.append(cp)
        o_ref[me] = x_ref[...]
        for cp in copies:
            cp.wait()

    return pl.pallas_call(
        body,
        out_shape=jax.ShapeDtypeStruct((n,) + x.shape, x.dtype),
        in_specs=[pl.BlockSpec(memory_space=pltpu.VMEM)],
        out_specs=pl.BlockSpec(memory_space=pltpu.VMEM),
        scratch_shapes=[pltpu.SemaphoreType.DMA((n,)), pltpu.SemaphoreType.DMA((n,))],
        compiler_params=pltpu.CompilerParams(collective_id=cid, has_side_effects=True),
        name="gather_rows",
    )(x)


def combine(acc, ml, axis, n, cid):
    rows, r, hd = acc.shape
    b = rows // n

    def body(acc_ref, ml_ref, o_ref, acc_in, ml_in, send_sem, recv_sem, send_ml, recv_ml):
        me = lax.axis_index(axis)
        enter(axis, n, me)
        copies = []
        for d in range(1, n):
            peer = lax.rem(me + d, n)
            for src, dst, ss, rs in (
                (acc_ref.at[pl.ds(peer * b, b)], acc_in.at[d], send_sem, recv_sem),
                (ml_ref, ml_in.at[d], send_ml, recv_ml),
            ):
                cp = pltpu.make_async_remote_copy(
                    src_ref=src, dst_ref=dst, send_sem=ss.at[d], recv_sem=rs.at[d],
                    device_id={axis: peer}, device_id_type=MESH_ID)
                cp.start()
                copies.append(cp)
        for cp in copies:
            cp.wait()
        lane = lax.broadcasted_iota(jnp.int32, (r, ml_ref.shape[2]), 1)
        for i in range(b):
            sel = lane == me * b + i
            pick = lambda t: jnp.sum(jnp.where(sel, t, 0.0), axis=1, keepdims=True)
            ms = [pick(ml_ref[0])] + [pick(ml_in[d, 0]) for d in range(1, n)]
            ls = [pick(ml_ref[1])] + [pick(ml_in[d, 1]) for d in range(1, n)]
            top = functools.reduce(jnp.maximum, ms)
            ws = [jnp.exp(m - top) for m in ms]
            den = sum(w * l for w, l in zip(ws, ls))
            num = ws[0] * acc_ref[me * b + i]
            for d in range(1, n):
                num += ws[d] * acc_in[d, i]
            o_ref[i] = (num / den).astype(o_ref.dtype)

    return pl.pallas_call(
        body,
        out_shape=jax.ShapeDtypeStruct((b, r, hd), jnp.bfloat16),
        in_specs=[pl.BlockSpec(memory_space=pltpu.VMEM)] * 2,
        out_specs=pl.BlockSpec(memory_space=pltpu.VMEM),
        scratch_shapes=[
            pltpu.VMEM((n, b, r, hd), jnp.float32),
            pltpu.VMEM((n,) + ml.shape, jnp.float32),
            pltpu.SemaphoreType.DMA((n,)), pltpu.SemaphoreType.DMA((n,)),
            pltpu.SemaphoreType.DMA((n,)), pltpu.SemaphoreType.DMA((n,)),
        ],
        compiler_params=pltpu.CompilerParams(collective_id=cid, has_side_effects=True),
        name="combine",
    )(acc, ml)


def mlp_pair(attn, hidden, w_out, w_up, w_down, layer, cid):
    rows, d = attn.shape
    ff = w_up.shape[2]
    r = -(-rows // 32) * 32
    tile = 512
    d_half, f_half = d // 2, ff // 2
    n_o, n_f = d_half // tile, f_half // tile
    ring_c, ring_r = min(8, n_o + n_f), min(6, n_f)
    attn, hidden = (jnp.pad(t, ((0, r - rows), (0, 0))) for t in (attn, hidden))

    def body(attn_ref, hid_ref, wo_ref, wu_ref, wd_ref, o_ref, x_all, h_all, hm, act, acc, rx, wc, wr, csem, rsem, ssem, qsem):
        me = lax.axis_index('kv')
        core = lax.rem(me, 2)
        peer = me + 1 - 2 * core
        mine, other = pl.ds(core * r, r), pl.ds((1 - core) * r, r)

        def col(c, is_out):
            if is_out:
                src = wo_ref.at[layer, :, pl.ds(pl.multiple_of(core * d_half + c * tile, tile), tile)]
            else:
                src = wu_ref.at[layer, :, pl.ds(pl.multiple_of(core * f_half + (c - n_o) * tile, tile), tile)]
            slot = lax.rem(c, ring_c)
            return pltpu.make_async_copy(src, wc.at[slot], csem.at[slot])

        def row(j):
            slot = lax.rem(j, ring_r)
            src = wd_ref.at[layer, pl.ds(pl.multiple_of(core * f_half + j * tile, tile), tile), :]
            return pltpu.make_async_copy(src, wr.at[slot], rsem.at[slot])

        for c in range(ring_c):
            col(c, c < n_o).start()

        barrier = pltpu.get_barrier_semaphore()
        pl.semaphore_signal(barrier, inc=1, device_id={'kv': peer}, device_id_type=MESH_ID)
        pl.semaphore_wait(barrier, 1)

        def send(src, dst, i):
            return pltpu.make_async_remote_copy(
                src_ref=src, dst_ref=dst, send_sem=ssem.at[i], recv_sem=qsem.at[i],
                device_id={'kv': peer}, device_id_type=MESH_ID)

        swaps = [send(attn_ref, x_all.at[mine], 0), send(hid_ref, h_all.at[mine], 1)]
        for cp in swaps:
            cp.start()
        x_all[mine] = attn_ref[...]
        h_all[mine] = hid_ref[...]
        for cp in swaps:
            cp.wait()

        @pl.loop(0, n_o)
        def _(c):
            col(c, True).wait()
            at = pl.ds(pl.multiple_of(core * d_half + c * tile, tile), tile)
            part = jnp.dot(x_all[...], wc[lax.rem(c, ring_c)], preferred_element_type=jnp.float32)
            hm[:, at] = (h_all[:, at].astype(jnp.float32) + part).astype(jnp.bfloat16)

            @pl.when(c + ring_c < n_o + n_f)
            def _():
                col(c + ring_c, False).start()

        own_cols = pl.ds(pl.multiple_of(core * d_half, tile), d_half)
        cp = send(hm.at[:, own_cols], hm.at[:, own_cols], 2)
        cp.start()
        acc[...] = jnp.zeros_like(acc)
        cp.wait()

        @pl.loop(0, n_f)
        def _(j):
            c = j + n_o
            col(c, False).wait()
            up = jnp.dot(hm[...], wc[lax.rem(c, ring_c)], preferred_element_type=jnp.float32)
            act[:, pl.ds(pl.multiple_of(j * tile, tile), tile)] = jax.nn.gelu(up).astype(jnp.bfloat16)

            @pl.when(c + ring_c < n_o + n_f)
            def _():
                col(c + ring_c, False).start()

            @pl.when(j < ring_r)
            def _():
                row(j).start()

        @pl.loop(0, n_f)
        def _(j):
            row(j).wait()
            acc[...] += jnp.dot(act[:, pl.ds(pl.multiple_of(j * tile, tile), tile)], wr[lax.rem(j, ring_r)],
                                preferred_element_type=jnp.float32)

            @pl.when(j + ring_r < n_f)
            def _():
                row(j + ring_r).start()

        cp = send(acc.at[other], rx, 3)
        cp.start()
        cp.wait()
        o_ref[...] = (hm[mine].astype(jnp.float32) + (acc[mine] + rx[...])).astype(o_ref.dtype)

    vmem, any_spec = pl.BlockSpec(memory_space=pltpu.VMEM), pl.BlockSpec(memory_space=pl.ANY)
    out = pl.pallas_call(
        body,
        out_shape=jax.ShapeDtypeStruct((r, d), jnp.bfloat16),
        in_specs=[vmem, vmem, any_spec, any_spec, any_spec],
        out_specs=vmem,
        scratch_shapes=[
            pltpu.VMEM((2 * r, d), jnp.bfloat16), pltpu.VMEM((2 * r, d), jnp.bfloat16), pltpu.VMEM((2 * r, d), jnp.bfloat16),
            pltpu.VMEM((2 * r, f_half), jnp.bfloat16), pltpu.VMEM((2 * r, d), jnp.float32), pltpu.VMEM((r, d), jnp.float32),
            pltpu.VMEM((ring_c, d, tile), jnp.bfloat16), pltpu.VMEM((ring_r, tile, d), jnp.bfloat16),
            pltpu.SemaphoreType.DMA((ring_c,)), pltpu.SemaphoreType.DMA((ring_r,)),
            pltpu.SemaphoreType.DMA((4,)), pltpu.SemaphoreType.DMA((4,)),
        ],
        compiler_params=pltpu.CompilerParams(collective_id=cid, has_side_effects=True, vmem_limit_bytes=58 * 1024 * 1024),
        cost_estimate=pl.CostEstimate(flops=6_000_000_000, bytes_accessed=60_000_000, transcendentals=0),
    )(attn, hidden, w_out, w_up, w_down)
    return out[:rows]


def attend(info, counts, qkv, pools_in, unit_srcs, first_unit, prev_pools, state, layer, part, n_slots, layers, page, kvh, q_group, hd):
    sources = list(pools_in) + list(unit_srcs)
    n_pool = len(pools_in)
    prow = page * kvh
    qr = 2 * kvh * q_group
    n_seq = qkv.shape[0]
    scale = hd ** -0.5
    aliased = prev_pools is not None
    carried = state is not None

    def body(info_ref, cnt_ref, qkv_ref, *rest):
        ins, rest = rest[:len(sources)], rest[len(sources):]
        if aliased:
            rest = rest[2:]
        if carried:
            acc_prev, ml_prev = rest[:2]
            rest = rest[2:]
        k_out, v_out, acc_ref, ml_ref, kbuf, vbuf, isem, osem = rest
        lo = cnt_ref[2 * part - 1] if part else 0
        mid = cnt_ref[2 * part]
        hi = cnt_ref[2 * part + 1]

        def load_from(k_page, v_page, i):
            return (pltpu.make_async_copy(k_page, kbuf.at[i], isem.at[0, i]),
                    pltpu.make_async_copy(v_page, vbuf.at[i], isem.at[1, i]))

        def from_pool(i):
            at = info_ref[0, i] * layers + layer
            return load_from(ins[0].at[at], ins[1].at[at], i)

        def loads(i):
            if n_pool:
                return from_pool(i)
            return load_from(ins[0].at[0, pl.ds(0, prow)], ins[0].at[0, pl.ds(prow, prow)], i)

        def start_loads(i):
            at, first = info_ref[3, i], first_unit
            if n_pool and unit_srcs:
                pl.when(at < 0)(lambda: [cp.start() for cp in from_pool(i)] and None)
            elif n_pool:
                for cp in from_pool(i):
                    cp.start()
            for ref in ins[n_pool:]:
                last = first + ref.shape[0]

                @pl.when((at >= first) & (at < last))
                def _():
                    u = at - first
                    for cp in load_from(ref.at[u, pl.ds(0, prow)], ref.at[u, pl.ds(prow, prow)], i):
                        cp.start()

                first = last

        def stores(i):
            slot = info_ref[0, i]
            return (pltpu.make_async_copy(kbuf.at[i], k_out.at[slot * layers + layer], osem.at[0, i]),
                    pltpu.make_async_copy(vbuf.at[i], v_out.at[slot * layers + layer], osem.at[1, i]))

        @pl.loop(lo, hi)
        def _(i):
            start_loads(i)

        if carried:
            acc_ref[...] = acc_prev[...]
            ml_ref[...] = ml_prev[...]
        else:
            acc_ref[...] = jnp.zeros_like(acc_ref)
            ml_ref[0] = jnp.full(ml_ref.shape[1:], NEG, jnp.float32)
            ml_ref[1] = jnp.zeros(ml_ref.shape[1:], jnp.float32)

        col = lax.broadcasted_iota(jnp.int32, (qr, prow), 1)
        row = lax.broadcasted_iota(jnp.int32, (qr, prow), 0)
        late = (row >= kvh * q_group).astype(jnp.int32)
        head_ok = lax.rem(col, kvh) == (row - late * (kvh * q_group)) // q_group
        need = col // kvh - late
        need = jnp.where(head_ok, need, 1 << 20)
        lane = lax.broadcasted_iota(jnp.int32, ml_ref.shape[1:], 1)
        wrow = lax.broadcasted_iota(jnp.int32, (4 * kvh, hd), 0) // kvh

        @pl.loop(0, (mid - lo + UNROLL - 1) // UNROLL)
        def _(g):
            base = lo + g * UNROLL
            idx, seqs, offs = [], [], []
            for u in range(UNROLL):
                i = base + u
                live = i < mid
                j = jnp.minimum(i, mid - 1)
                idx.append(j)
                seqs.append(jnp.where(live, info_ref[1, j], n_seq))
                offs.append(info_ref[2, j])

                @pl.when(live)
                def _():
                    for cp in loads(j):
                        cp.wait()

                    @pl.when(info_ref[2, j] < page)
                    def _():
                        off = info_ref[2, j]
                        w = jnp.minimum(off // 2, page // 2 - 2)
                        at = pl.ds(pl.multiple_of(w * (2 * kvh), 2 * kvh), 4 * kvh)
                        for buf, r0 in ((kbuf, qr), (vbuf, qr + 2 * kvh)):
                            new = qkv_ref[info_ref[1, j], r0:r0 + 2 * kvh, :].astype(jnp.float32)
                            first = jnp.concatenate([new[:kvh]] * 4, axis=0)
                            second = jnp.concatenate([new[kvh:]] * 4, axis=0)
                            old = buf[j, at, :].astype(jnp.float32)
                            tok = wrow + 2 * w
                            old = jnp.where(tok == off, first, jnp.where(tok == off + 1, second, old))
                            buf[j, at, :] = old.astype(jnp.bfloat16)

            res = []
            for u in range(UNROLL):
                q = qkv_ref[jnp.minimum(seqs[u], n_seq - 1), :qr, :]
                s = lax.dot_general(q, kbuf[idx[u]], (((1,), (1,)), ((), ())), preferred_element_type=jnp.float32) * scale
                s = jnp.where(need <= offs[u], s, NEG)
                m = jnp.max(s, axis=1, keepdims=True)
                p = jnp.exp(s - m)
                l = jnp.sum(p, axis=1, keepdims=True)
                o = jnp.dot(p.astype(jnp.bfloat16), vbuf[idx[u]], preferred_element_type=jnp.float32)
                res.append((m, l, o))
            for u in range(UNROLL):
                m, l, o = res[u]
                sel = lane == seqs[u]
                m_all, l_all = ml_ref[0], ml_ref[1]
                m_old = jnp.max(jnp.where(sel, m_all, NEG), axis=1, keepdims=True)
                m_new = jnp.maximum(m_old, m)
                alpha = jnp.exp(m_old - m_new)
                beta = jnp.exp(m - m_new)
                acc_ref[seqs[u]] = acc_ref[seqs[u]] * alpha + o * beta
                ml_ref[0] = jnp.where(sel, m_new, m_all)
                ml_ref[1] = jnp.where(sel, l_all * alpha + l * beta, l_all)
            for u in range(UNROLL):
                @pl.when(base + u < mid)
                def _():
                    for cp in stores(base + u):
                        cp.start()

        @pl.loop(mid, hi)
        def _(i):
            for cp in loads(i):
                cp.wait()
            for cp in stores(i):
                cp.start()

        @pl.loop(lo, hi)
        def _(i):
            for cp in stores(i):
                cp.wait()

    any_spec = pl.BlockSpec(memory_space=pl.ANY)
    vmem = pl.BlockSpec(memory_space=pltpu.VMEM)
    smem = pl.BlockSpec(memory_space=pltpu.SMEM)
    operands = [info, counts, qkv, *sources]
    specs = [smem, smem, vmem] + [any_spec] * len(sources)
    alias = {}
    if aliased:
        alias = {len(operands): 0, len(operands) + 1: 1}
        operands += list(prev_pools)
        specs += [any_spec, any_spec]
    if carried:
        operands += list(state)
        specs += [vmem, vmem]
    pool = jax.ShapeDtypeStruct((n_slots * layers, prow, hd), jnp.bfloat16)
    return pl.pallas_call(
        body,
        out_shape=[pool, pool,
                   jax.ShapeDtypeStruct((n_seq + 1, qr, hd), jnp.float32),
                   jax.ShapeDtypeStruct((2, qr, 128), jnp.float32)],
        in_specs=specs,
        out_specs=[any_spec, any_spec, vmem, vmem],
        scratch_shapes=[
            pltpu.VMEM((n_slots, prow, hd), jnp.bfloat16),
            pltpu.VMEM((n_slots, prow, hd), jnp.bfloat16),
            pltpu.SemaphoreType.DMA((2, n_slots)),
            pltpu.SemaphoreType.DMA((2, n_slots)),
        ],
        input_output_aliases=alias,
        cost_estimate=pl.CostEstimate(flops=400_000_000, bytes_accessed=16_000_000, transcendentals=0),
    )(*operands)


def solution(mesh):
    n_rows = mesh.shape['kv2']
    n_cols = mesh.shape['kv']
    dev_axes = ('rep', 'kv2', 'kv')
    seq_spec = P(None, dev_axes, None)
    pool_spec = P(dev_axes, None, None, None, None)
    table_spec = P(dev_axes, None)
    vec_spec = P(dev_axes)
    full_spec = P()

    def per_device(x_embed, w_query, w_key, w_value, w_out, w_up, w_down, k_pool, v_pool, old_table, seq_len, src_slot, dst_slot):
        n_slots, layers, page, kv_heads, head_dim = k_pool.shape
        heads = w_query.shape[2] // head_dim
        q_group = heads // kv_heads
        seq_dev = x_embed.shape[1]
        n_pages = old_table.shape[1]
        n_mig = src_slot.shape[0]
        n_dev = n_rows * n_cols
        row_seqs = seq_dev * n_cols
        prow = page * kv_heads
        width = x_embed.shape[2]
        me_row, me_col = lax.axis_index('kv2'), lax.axis_index('kv')
        me = me_row * n_cols + me_col
        base = me * n_slots

        k_rows = k_pool.reshape(n_slots * layers, prow, head_dim)
        v_rows = v_pool.reshape(n_slots * layers, prow, head_dim)
        pair = [(c, c ^ 1) for c in range(n_cols)]
        over = [(c, c ^ 2) for c in range(n_cols)]
        z_hops = [[(r, (r + s) % n_rows) for r in range(n_rows)] for s in range(1, n_rows)]
        pos = jnp.stack([me_row, me_col]).astype(jnp.int32)
        dev_own = dst_slot // n_slots
        leaving = take_pages((src_slot - base) * layers, k_rows, v_rows, layers)
        units = [[leaving[0], lax.ppermute(leaving[0], 'kv', pair)]]
        dev_pair = lax.ppermute(dev_own, 'kv', pair)

        n_rep = mesh.shape['rep']
        words = [src_slot, dst_slot, dst_slot // n_slots, old_table.reshape(-1), seq_len]
        cuts = [0]
        for w in words:
            cuts.append(cuts[-1] + w.shape[0])
        meta = jnp.pad(jnp.concatenate(words), (0, 128 - cuts[-1])).reshape(1, 128)
        meta_all = share_plan(meta, (n_rep, n_rows, n_cols), 2).reshape(n_rep, n_dev, 128)

        meta_all, pos = lax.optimization_barrier((meta_all, pos))
        z_list = route_z(dev_own, dev_pair, pos)
        hops = pick(z_list, units[0], [Z_CORE] * (n_rows - 1))
        hops, z_list, hidden, meta_all, later = lax.optimization_barrier(
            (hops, z_list, x_embed.reshape(2 * seq_dev, width), meta_all, leaving[1:]))
        units += [[own, lax.ppermute(own, 'kv', pair)] for own in later]

        meta = lax.dynamic_index_in_dim(meta_all, lax.axis_index('rep'), 0, keepdims=False)
        src_all, dst_all, dev_all = (meta[:, cuts[t]:cuts[t + 1]].reshape(-1) for t in range(3))
        row_meta = lax.dynamic_slice_in_dim(meta, me_row * n_cols, n_cols, axis=0)
        row_table = row_meta[:, cuts[3]:cuts[4]].reshape(-1)
        row_len = row_meta[:, cuts[4]:cuts[5]].reshape(-1)

        dev_by = meta_all[:, :, cuts[2]:cuts[3]]
        to_row = dev_by // n_cols
        rows4 = jnp.arange(n_rows, dtype=jnp.int32)
        goes = (to_row[..., None] == rows4).astype(jnp.int32).sum(axis=2)
        per_chip = goes.reshape(n_rep, n_rows, n_cols // 2, 2, n_rows).sum(axis=3)
        leaves = rows4[:, None] != rows4[None, :]
        z_full = ((per_chip > 2 * Z_CORE) & leaves[None, :, None, :]).any()
        side = (jnp.arange(n_dev, dtype=jnp.int32) // 2 % 2)[None, :, None]
        crosses = dev_by // 2 % 2 != side
        per_side = ((to_row[..., None] == rows4) & crosses[..., None]).astype(jnp.int32).sum(axis=2)
        y_full = (per_side.reshape(n_rep, n_rows, n_cols // 2, 2, n_rows).sum(axis=(1, 3)) > 2 * Y_CORE).any()
        full = z_full | y_full

        y_list, unit_of = route(dst_all, dev_all, pos, n_mig, n_slots)

        def along_z(hops):
            got = []
            for h, z in zip(hops, z_hops):
                got.append(lax.ppermute(h, 'kv2', z))
            return got

        def swap(units, got):
            return units + got + [lax.ppermute(g, 'kv', pair) for g in got]

        def along_y(hop):
            got = lax.ppermute(hop, 'kv', over)
            return [got, lax.ppermute(got, 'kv', pair)]

        same = row_table[:, None] == src_all[None, :]
        new_table = jnp.where(same.any(axis=1), jnp.sum(jnp.where(same, dst_all[None, :], 0), axis=1), row_table)
        slots = jnp.arange(n_slots, dtype=jnp.int32)
        cells = jnp.arange(row_seqs * n_pages, dtype=jnp.int32)
        slot_cell = jnp.max(jnp.where(new_table[None, :] == (slots + base)[:, None], cells[None, :], -1), axis=1)
        moves = jnp.arange(n_dev * n_mig, dtype=jnp.int32)
        move_of = jnp.max(jnp.where(dst_all[None, :] == (slots + base)[:, None], moves[None, :], -1), axis=1)
        is_mig = move_of >= 0
        used = slot_cell >= 0
        seq_of = jnp.where(used, slot_cell // n_pages, row_seqs)
        seq_one = seq_of[:, None] == jnp.arange(row_seqs, dtype=jnp.int32)[None, :]
        len_of = jnp.sum(jnp.where(seq_one, row_len[None, :], 0), axis=1)
        off_of = len_of - (slot_cell % n_pages) * page
        off_of = jnp.where(used & (off_of >= 0) & (off_of < page), off_of, 2 * page)
        y_at = 2 * n_mig + 2 * (n_rows - 1) * Z_CORE
        unit = jnp.where(is_mig, jnp.where(full, slots + y_at + 2 * Y_CORE, unit_of[:n_slots]), -1)

        def lists(cls, n_cls):
            key = cls * 2 + (~used).astype(jnp.int32)
            order = key * n_slots + slots
            at = jnp.sum((order[None, :] < order[:, None]).astype(jnp.int32), axis=1)
            place = at[None, :] == jnp.arange(64, dtype=jnp.int32)[:, None]
            info = jnp.stack([jnp.sum(jnp.where(place, t[None, :], 0), axis=1) for t in (slots, seq_of, off_of, unit)])
            counts = jnp.sum((key[None, :] <= jnp.arange(2 * n_cls, dtype=jnp.int32)[:, None]).astype(jnp.int32), axis=1)
            return info, counts

        by_class = lists(is_mig.astype(jnp.int32) + (unit >= y_at).astype(jnp.int32), 3)
        by_use = lists(jnp.zeros_like(slots), 1)

        def all_pages(layer):
            def collect():
                every = lax.all_gather(leaving[layer], ('kv2', 'kv'), tiled=True)
                return pick(jnp.maximum(move_of, 0), [every], [n_slots])[0]

            return lax.cond(full, collect, lambda: uninit((n_slots, 2 * prow, head_dim), jnp.bfloat16))

        pools = None
        got = along_z(hops)
        for layer in range(layers):
            dot = lambda a, w: jnp.dot(a, w[layer], preferred_element_type=jnp.float32)
            query = dot(hidden, w_query).astype(jnp.bfloat16).reshape(2, seq_dev, heads, head_dim)
            k_new = dot(hidden, w_key).astype(jnp.bfloat16).reshape(2, seq_dev, kv_heads, head_dim)
            v_new = dot(hidden, w_value).astype(jnp.bfloat16).reshape(2, seq_dev, kv_heads, head_dim)
            per_seq = lambda t: jnp.swapaxes(t, 0, 1).reshape(seq_dev, -1, head_dim)
            qkv = jnp.concatenate([per_seq(query), per_seq(k_new), per_seq(v_new)], axis=1)
            qkv = gather_rows(qkv, 'kv', n_cols, 0).reshape(row_seqs, -1, head_dim)
            dims = dict(layer=layer, n_slots=n_slots, layers=layers, page=page, kvh=kv_heads, q_group=q_group, hd=head_dim)
            if layer == 0:
                *pools, acc, ml = attend(*by_class, qkv, [k_rows, v_rows], [], 0, pools, None, part=0, **dims)
                next_hops = pick(z_list, units[1], [Z_CORE] * (n_rows - 1))
                got, acc, next_hops = lax.optimization_barrier((got, acc, next_hops))
                next_got = along_z(next_hops)
                all_units = swap(units[0], got)
                hop, = pick(y_list, all_units, [Y_CORE])
                last = along_y(hop) + [all_pages(0)]
                *pools, acc, ml = attend(*by_class, qkv, [], all_units, 0, pools, (acc, ml), part=1, **dims)
                *pools, acc, ml = attend(*by_class, qkv, [], last, y_at, pools, (acc, ml), part=2, **dims)
            else:
                srcs = all_units + along_y(hop) + [all_pages(layer)]
                *pools, acc, ml = attend(*by_use, qkv, [k_rows, v_rows], srcs, 0, pools, None, part=0, **dims)
            o = combine(acc, ml, 'kv', n_cols, 1)
            if layer + 1 < layers:
                next_got, o = lax.optimization_barrier((next_got, o))
                all_units = swap(units[layer + 1], next_got)
                hop, = pick(y_list, all_units, [Y_CORE])
                hop, o = lax.optimization_barrier((hop, o))
            attn_out = jnp.swapaxes(o.reshape(seq_dev, 2, heads * head_dim), 0, 1).reshape(2 * seq_dev, heads * head_dim)
            hidden = mlp_pair(attn_out, hidden, w_out, w_up, w_down, layer, 3 + layer)
        k_out, v_out = (p.reshape(k_pool.shape) for p in pools)
        return hidden.reshape(2, seq_dev, width), k_out, v_out

    return jax.shard_map(per_device, mesh=mesh, in_specs=(seq_spec, full_spec, full_spec, full_spec, full_spec, full_spec, full_spec, pool_spec, pool_spec, table_spec, vec_spec, vec_spec, vec_spec), out_specs=(seq_spec, pool_spec, pool_spec), check_vma=False)
```

```python
import jax
import jax.numpy as jnp
from jax import lax
from jax.experimental import pallas as pl
from jax.experimental.pallas import tpu as pltpu
from jax.sharding import PartitionSpec as P


MESH_ID = pl.DeviceIdType.MESH
NEG = -1e30
UNROLL = 4
Z_CORE = 6
Y_CORE = 10


def uninit(shape, dtype):
    def body(o_ref):
        pass

    return pl.pallas_call(
        body, out_shape=jax.ShapeDtypeStruct(shape, dtype), out_specs=pl.BlockSpec(memory_space=pl.ANY), name="uninit")()


def take_pages(rows, k_rows, v_rows, layers):
    m = rows.shape[0]
    prow, hd = k_rows.shape[1:]

    def body(rows_ref, k_in, v_in, *rest):
        outs, (buf, isem, osem) = rest[:layers], rest[layers:]
        ins, puts = [], []
        for layer in range(layers):
            for i in range(m):
                for which, ref in enumerate((k_in, v_in)):
                    cp = pltpu.make_async_copy(
                        ref.at[rows_ref[i] + layer], buf.at[layer, i, pl.ds(which * prow, prow)], isem.at[layer, 2 * i + which])
                    cp.start()
                    ins.append(cp)
        for layer in range(layers):
            for cp in ins[layer * 2 * m:(layer + 1) * 2 * m]:
                cp.wait()
            cp = pltpu.make_async_copy(buf.at[layer], outs[layer], osem.at[layer])
            cp.start()
            puts.append(cp)
        for cp in puts:
            cp.wait()

    any_spec = pl.BlockSpec(memory_space=pl.ANY)
    return pl.pallas_call(
        body,
        out_shape=[jax.ShapeDtypeStruct((m, 2 * prow, hd), k_rows.dtype)] * layers,
        in_specs=[pl.BlockSpec(memory_space=pltpu.SMEM), any_spec, any_spec],
        out_specs=[any_spec] * layers,
        scratch_shapes=[pltpu.VMEM((layers, m, 2 * prow, hd), k_rows.dtype),
                        pltpu.SemaphoreType.DMA((layers, 2 * m)), pltpu.SemaphoreType.DMA((layers,))],
        cost_estimate=pl.CostEstimate(flops=100_000_000, bytes_accessed=12_000_000, transcendentals=0),
        name="take_pages",
    )(rows, k_rows, v_rows)


def pick(lists, sources, splits):
    n = sum(splits)
    tail, dtype = sources[0].shape[1:], sources[0].dtype

    def body(idx_ref, *rest):
        ins, outs, (buf, isem, osem) = rest[:len(sources)], rest[len(sources):-3], rest[-3:]

        @pl.loop(0, n)
        def _(i):
            at, lo = idx_ref[i], 0
            for ref in ins:
                hi = lo + ref.shape[0]

                @pl.when((at >= lo) & (at < hi))
                def _():
                    pltpu.make_async_copy(ref.at[at - lo], buf.at[i], isem.at[i]).start()

                lo = hi

        @pl.loop(0, n)
        def _(i):
            pltpu.make_async_copy(ins[0].at[0], buf.at[i], isem.at[i]).wait()

        puts, lo = [], 0
        for j, size in enumerate(splits):
            cp = pltpu.make_async_copy(buf.at[pl.ds(lo, size)], outs[j], osem.at[j])
            cp.start()
            puts.append(cp)
            lo += size
        for cp in puts:
            cp.wait()

    any_spec = pl.BlockSpec(memory_space=pl.ANY)
    return pl.pallas_call(
        body,
        out_shape=[jax.ShapeDtypeStruct((size,) + tail, dtype) for size in splits],
        in_specs=[pl.BlockSpec(memory_space=pltpu.SMEM)] + [any_spec] * len(sources),
        out_specs=[any_spec] * len(splits),
        scratch_shapes=[pltpu.VMEM((n,) + tail, dtype), pltpu.SemaphoreType.DMA((n,)), pltpu.SemaphoreType.DMA((len(splits),))],
        cost_estimate=pl.CostEstimate(flops=100_000_000, bytes_accessed=5_000_000, transcendentals=0),
    )(lists, *sources)


def share_plan(x, mesh_shape, cid):
    nx, ny, nz = mesh_shape
    n = nx * ny * nz

    def body(x_ref, o_ref, send_sem, recv_sem):
        me = (lax.axis_index('rep') * ny + lax.axis_index('kv2')) * nz + lax.axis_index('kv')

        def coords(d):
            p = lax.rem(me + d, n)
            return (p // (ny * nz), lax.rem(p // nz, ny), lax.rem(p, nz))

        barrier = pltpu.get_barrier_semaphore()
        for d in range(1, n):
            pl.semaphore_signal(barrier, inc=1, device_id=coords(d), device_id_type=MESH_ID)
        pl.semaphore_wait(barrier, n - 1)
        copies = []
        for d in range(1, n):
            cp = pltpu.make_async_remote_copy(
                src_ref=x_ref, dst_ref=o_ref.at[me], send_sem=send_sem.at[d], recv_sem=recv_sem.at[d],
                device_id=coords(d), device_id_type=MESH_ID)
            cp.start()
            copies.append(cp)
        o_ref[me] = x_ref[...]
        for cp in copies:
            cp.wait()

    return pl.pallas_call(
        body,
        out_shape=jax.ShapeDtypeStruct((n,) + x.shape, x.dtype),
        in_specs=[pl.BlockSpec(memory_space=pltpu.VMEM)],
        out_specs=pl.BlockSpec(memory_space=pltpu.VMEM),
        scratch_shapes=[pltpu.SemaphoreType.DMA((n,)), pltpu.SemaphoreType.DMA((n,))],
        compiler_params=pltpu.CompilerParams(collective_id=cid, has_side_effects=True),
        name="share_plan",
    )(x)


def route_z(own, pair, pos):
    n_mig = own.shape[0]

    def body(own_ref, pair_ref, pos_ref, z_ref, cnt):
        row, core = pos_ref[0], pos_ref[1] & 1

        @pl.loop(0, 3 * Z_CORE)
        def _(i):
            z_ref[i] = 0

        for i in range(4):
            cnt[i] = 0

        @pl.loop(0, 2 * n_mig)
        def _(i):
            second = (i >= n_mig).astype(jnp.int32)
            e = i - second * n_mig
            mine = second == core
            dd = jnp.where(mine, own_ref[e], pair_ref[e])
            di = dd >> 2
            k = cnt[di]
            cnt[di] = k + 1
            shift = (di - row) & 3

            @pl.when((shift != 0) & ((k & 1) == core) & (k < 2 * Z_CORE))
            def _():
                z_ref[(shift - 1) * Z_CORE + (k >> 1)] = jnp.where(mine, e, n_mig + e)

    smem = pl.BlockSpec(memory_space=pltpu.SMEM)
    return pl.pallas_call(
        body,
        out_shape=jax.ShapeDtypeStruct((64,), jnp.int32),
        in_specs=[smem] * 3,
        out_specs=smem,
        scratch_shapes=[pltpu.SMEM((4,), jnp.int32)],
        name="route_z",
    )(own, pair, pos)


def route(dst, dev, pos, n_mig, n_slots):
    n_dev = dev.shape[0] // n_mig
    z_at, y_at = 2 * n_mig, 2 * n_mig + 2 * 3 * Z_CORE

    def body(dst_ref, dev_ref, pos_ref, y_ref, s_ref, cnt, cnt2):
        row, colm = pos_ref[0], pos_ref[1]
        half, core = colm >> 1, colm & 1
        me = row * 4 + colm

        @pl.loop(0, 64)
        def _(i):
            y_ref[i] = 0
            s_ref[i] = -1
            cnt[i] = 0

        @pl.loop(0, 8)
        def _(i):
            cnt2[i] = 0

        @pl.loop(0, n_dev)
        def _(d):
            si, sy, sc = d >> 2, (d >> 1) & 1, d & 1

            @pl.loop(0, n_mig)
            def _(e):
                dd = dev_ref[d * n_mig + e]
                di, dy = dd >> 2, (dd >> 1) & 1
                c1 = (d >> 1) * 4 + di
                k = cnt[c1]
                cnt[c1] = k + 1
                cross = (dy != sy).astype(jnp.int32)
                c2 = di * 2 + sy
                k2 = cnt2[c2]
                cnt2[c2] = k2 + cross

                @pl.when(di == row)
                def _():
                    shift = (di - si) & 3
                    at = jnp.where(sc == core, e, n_mig + e)
                    z_slot = (shift - 1) * Z_CORE + (k >> 1)
                    here = jnp.where(shift == 0, at, z_at + z_slot + jnp.where((k & 1) == core, 0, 3 * Z_CORE))

                    @pl.when((sy == half) & (cross == 1) & ((k2 & 1) == core) & (k2 < 2 * Y_CORE))
                    def _():
                        y_ref[k2 >> 1] = jnp.minimum(here, y_at - 1)

                    @pl.when(dd == me)
                    def _():
                        by_y = y_at + (k2 >> 1) + jnp.where((k2 & 1) == core, 0, Y_CORE)
                        s_ref[dst_ref[d * n_mig + e] - me * n_slots] = jnp.where(cross == 1, by_y, here)

    smem = pl.BlockSpec(memory_space=pltpu.SMEM)
    return pl.pallas_call(
        body,
        out_shape=[jax.ShapeDtypeStruct((64,), jnp.int32)] * 2,
        in_specs=[smem] * 3,
        out_specs=[smem] * 2,
        scratch_shapes=[pltpu.SMEM((64,), jnp.int32), pltpu.SMEM((8,), jnp.int32)],
        cost_estimate=pl.CostEstimate(flops=100_000_000, bytes_accessed=1_000_000, transcendentals=0),
        name="route",
    )(dst, dev, pos)


def around(me):
    sib = me + 1 - 2 * lax.rem(me, 2)
    over = lax.rem(me + 2, 4)
    return sib, over, lax.rem(sib + 2, 4)


def enter(axis, peers):
    barrier = pltpu.get_barrier_semaphore()
    for p in peers:
        pl.semaphore_signal(barrier, inc=1, device_id={axis: p}, device_id_type=MESH_ID)
    pl.semaphore_wait(barrier, len(peers))


def gather_rows(x, axis, n, cid):
    def body(x_ref, o_ref, send_sem, recv_sem):
        me = lax.axis_index(axis)
        sib, over, _ = around(me)
        enter(axis, (sib, over))

        def send(src, at, peer, i):
            return pltpu.make_async_remote_copy(
                src_ref=src, dst_ref=o_ref.at[at], send_sem=send_sem.at[i], recv_sem=recv_sem.at[i],
                device_id={axis: peer}, device_id_type=MESH_ID)

        cross, near = send(x_ref, me, over, 0), send(x_ref, me, sib, 1)
        cross.start()
        near.start()
        o_ref[me] = x_ref[...]
        cross.wait()
        hand = send(o_ref.at[over], over, sib, 2)
        hand.start()
        near.wait()
        hand.wait()

    return pl.pallas_call(
        body,
        out_shape=jax.ShapeDtypeStruct((n,) + x.shape, x.dtype),
        in_specs=[pl.BlockSpec(memory_space=pltpu.VMEM)],
        out_specs=pl.BlockSpec(memory_space=pltpu.VMEM),
        scratch_shapes=[pltpu.SemaphoreType.DMA((3,)), pltpu.SemaphoreType.DMA((3,))],
        compiler_params=pltpu.CompilerParams(collective_id=cid, has_side_effects=True),
        cost_estimate=pl.CostEstimate(flops=1_000_000_000, bytes_accessed=2_000_000, transcendentals=0),
        name="gather_rows",
    )(x)


def combine(acc, ml, axis, n, cid):
    rows, r, hd = acc.shape
    b = rows // n

    def body(acc_ref, ml_ref, o_ref, sib_me, sib_over, ml_sib, to_over, ml_to, y_acc, ml_y, send_sem, recv_sem):
        me = lax.axis_index(axis)
        sib, over, diag = around(me)
        enter(axis, (sib, over))

        def send(src, dst, peer, i):
            return pltpu.make_async_remote_copy(
                src_ref=src, dst_ref=dst, send_sem=send_sem.at[i], recv_sem=recv_sem.at[i],
                device_id={axis: peer}, device_id_type=MESH_ID)

        near = [send(acc_ref.at[pl.ds(diag * b, b)], sib_over, sib, 0), send(ml_ref, ml_sib, sib, 1),
                send(acc_ref.at[pl.ds(sib * b, b)], sib_me, sib, 2)]
        for cp in near:
            cp.start()
        near[0].wait()
        near[1].wait()
        lane = lax.broadcasted_iota(jnp.int32, (r, ml_ref.shape[2]), 1)

        def pick(t, s):
            return jnp.sum(jnp.where(lane == s, t, 0.0), axis=1, keepdims=True)

        top = jnp.maximum(ml_ref[0], ml_sib[0])
        w_own, w_sib = jnp.exp(ml_ref[0] - top), jnp.exp(ml_sib[0] - top)
        tot = w_own * ml_ref[1] + w_sib * ml_sib[1]
        ml_to[0] = top
        ml_to[1] = tot
        for i in range(b):
            s = over * b + i
            to_over[i] = pick(w_own, s) * acc_ref[s] + pick(w_sib, s) * sib_over[i]
        far = [send(to_over, y_acc, over, 3), send(ml_to, ml_y, over, 4)]
        for cp in far:
            cp.start()
        near[2].wait()
        far[1].wait()
        last = jnp.maximum(top, ml_y[0])
        f, g = jnp.exp(top - last), jnp.exp(ml_y[0] - last)
        den = f * tot + g * ml_y[1]
        f, g = f / den, g / den
        w_own, w_sib = f * w_own, f * w_sib
        for i in range(b):
            s = me * b + i
            sib_me[i] = pick(w_own, s) * acc_ref[s] + pick(w_sib, s) * sib_me[i]
        far[0].wait()
        for i in range(b):
            o_ref[i] = (sib_me[i] + pick(g, me * b + i) * y_acc[i]).astype(o_ref.dtype)

    block = pltpu.VMEM((b, r, hd), jnp.float32)
    stats = pltpu.VMEM(ml.shape, jnp.float32)
    return pl.pallas_call(
        body,
        out_shape=jax.ShapeDtypeStruct((b, r, hd), jnp.bfloat16),
        in_specs=[pl.BlockSpec(memory_space=pltpu.VMEM)] * 2,
        out_specs=pl.BlockSpec(memory_space=pltpu.VMEM),
        scratch_shapes=[block, block, stats, block, stats, block, stats,
                        pltpu.SemaphoreType.DMA((5,)), pltpu.SemaphoreType.DMA((5,))],
        compiler_params=pltpu.CompilerParams(collective_id=cid, has_side_effects=True),
        cost_estimate=pl.CostEstimate(flops=1_000_000_000, bytes_accessed=2_000_000, transcendentals=0),
        name="combine",
    )(acc, ml)


def mlp_pair(attn, hidden, w_out, w_up, w_down, layer, cid):
    rows, d = attn.shape
    ff = w_up.shape[2]
    r = -(-rows // 32) * 32
    tile = 512
    d_half, f_half = d // 2, ff // 2
    n_o, n_f = d_half // tile, f_half // tile
    ring_c, ring_r = min(8, n_o + n_f), min(6, n_f)
    attn, hidden = (jnp.pad(t, ((0, r - rows), (0, 0))) for t in (attn, hidden))

    def body(attn_ref, hid_ref, wo_ref, wu_ref, wd_ref, o_ref, x_all, h_all, hm, act, acc, rx, wc, wr, csem, rsem, ssem, qsem):
        me = lax.axis_index('kv')
        core = lax.rem(me, 2)
        peer = me + 1 - 2 * core
        mine, other = pl.ds(core * r, r), pl.ds((1 - core) * r, r)

        def col(c, is_out):
            if is_out:
                src = wo_ref.at[layer, :, pl.ds(pl.multiple_of(core * d_half + c * tile, tile), tile)]
            else:
                src = wu_ref.at[layer, :, pl.ds(pl.multiple_of(core * f_half + (c - n_o) * tile, tile), tile)]
            slot = lax.rem(c, ring_c)
            return pltpu.make_async_copy(src, wc.at[slot], csem.at[slot])

        def row(j):
            slot = lax.rem(j, ring_r)
            src = wd_ref.at[layer, pl.ds(pl.multiple_of(core * f_half + j * tile, tile), tile), :]
            return pltpu.make_async_copy(src, wr.at[slot], rsem.at[slot])

        for c in range(ring_c):
            col(c, c < n_o).start()

        barrier = pltpu.get_barrier_semaphore()
        pl.semaphore_signal(barrier, inc=1, device_id={'kv': peer}, device_id_type=MESH_ID)
        pl.semaphore_wait(barrier, 1)

        def send(src, dst, i):
            return pltpu.make_async_remote_copy(
                src_ref=src, dst_ref=dst, send_sem=ssem.at[i], recv_sem=qsem.at[i],
                device_id={'kv': peer}, device_id_type=MESH_ID)

        swaps = [send(attn_ref, x_all.at[mine], 0), send(hid_ref, h_all.at[mine], 1)]
        for cp in swaps:
            cp.start()
        x_all[mine] = attn_ref[...]
        h_all[mine] = hid_ref[...]
        for cp in swaps:
            cp.wait()

        @pl.loop(0, n_o)
        def _(c):
            col(c, True).wait()
            at = pl.ds(pl.multiple_of(core * d_half + c * tile, tile), tile)
            part = jnp.dot(x_all[...], wc[lax.rem(c, ring_c)], preferred_element_type=jnp.float32)
            hm[:, at] = (h_all[:, at].astype(jnp.float32) + part).astype(jnp.bfloat16)

            @pl.when(c + ring_c < n_o + n_f)
            def _():
                col(c + ring_c, False).start()

        own_cols = pl.ds(pl.multiple_of(core * d_half, tile), d_half)
        cp = send(hm.at[:, own_cols], hm.at[:, own_cols], 2)
        cp.start()
        acc[...] = jnp.zeros_like(acc)
        cp.wait()

        @pl.loop(0, n_f)
        def _(j):
            c = j + n_o
            col(c, False).wait()
            up = jnp.dot(hm[...], wc[lax.rem(c, ring_c)], preferred_element_type=jnp.float32)
            act[:, pl.ds(pl.multiple_of(j * tile, tile), tile)] = jax.nn.gelu(up).astype(jnp.bfloat16)

            @pl.when(c + ring_c < n_o + n_f)
            def _():
                col(c + ring_c, False).start()

            @pl.when(j < ring_r)
            def _():
                row(j).start()

        @pl.loop(0, n_f)
        def _(j):
            row(j).wait()
            acc[...] += jnp.dot(act[:, pl.ds(pl.multiple_of(j * tile, tile), tile)], wr[lax.rem(j, ring_r)],
                                preferred_element_type=jnp.float32)

            @pl.when(j + ring_r < n_f)
            def _():
                row(j + ring_r).start()

        cp = send(acc.at[other], rx, 3)
        cp.start()
        cp.wait()
        o_ref[...] = (hm[mine].astype(jnp.float32) + (acc[mine] + rx[...])).astype(o_ref.dtype)

    vmem, any_spec = pl.BlockSpec(memory_space=pltpu.VMEM), pl.BlockSpec(memory_space=pl.ANY)
    out = pl.pallas_call(
        body,
        out_shape=jax.ShapeDtypeStruct((r, d), jnp.bfloat16),
        in_specs=[vmem, vmem, any_spec, any_spec, any_spec],
        out_specs=vmem,
        scratch_shapes=[
            pltpu.VMEM((2 * r, d), jnp.bfloat16), pltpu.VMEM((2 * r, d), jnp.bfloat16), pltpu.VMEM((2 * r, d), jnp.bfloat16),
            pltpu.VMEM((2 * r, f_half), jnp.bfloat16), pltpu.VMEM((2 * r, d), jnp.float32), pltpu.VMEM((r, d), jnp.float32),
            pltpu.VMEM((ring_c, d, tile), jnp.bfloat16), pltpu.VMEM((ring_r, tile, d), jnp.bfloat16),
            pltpu.SemaphoreType.DMA((ring_c,)), pltpu.SemaphoreType.DMA((ring_r,)),
            pltpu.SemaphoreType.DMA((4,)), pltpu.SemaphoreType.DMA((4,)),
        ],
        compiler_params=pltpu.CompilerParams(collective_id=cid, has_side_effects=True, vmem_limit_bytes=58 * 1024 * 1024),
        cost_estimate=pl.CostEstimate(flops=6_000_000_000, bytes_accessed=60_000_000, transcendentals=0),
    )(attn, hidden, w_out, w_up, w_down)
    return out[:rows]


def attend(info, counts, qkv, pools_in, unit_srcs, first_unit, prev_pools, state, layer, part, n_slots, layers, page, kvh, q_group, hd):
    sources = list(pools_in) + list(unit_srcs)
    n_pool = len(pools_in)
    prow = page * kvh
    qr = 2 * kvh * q_group
    n_seq = qkv.shape[0]
    scale = hd ** -0.5
    aliased = prev_pools is not None
    carried = state is not None

    def body(info_ref, cnt_ref, qkv_ref, *rest):
        ins, rest = rest[:len(sources)], rest[len(sources):]
        if aliased:
            rest = rest[2:]
        if carried:
            acc_prev, ml_prev = rest[:2]
            rest = rest[2:]
        k_out, v_out, acc_ref, ml_ref, kbuf, vbuf, isem, osem = rest
        lo = cnt_ref[2 * part - 1] if part else 0
        mid = cnt_ref[2 * part]
        hi = cnt_ref[2 * part + 1]

        def load_from(k_page, v_page, i):
            return (pltpu.make_async_copy(k_page, kbuf.at[i], isem.at[0, i]),
                    pltpu.make_async_copy(v_page, vbuf.at[i], isem.at[1, i]))

        def from_pool(i):
            at = info_ref[0, i] * layers + layer
            return load_from(ins[0].at[at], ins[1].at[at], i)

        def loads(i):
            if n_pool:
                return from_pool(i)
            return load_from(ins[0].at[0, pl.ds(0, prow)], ins[0].at[0, pl.ds(prow, prow)], i)

        def start_loads(i):
            at, first = info_ref[3, i], first_unit
            if n_pool and unit_srcs:
                pl.when(at < 0)(lambda: [cp.start() for cp in from_pool(i)] and None)
            elif n_pool:
                for cp in from_pool(i):
                    cp.start()
            for ref in ins[n_pool:]:
                last = first + ref.shape[0]

                @pl.when((at >= first) & (at < last))
                def _():
                    u = at - first
                    for cp in load_from(ref.at[u, pl.ds(0, prow)], ref.at[u, pl.ds(prow, prow)], i):
                        cp.start()

                first = last

        def stores(i):
            slot = info_ref[0, i]
            return (pltpu.make_async_copy(kbuf.at[i], k_out.at[slot * layers + layer], osem.at[0, i]),
                    pltpu.make_async_copy(vbuf.at[i], v_out.at[slot * layers + layer], osem.at[1, i]))

        @pl.loop(lo, hi)
        def _(i):
            start_loads(i)

        if carried:
            acc_ref[...] = acc_prev[...]
            ml_ref[...] = ml_prev[...]
        else:
            acc_ref[...] = jnp.zeros_like(acc_ref)
            ml_ref[0] = jnp.full(ml_ref.shape[1:], NEG, jnp.float32)
            ml_ref[1] = jnp.zeros(ml_ref.shape[1:], jnp.float32)

        col = lax.broadcasted_iota(jnp.int32, (qr, prow), 1)
        row = lax.broadcasted_iota(jnp.int32, (qr, prow), 0)
        late = (row >= kvh * q_group).astype(jnp.int32)
        head_ok = lax.rem(col, kvh) == (row - late * (kvh * q_group)) // q_group
        need = col // kvh - late
        need = jnp.where(head_ok, need, 1 << 20)
        lane = lax.broadcasted_iota(jnp.int32, ml_ref.shape[1:], 1)
        wrow = lax.broadcasted_iota(jnp.int32, (4 * kvh, hd), 0) // kvh

        @pl.loop(0, (mid - lo + UNROLL - 1) // UNROLL)
        def _(g):
            base = lo + g * UNROLL
            idx, seqs, offs = [], [], []
            for u in range(UNROLL):
                i = base + u
                live = i < mid
                j = jnp.minimum(i, mid - 1)
                idx.append(j)
                seqs.append(jnp.where(live, info_ref[1, j], n_seq))
                offs.append(info_ref[2, j])

                @pl.when(live)
                def _():
                    for cp in loads(j):
                        cp.wait()

            for j, seq, off in zip(idx, seqs, offs):
                w = jnp.minimum(off // 2, page // 2 - 2)
                at = pl.ds(pl.multiple_of(w * (2 * kvh), 2 * kvh), 4 * kvh)
                tok = wrow + 2 * w
                seq = jnp.minimum(info_ref[1, j], n_seq - 1)
                for buf, r0 in ((kbuf, qr), (vbuf, qr + 2 * kvh)):
                    new = qkv_ref[seq, r0:r0 + 2 * kvh, :].astype(jnp.float32)
                    first = jnp.concatenate([new[:kvh]] * 4, axis=0)
                    second = jnp.concatenate([new[kvh:]] * 4, axis=0)
                    old = buf[j, at, :].astype(jnp.float32)
                    old = jnp.where(tok == off, first, jnp.where(tok == off + 1, second, old))
                    buf[j, at, :] = old.astype(jnp.bfloat16)

            res = []
            for u in range(UNROLL):
                q = qkv_ref[jnp.minimum(seqs[u], n_seq - 1), :qr, :]
                s = lax.dot_general(q, kbuf[idx[u]], (((1,), (1,)), ((), ())), preferred_element_type=jnp.float32) * scale
                s = jnp.where(need <= offs[u], s, NEG)
                m = jnp.max(s, axis=1, keepdims=True)
                p = jnp.exp(s - m)
                l = jnp.sum(p, axis=1, keepdims=True)
                o = jnp.dot(p.astype(jnp.bfloat16), vbuf[idx[u]], preferred_element_type=jnp.float32)
                res.append((m, l, o))
            for u in range(UNROLL):
                m, l, o = res[u]
                sel = lane == seqs[u]
                m_all, l_all = ml_ref[0], ml_ref[1]
                m_old = jnp.max(jnp.where(sel, m_all, NEG), axis=1, keepdims=True)
                m_new = jnp.maximum(m_old, m)
                alpha = jnp.exp(m_old - m_new)
                beta = jnp.exp(m - m_new)
                acc_ref[seqs[u]] = acc_ref[seqs[u]] * alpha + o * beta
                ml_ref[0] = jnp.where(sel, m_new, m_all)
                ml_ref[1] = jnp.where(sel, l_all * alpha + l * beta, l_all)
            for u in range(UNROLL):
                @pl.when(base + u < mid)
                def _():
                    for cp in stores(base + u):
                        cp.start()

        @pl.loop(mid, hi)
        def _(i):
            for cp in loads(i):
                cp.wait()
            for cp in stores(i):
                cp.start()

        @pl.loop(lo, hi)
        def _(i):
            for cp in stores(i):
                cp.wait()

    any_spec = pl.BlockSpec(memory_space=pl.ANY)
    vmem = pl.BlockSpec(memory_space=pltpu.VMEM)
    smem = pl.BlockSpec(memory_space=pltpu.SMEM)
    operands = [info, counts, qkv, *sources]
    specs = [smem, smem, vmem] + [any_spec] * len(sources)
    alias = {}
    if aliased:
        alias = {len(operands): 0, len(operands) + 1: 1}
        operands += list(prev_pools)
        specs += [any_spec, any_spec]
    if carried:
        operands += list(state)
        specs += [vmem, vmem]
    pool = jax.ShapeDtypeStruct((n_slots * layers, prow, hd), jnp.bfloat16)
    return pl.pallas_call(
        body,
        out_shape=[pool, pool,
                   jax.ShapeDtypeStruct((n_seq + 1, qr, hd), jnp.float32),
                   jax.ShapeDtypeStruct((2, qr, 128), jnp.float32)],
        in_specs=specs,
        out_specs=[any_spec, any_spec, vmem, vmem],
        scratch_shapes=[
            pltpu.VMEM((n_slots, prow, hd), jnp.bfloat16),
            pltpu.VMEM((n_slots, prow, hd), jnp.bfloat16),
            pltpu.SemaphoreType.DMA((2, n_slots)),
            pltpu.SemaphoreType.DMA((2, n_slots)),
        ],
        input_output_aliases=alias,
        cost_estimate=pl.CostEstimate(flops=400_000_000, bytes_accessed=16_000_000, transcendentals=0),
    )(*operands)


def solution(mesh):
    n_rows = mesh.shape['kv2']
    n_cols = mesh.shape['kv']
    dev_axes = ('rep', 'kv2', 'kv')
    seq_spec = P(None, dev_axes, None)
    pool_spec = P(dev_axes, None, None, None, None)
    table_spec = P(dev_axes, None)
    vec_spec = P(dev_axes)
    full_spec = P()

    def per_device(x_embed, w_query, w_key, w_value, w_out, w_up, w_down, k_pool, v_pool, old_table, seq_len, src_slot, dst_slot):
        n_slots, layers, page, kv_heads, head_dim = k_pool.shape
        heads = w_query.shape[2] // head_dim
        q_group = heads // kv_heads
        seq_dev = x_embed.shape[1]
        n_pages = old_table.shape[1]
        n_mig = src_slot.shape[0]
        n_dev = n_rows * n_cols
        row_seqs = seq_dev * n_cols
        prow = page * kv_heads
        width = x_embed.shape[2]
        me_row, me_col = lax.axis_index('kv2'), lax.axis_index('kv')
        me = me_row * n_cols + me_col
        base = me * n_slots

        k_rows = k_pool.reshape(n_slots * layers, prow, head_dim)
        v_rows = v_pool.reshape(n_slots * layers, prow, head_dim)
        pair = [(c, c ^ 1) for c in range(n_cols)]
        over = [(c, c ^ 2) for c in range(n_cols)]
        z_hops = [[(r, (r + s) % n_rows) for r in range(n_rows)] for s in range(1, n_rows)]
        pos = jnp.stack([me_row, me_col]).astype(jnp.int32)
        dev_own = dst_slot // n_slots
        leaving = take_pages((src_slot - base) * layers, k_rows, v_rows, layers)
        units = [[leaving[0], lax.ppermute(leaving[0], 'kv', pair)]]
        dev_pair = lax.ppermute(dev_own, 'kv', pair)

        n_rep = mesh.shape['rep']
        words = [src_slot, dst_slot, dst_slot // n_slots, old_table.reshape(-1), seq_len]
        cuts = [0]
        for w in words:
            cuts.append(cuts[-1] + w.shape[0])
        meta = jnp.pad(jnp.concatenate(words), (0, 128 - cuts[-1])).reshape(1, 128)
        meta_all = share_plan(meta, (n_rep, n_rows, n_cols), 2).reshape(n_rep, n_dev, 128)

        meta_all, pos = lax.optimization_barrier((meta_all, pos))
        z_list = route_z(dev_own, dev_pair, pos)
        hops = pick(z_list, units[0], [Z_CORE] * (n_rows - 1))
        hops, z_list, hidden, meta_all, later = lax.optimization_barrier(
            (hops, z_list, x_embed.reshape(2 * seq_dev, width), meta_all, leaving[1:]))
        units += [[own, lax.ppermute(own, 'kv', pair)] for own in later]

        meta = lax.dynamic_index_in_dim(meta_all, lax.axis_index('rep'), 0, keepdims=False)
        src_all, dst_all, dev_all = (meta[:, cuts[t]:cuts[t + 1]].reshape(-1) for t in range(3))
        row_meta = lax.dynamic_slice_in_dim(meta, me_row * n_cols, n_cols, axis=0)
        row_table = row_meta[:, cuts[3]:cuts[4]].reshape(-1)
        row_len = row_meta[:, cuts[4]:cuts[5]].reshape(-1)

        dev_by = meta_all[:, :, cuts[2]:cuts[3]]
        to_row = dev_by // n_cols
        rows4 = jnp.arange(n_rows, dtype=jnp.int32)
        goes = (to_row[..., None] == rows4).astype(jnp.int32).sum(axis=2)
        per_chip = goes.reshape(n_rep, n_rows, n_cols // 2, 2, n_rows).sum(axis=3)
        leaves = rows4[:, None] != rows4[None, :]
        z_full = ((per_chip > 2 * Z_CORE) & leaves[None, :, None, :]).any()
        side = (jnp.arange(n_dev, dtype=jnp.int32) // 2 % 2)[None, :, None]
        crosses = dev_by // 2 % 2 != side
        per_side = ((to_row[..., None] == rows4) & crosses[..., None]).astype(jnp.int32).sum(axis=2)
        y_full = (per_side.reshape(n_rep, n_rows, n_cols // 2, 2, n_rows).sum(axis=(1, 3)) > 2 * Y_CORE).any()
        full = z_full | y_full

        y_list, unit_of = route(dst_all, dev_all, pos, n_mig, n_slots)

        def along_z(hops):
            got = []
            for h, z in zip(hops, z_hops):
                got.append(lax.ppermute(h, 'kv2', z))
            return got

        def swap(units, got):
            return units + got + [lax.ppermute(g, 'kv', pair) for g in got]

        def along_y(hop):
            got = lax.ppermute(hop, 'kv', over)
            return [got, lax.ppermute(got, 'kv', pair)]

        same = row_table[:, None] == src_all[None, :]
        new_table = jnp.where(same.any(axis=1), jnp.sum(jnp.where(same, dst_all[None, :], 0), axis=1), row_table)
        slots = jnp.arange(n_slots, dtype=jnp.int32)
        cells = jnp.arange(row_seqs * n_pages, dtype=jnp.int32)
        slot_cell = jnp.max(jnp.where(new_table[None, :] == (slots + base)[:, None], cells[None, :], -1), axis=1)
        moves = jnp.arange(n_dev * n_mig, dtype=jnp.int32)
        move_of = jnp.max(jnp.where(dst_all[None, :] == (slots + base)[:, None], moves[None, :], -1), axis=1)
        is_mig = move_of >= 0
        used = slot_cell >= 0
        seq_of = jnp.where(used, slot_cell // n_pages, row_seqs)
        seq_one = seq_of[:, None] == jnp.arange(row_seqs, dtype=jnp.int32)[None, :]
        len_of = jnp.sum(jnp.where(seq_one, row_len[None, :], 0), axis=1)
        off_of = len_of - (slot_cell % n_pages) * page
        off_of = jnp.where(used & (off_of >= 0) & (off_of < page), off_of, 2 * page)
        y_at = 2 * n_mig + 2 * (n_rows - 1) * Z_CORE
        unit = jnp.where(is_mig, jnp.where(full, slots + y_at + 2 * Y_CORE, unit_of[:n_slots]), -1)

        def lists(cls, n_cls):
            key = cls * 2 + (~used).astype(jnp.int32)
            order = key * n_slots + slots
            at = jnp.sum((order[None, :] < order[:, None]).astype(jnp.int32), axis=1)
            place = at[None, :] == jnp.arange(64, dtype=jnp.int32)[:, None]
            info = jnp.stack([jnp.sum(jnp.where(place, t[None, :], 0), axis=1) for t in (slots, seq_of, off_of, unit)])
            counts = jnp.sum((key[None, :] <= jnp.arange(2 * n_cls, dtype=jnp.int32)[:, None]).astype(jnp.int32), axis=1)
            return info, counts

        by_class = lists(is_mig.astype(jnp.int32) + (unit >= y_at).astype(jnp.int32), 3)
        by_use = lists(jnp.zeros_like(slots), 1)

        def all_pages(layer):
            def collect():
                every = lax.all_gather(leaving[layer], ('kv2', 'kv'), tiled=True)
                return pick(jnp.maximum(move_of, 0), [every], [n_slots])[0]

            return lax.cond(full, collect, lambda: uninit((n_slots, 2 * prow, head_dim), jnp.bfloat16))

        pools = None
        got = along_z(hops)
        for layer in range(layers):
            dot = lambda a, w: jnp.dot(a, w[layer], preferred_element_type=jnp.float32)
            query = dot(hidden, w_query).astype(jnp.bfloat16).reshape(2, seq_dev, heads, head_dim)
            k_new = dot(hidden, w_key).astype(jnp.bfloat16).reshape(2, seq_dev, kv_heads, head_dim)
            v_new = dot(hidden, w_value).astype(jnp.bfloat16).reshape(2, seq_dev, kv_heads, head_dim)
            per_seq = lambda t: jnp.swapaxes(t, 0, 1).reshape(seq_dev, -1, head_dim)
            qkv = jnp.concatenate([per_seq(query), per_seq(k_new), per_seq(v_new)], axis=1)
            qkv = gather_rows(qkv, 'kv', n_cols, 0).reshape(row_seqs, -1, head_dim)
            dims = dict(layer=layer, n_slots=n_slots, layers=layers, page=page, kvh=kv_heads, q_group=q_group, hd=head_dim)
            if layer == 0:
                *pools, acc, ml = attend(*by_class, qkv, [k_rows, v_rows], [], 0, pools, None, part=0, **dims)
                next_hops = pick(z_list, units[1], [Z_CORE] * (n_rows - 1))
                got, acc, next_hops = lax.optimization_barrier((got, acc, next_hops))
                next_got = along_z(next_hops)
                all_units = swap(units[0], got)
                hop, = pick(y_list, all_units, [Y_CORE])
                last = along_y(hop) + [all_pages(0)]
                *pools, acc, ml = attend(*by_class, qkv, [], all_units, 0, pools, (acc, ml), part=1, **dims)
                *pools, acc, ml = attend(*by_class, qkv, [], last, y_at, pools, (acc, ml), part=2, **dims)
            else:
                srcs = all_units + along_y(hop) + [all_pages(layer)]
                *pools, acc, ml = attend(*by_use, qkv, [k_rows, v_rows], srcs, 0, pools, None, part=0, **dims)
            o = combine(acc, ml, 'kv', n_cols, 1)
            if layer + 1 < layers:
                next_got, o = lax.optimization_barrier((next_got, o))
                all_units = swap(units[layer + 1], next_got)
                hop, = pick(y_list, all_units, [Y_CORE])
                hop, o = lax.optimization_barrier((hop, o))
            attn_out = jnp.swapaxes(o.reshape(seq_dev, 2, heads * head_dim), 0, 1).reshape(2 * seq_dev, heads * head_dim)
            hidden = mlp_pair(attn_out, hidden, w_out, w_up, w_down, layer, 3 + layer)
        k_out, v_out = (p.reshape(k_pool.shape) for p in pools)
        return hidden.reshape(2, seq_dev, width), k_out, v_out

    return jax.shard_map(per_device, mesh=mesh, in_specs=(seq_spec, full_spec, full_spec, full_spec, full_spec, full_spec, full_spec, pool_spec, pool_spec, table_spec, vec_spec, vec_spec, vec_spec), out_specs=(seq_spec, pool_spec, pool_spec), check_vma=False)
```

```python
import jax
import jax.numpy as jnp
from jax import lax
from jax.experimental import pallas as pl
from jax.experimental.pallas import tpu as pltpu
from jax.sharding import PartitionSpec as P


MESH_ID = pl.DeviceIdType.MESH
NEG = -1e30
UNROLL = 4
Z_CORE = 6
Y_CORE = 10


def uninit(shape, dtype):
    def body(o_ref):
        pass

    return pl.pallas_call(
        body, out_shape=jax.ShapeDtypeStruct(shape, dtype), out_specs=pl.BlockSpec(memory_space=pl.ANY), name="uninit")()


def take_pages(rows, k_rows, v_rows, layers):
    m = rows.shape[0]
    prow, hd = k_rows.shape[1:]

    def body(rows_ref, k_in, v_in, *rest):
        outs, (buf, isem, osem) = rest[:layers], rest[layers:]
        ins, puts = [], []
        for layer in range(layers):
            for i in range(m):
                for which, ref in enumerate((k_in, v_in)):
                    cp = pltpu.make_async_copy(
                        ref.at[rows_ref[i] + layer], buf.at[layer, i, pl.ds(which * prow, prow)], isem.at[layer, 2 * i + which])
                    cp.start()
                    ins.append(cp)
        for layer in range(layers):
            for cp in ins[layer * 2 * m:(layer + 1) * 2 * m]:
                cp.wait()
            cp = pltpu.make_async_copy(buf.at[layer], outs[layer], osem.at[layer])
            cp.start()
            puts.append(cp)
        for cp in puts:
            cp.wait()

    any_spec = pl.BlockSpec(memory_space=pl.ANY)
    return pl.pallas_call(
        body,
        out_shape=[jax.ShapeDtypeStruct((m, 2 * prow, hd), k_rows.dtype)] * layers,
        in_specs=[pl.BlockSpec(memory_space=pltpu.SMEM), any_spec, any_spec],
        out_specs=[any_spec] * layers,
        scratch_shapes=[pltpu.VMEM((layers, m, 2 * prow, hd), k_rows.dtype),
                        pltpu.SemaphoreType.DMA((layers, 2 * m)), pltpu.SemaphoreType.DMA((layers,))],
        cost_estimate=pl.CostEstimate(flops=100_000_000, bytes_accessed=12_000_000, transcendentals=0),
        name="take_pages",
    )(rows, k_rows, v_rows)


def pick(lists, sources, splits):
    n = sum(splits)
    tail, dtype = sources[0].shape[1:], sources[0].dtype

    def body(idx_ref, *rest):
        ins, outs, (buf, isem, osem) = rest[:len(sources)], rest[len(sources):-3], rest[-3:]

        @pl.loop(0, n)
        def _(i):
            at, lo = idx_ref[i], 0
            for ref in ins:
                hi = lo + ref.shape[0]

                @pl.when((at >= lo) & (at < hi))
                def _():
                    pltpu.make_async_copy(ref.at[at - lo], buf.at[i], isem.at[i]).start()

                lo = hi

        @pl.loop(0, n)
        def _(i):
            pltpu.make_async_copy(ins[0].at[0], buf.at[i], isem.at[i]).wait()

        puts, lo = [], 0
        for j, size in enumerate(splits):
            cp = pltpu.make_async_copy(buf.at[pl.ds(lo, size)], outs[j], osem.at[j])
            cp.start()
            puts.append(cp)
            lo += size
        for cp in puts:
            cp.wait()

    any_spec = pl.BlockSpec(memory_space=pl.ANY)
    return pl.pallas_call(
        body,
        out_shape=[jax.ShapeDtypeStruct((size,) + tail, dtype) for size in splits],
        in_specs=[pl.BlockSpec(memory_space=pltpu.SMEM)] + [any_spec] * len(sources),
        out_specs=[any_spec] * len(splits),
        scratch_shapes=[pltpu.VMEM((n,) + tail, dtype), pltpu.SemaphoreType.DMA((n,)), pltpu.SemaphoreType.DMA((len(splits),))],
        cost_estimate=pl.CostEstimate(flops=100_000_000, bytes_accessed=5_000_000, transcendentals=0),
    )(lists, *sources)


def share_plan(x, mesh_shape, cid):
    nx, ny, nz = mesh_shape
    n = nx * ny * nz

    def body(x_ref, o_ref, send_sem, recv_sem):
        me = (lax.axis_index('rep') * ny + lax.axis_index('kv2')) * nz + lax.axis_index('kv')

        def coords(d):
            p = lax.rem(me + d, n)
            return (p // (ny * nz), lax.rem(p // nz, ny), lax.rem(p, nz))

        barrier = pltpu.get_barrier_semaphore()
        for d in range(1, n):
            pl.semaphore_signal(barrier, inc=1, device_id=coords(d), device_id_type=MESH_ID)
        pl.semaphore_wait(barrier, n - 1)
        copies = []
        for d in range(1, n):
            cp = pltpu.make_async_remote_copy(
                src_ref=x_ref, dst_ref=o_ref.at[me], send_sem=send_sem.at[d], recv_sem=recv_sem.at[d],
                device_id=coords(d), device_id_type=MESH_ID)
            cp.start()
            copies.append(cp)
        o_ref[me] = x_ref[...]
        for cp in copies:
            cp.wait()

    return pl.pallas_call(
        body,
        out_shape=jax.ShapeDtypeStruct((n,) + x.shape, x.dtype),
        in_specs=[pl.BlockSpec(memory_space=pltpu.VMEM)],
        out_specs=pl.BlockSpec(memory_space=pltpu.VMEM),
        scratch_shapes=[pltpu.SemaphoreType.DMA((n,)), pltpu.SemaphoreType.DMA((n,))],
        compiler_params=pltpu.CompilerParams(collective_id=cid, has_side_effects=True),
        name="share_plan",
    )(x)


def route_z(own, pair, pos):
    n_mig = own.shape[0]

    def body(own_ref, pair_ref, pos_ref, z_ref, cnt):
        row, core = pos_ref[0], pos_ref[1] & 1

        @pl.loop(0, 3 * Z_CORE)
        def _(i):
            z_ref[i] = 0

        for i in range(4):
            cnt[i] = 0

        @pl.loop(0, 2 * n_mig)
        def _(i):
            second = (i >= n_mig).astype(jnp.int32)
            e = i - second * n_mig
            mine = second == core
            dd = jnp.where(mine, own_ref[e], pair_ref[e])
            di = dd >> 2
            k = cnt[di]
            cnt[di] = k + 1
            shift = (di - row) & 3

            @pl.when((shift != 0) & ((k & 1) == core) & (k < 2 * Z_CORE))
            def _():
                z_ref[(shift - 1) * Z_CORE + (k >> 1)] = jnp.where(mine, e, n_mig + e)

    smem = pl.BlockSpec(memory_space=pltpu.SMEM)
    return pl.pallas_call(
        body,
        out_shape=jax.ShapeDtypeStruct((64,), jnp.int32),
        in_specs=[smem] * 3,
        out_specs=smem,
        scratch_shapes=[pltpu.SMEM((4,), jnp.int32)],
        name="route_z",
    )(own, pair, pos)


def route(dst, dev, pos, n_mig, n_slots):
    n_dev = dev.shape[0] // n_mig
    z_at, y_at = 2 * n_mig, 2 * n_mig + 2 * 3 * Z_CORE

    def body(dst_ref, dev_ref, pos_ref, y_ref, s_ref, cnt, cnt2):
        row, colm = pos_ref[0], pos_ref[1]
        half, core = colm >> 1, colm & 1
        me = row * 4 + colm

        @pl.loop(0, 64)
        def _(i):
            y_ref[i] = 0
            s_ref[i] = -1
            cnt[i] = 0

        @pl.loop(0, 8)
        def _(i):
            cnt2[i] = 0

        @pl.loop(0, n_dev)
        def _(d):
            si, sy, sc = d >> 2, (d >> 1) & 1, d & 1

            @pl.loop(0, n_mig)
            def _(e):
                dd = dev_ref[d * n_mig + e]
                di, dy = dd >> 2, (dd >> 1) & 1
                c1 = (d >> 1) * 4 + di
                k = cnt[c1]
                cnt[c1] = k + 1
                cross = (dy != sy).astype(jnp.int32)
                c2 = di * 2 + sy
                k2 = cnt2[c2]
                cnt2[c2] = k2 + cross

                @pl.when(di == row)
                def _():
                    shift = (di - si) & 3
                    at = jnp.where(sc == core, e, n_mig + e)
                    z_slot = (shift - 1) * Z_CORE + (k >> 1)
                    here = jnp.where(shift == 0, at, z_at + z_slot + jnp.where((k & 1) == core, 0, 3 * Z_CORE))

                    @pl.when((sy == half) & (cross == 1) & ((k2 & 1) == core) & (k2 < 2 * Y_CORE))
                    def _():
                        y_ref[k2 >> 1] = jnp.minimum(here, y_at - 1)

                    @pl.when(dd == me)
                    def _():
                        by_y = y_at + (k2 >> 1) + jnp.where((k2 & 1) == core, 0, Y_CORE)
                        s_ref[dst_ref[d * n_mig + e] - me * n_slots] = jnp.where(cross == 1, by_y, here)

    smem = pl.BlockSpec(memory_space=pltpu.SMEM)
    return pl.pallas_call(
        body,
        out_shape=[jax.ShapeDtypeStruct((64,), jnp.int32)] * 2,
        in_specs=[smem] * 3,
        out_specs=[smem] * 2,
        scratch_shapes=[pltpu.SMEM((64,), jnp.int32), pltpu.SMEM((8,), jnp.int32)],
        cost_estimate=pl.CostEstimate(flops=100_000_000, bytes_accessed=1_000_000, transcendentals=0),
        name="route",
    )(dst, dev, pos)


def around(me):
    sib = me + 1 - 2 * lax.rem(me, 2)
    over = lax.rem(me + 2, 4)
    return sib, over, lax.rem(sib + 2, 4)


def enter(axis, peers):
    barrier = pltpu.get_barrier_semaphore()
    for p in peers:
        pl.semaphore_signal(barrier, inc=1, device_id={axis: p}, device_id_type=MESH_ID)
    pl.semaphore_wait(barrier, len(peers))


def gather_rows(x, axis, n, cid):
    def body(x_ref, o_ref, send_sem, recv_sem):
        me = lax.axis_index(axis)
        sib, over, _ = around(me)
        enter(axis, (sib, over))

        def send(src, at, peer, i):
            return pltpu.make_async_remote_copy(
                src_ref=src, dst_ref=o_ref.at[at], send_sem=send_sem.at[i], recv_sem=recv_sem.at[i],
                device_id={axis: peer}, device_id_type=MESH_ID)

        cross, near = send(x_ref, me, over, 0), send(x_ref, me, sib, 1)
        cross.start()
        near.start()
        o_ref[me] = x_ref[...]
        cross.wait()
        hand = send(o_ref.at[over], over, sib, 2)
        hand.start()
        near.wait()
        hand.wait()

    return pl.pallas_call(
        body,
        out_shape=jax.ShapeDtypeStruct((n,) + x.shape, x.dtype),
        in_specs=[pl.BlockSpec(memory_space=pltpu.VMEM)],
        out_specs=pl.BlockSpec(memory_space=pltpu.VMEM),
        scratch_shapes=[pltpu.SemaphoreType.DMA((3,)), pltpu.SemaphoreType.DMA((3,))],
        compiler_params=pltpu.CompilerParams(collective_id=cid, has_side_effects=True),
        cost_estimate=pl.CostEstimate(flops=1_000_000_000, bytes_accessed=2_000_000, transcendentals=0),
        name="gather_rows",
    )(x)


def combine(acc, ml, axis, n, cid):
    rows, r, hd = acc.shape
    b = rows // n

    def body(acc_ref, ml_ref, o_ref, sib_me, sib_over, ml_sib, to_over, ml_to, y_acc, ml_y, send_sem, recv_sem):
        me = lax.axis_index(axis)
        sib, over, diag = around(me)
        enter(axis, (sib, over))

        def send(src, dst, peer, i):
            return pltpu.make_async_remote_copy(
                src_ref=src, dst_ref=dst, send_sem=send_sem.at[i], recv_sem=recv_sem.at[i],
                device_id={axis: peer}, device_id_type=MESH_ID)

        near = [send(acc_ref.at[pl.ds(diag * b, b)], sib_over, sib, 0), send(ml_ref, ml_sib, sib, 1),
                send(acc_ref.at[pl.ds(sib * b, b)], sib_me, sib, 2)]
        for cp in near:
            cp.start()
        near[0].wait()
        near[1].wait()
        lane = lax.broadcasted_iota(jnp.int32, (r, ml_ref.shape[2]), 1)

        def pick(t, s):
            return jnp.sum(jnp.where(lane == s, t, 0.0), axis=1, keepdims=True)

        top = jnp.maximum(ml_ref[0], ml_sib[0])
        w_own, w_sib = jnp.exp(ml_ref[0] - top), jnp.exp(ml_sib[0] - top)
        tot = w_own * ml_ref[1] + w_sib * ml_sib[1]
        ml_to[0] = top
        ml_to[1] = tot
        for i in range(b):
            s = over * b + i
            to_over[i] = pick(w_own, s) * acc_ref[s] + pick(w_sib, s) * sib_over[i]
        far = [send(to_over, y_acc, over, 3), send(ml_to, ml_y, over, 4)]
        for cp in far:
            cp.start()
        near[2].wait()
        far[1].wait()
        last = jnp.maximum(top, ml_y[0])
        f, g = jnp.exp(top - last), jnp.exp(ml_y[0] - last)
        den = f * tot + g * ml_y[1]
        f, g = f / den, g / den
        w_own, w_sib = f * w_own, f * w_sib
        for i in range(b):
            s = me * b + i
            sib_me[i] = pick(w_own, s) * acc_ref[s] + pick(w_sib, s) * sib_me[i]
        far[0].wait()
        for i in range(b):
            o_ref[i] = (sib_me[i] + pick(g, me * b + i) * y_acc[i]).astype(o_ref.dtype)

    block = pltpu.VMEM((b, r, hd), jnp.float32)
    stats = pltpu.VMEM(ml.shape, jnp.float32)
    return pl.pallas_call(
        body,
        out_shape=jax.ShapeDtypeStruct((b, r, hd), jnp.bfloat16),
        in_specs=[pl.BlockSpec(memory_space=pltpu.VMEM)] * 2,
        out_specs=pl.BlockSpec(memory_space=pltpu.VMEM),
        scratch_shapes=[block, block, stats, block, stats, block, stats,
                        pltpu.SemaphoreType.DMA((5,)), pltpu.SemaphoreType.DMA((5,))],
        compiler_params=pltpu.CompilerParams(collective_id=cid, has_side_effects=True),
        cost_estimate=pl.CostEstimate(flops=1_000_000_000, bytes_accessed=2_000_000, transcendentals=0),
        name="combine",
    )(acc, ml)


def mlp_pair(attn, hidden, w_out, w_up, w_down, w_next, layer, cid):
    rows, d = attn.shape
    ff = w_up.shape[2]
    r = -(-rows // 32) * 32
    tile = 512
    d_half, f_half = d // 2, ff // 2
    n_o, n_f = d_half // tile, f_half // tile
    ring_c, ring_r = 8, 6
    halves = [w.shape[2] // 2 for w in w_next]
    parts = [(w, t * tile) for w, h in enumerate(halves) for t in range(h // tile)]
    n_p, p_half = len(parts), sum(halves)
    attn, hidden = (jnp.pad(t, ((0, r - rows), (0, 0))) for t in (attn, hidden))

    def body(attn_ref, hid_ref, wo_ref, wu_ref, wd_ref, *rest):
        wn_refs, rest = rest[:len(w_next)], rest[len(w_next):]
        o_ref, rest = rest[0], rest[1:]
        if n_p:
            p_ref, p_to, p_in, rest = rest[0], rest[1], rest[2], rest[3:]
        x_all, h_all, hm, act, acc, rx, wc, wr, csem, rsem, ssem, qsem = rest
        me = lax.axis_index('kv')
        core = lax.rem(me, 2)
        peer = me + 1 - 2 * core
        mine, other = pl.ds(core * r, r), pl.ds((1 - core) * r, r)

        def col(c, is_out):
            if is_out:
                src = wo_ref.at[layer, :, pl.ds(pl.multiple_of(core * d_half + c * tile, tile), tile)]
            else:
                src = wu_ref.at[layer, :, pl.ds(pl.multiple_of(core * f_half + (c - n_o) * tile, tile), tile)]
            slot = lax.rem(c, ring_c)
            return pltpu.make_async_copy(src, wc.at[slot], csem.at[slot])

        def proj(p):
            w, lo = parts[p]
            src = wn_refs[w].at[layer + 1, :, pl.ds(pl.multiple_of(core * halves[w] + lo, tile), tile)]
            slot = (n_o + n_f + p) % ring_c
            return pltpu.make_async_copy(src, wc.at[slot], csem.at[slot])

        def row(j):
            slot = lax.rem(j, ring_r)
            src = wd_ref.at[layer, pl.ds(pl.multiple_of(core * f_half + j * tile, tile), tile), :]
            return pltpu.make_async_copy(src, wr.at[slot], rsem.at[slot])

        for c in range(ring_c):
            col(c, c < n_o).start()

        barrier = pltpu.get_barrier_semaphore()
        pl.semaphore_signal(barrier, inc=1, device_id={'kv': peer}, device_id_type=MESH_ID)
        pl.semaphore_wait(barrier, 1)

        def send(src, dst, i):
            return pltpu.make_async_remote_copy(
                src_ref=src, dst_ref=dst, send_sem=ssem.at[i], recv_sem=qsem.at[i],
                device_id={'kv': peer}, device_id_type=MESH_ID)

        swaps = [send(attn_ref, x_all.at[mine], 0), send(hid_ref, h_all.at[mine], 1)]
        for cp in swaps:
            cp.start()
        x_all[mine] = attn_ref[...]
        h_all[mine] = hid_ref[...]
        for cp in swaps:
            cp.wait()

        @pl.loop(0, n_o)
        def _(c):
            col(c, True).wait()
            at = pl.ds(pl.multiple_of(core * d_half + c * tile, tile), tile)
            part = jnp.dot(x_all[...], wc[lax.rem(c, ring_c)], preferred_element_type=jnp.float32)
            hm[:, at] = (h_all[:, at].astype(jnp.float32) + part).astype(jnp.bfloat16)

            @pl.when(c + ring_c < n_o + n_f)
            def _():
                col(c + ring_c, False).start()

        own_cols = pl.ds(pl.multiple_of(core * d_half, tile), d_half)
        cp = send(hm.at[:, own_cols], hm.at[:, own_cols], 2)
        cp.start()
        acc[...] = jnp.zeros_like(acc)
        cp.wait()

        @pl.loop(0, n_f)
        def _(j):
            c = j + n_o
            col(c, False).wait()
            up = jnp.dot(hm[...], wc[lax.rem(c, ring_c)], preferred_element_type=jnp.float32)
            act[:, pl.ds(pl.multiple_of(j * tile, tile), tile)] = jax.nn.gelu(up).astype(jnp.bfloat16)

            @pl.when(c + ring_c < n_o + n_f)
            def _():
                col(c + ring_c, False).start()

            for p in range(n_p):
                @pl.when(c + ring_c == n_o + n_f + p)
                def _():
                    proj(p).start()

            @pl.when(j < ring_r)
            def _():
                row(j).start()

        @pl.loop(0, n_f)
        def _(j):
            row(j).wait()
            acc[...] += jnp.dot(act[:, pl.ds(pl.multiple_of(j * tile, tile), tile)], wr[lax.rem(j, ring_r)],
                                preferred_element_type=jnp.float32)

            @pl.when(j + ring_r < n_f)
            def _():
                row(j + ring_r).start()

        cp = send(acc.at[other], rx, 3)
        cp.start()
        cp.wait()
        o_ref[...] = (hm[mine].astype(jnp.float32) + (acc[mine] + rx[...])).astype(o_ref.dtype)
        if not n_p:
            return
        cp = send(o_ref, x_all.at[mine], 4)
        cp.start()
        x_all[mine] = o_ref[...]
        cp.wait()
        at = 0
        for p in range(n_p):
            w, lo = parts[p]
            proj(p).wait()
            res = jnp.dot(x_all[...], wc[(n_o + n_f + p) % ring_c], preferred_element_type=jnp.float32).astype(jnp.bfloat16)
            first = 2 * sum(halves[:w])
            acc_at = pl.ds(pl.multiple_of(first + core * halves[w] + lo, tile), tile)

            @pl.when(core == 0)
            def _():
                p_ref[:, acc_at] = res[:r]
                p_to[:, at:at + tile] = res[r:]

            @pl.when(core == 1)
            def _():
                p_ref[:, acc_at] = res[r:]
                p_to[:, at:at + tile] = res[:r]

            at += tile
        cp = send(p_to, p_in, 5)
        cp.start()
        cp.wait()
        at = 0
        for w, lo in parts:
            first = 2 * sum(halves[:w])
            p_ref[:, pl.ds(pl.multiple_of(first + (1 - core) * halves[w] + lo, tile), tile)] = p_in[:, at:at + tile]
            at += tile

    vmem, any_spec = pl.BlockSpec(memory_space=pltpu.VMEM), pl.BlockSpec(memory_space=pl.ANY)
    out_shape = [jax.ShapeDtypeStruct((r, d), jnp.bfloat16)]
    extra = []
    if n_p:
        out_shape.append(jax.ShapeDtypeStruct((r, 2 * p_half), jnp.bfloat16))
        extra = [pltpu.VMEM((r, p_half), jnp.bfloat16)] * 2
    out = pl.pallas_call(
        body,
        out_shape=out_shape,
        in_specs=[vmem, vmem] + [any_spec] * (3 + len(w_next)),
        out_specs=[vmem] * len(out_shape),
        scratch_shapes=extra + [
            pltpu.VMEM((2 * r, d), jnp.bfloat16), pltpu.VMEM((2 * r, d), jnp.bfloat16), pltpu.VMEM((2 * r, d), jnp.bfloat16),
            pltpu.VMEM((2 * r, f_half), jnp.bfloat16), pltpu.VMEM((2 * r, d), jnp.float32), pltpu.VMEM((r, d), jnp.float32),
            pltpu.VMEM((ring_c, d, tile), jnp.bfloat16), pltpu.VMEM((ring_r, tile, d), jnp.bfloat16),
            pltpu.SemaphoreType.DMA((ring_c,)), pltpu.SemaphoreType.DMA((ring_r,)),
            pltpu.SemaphoreType.DMA((6,)), pltpu.SemaphoreType.DMA((6,)),
        ],
        compiler_params=pltpu.CompilerParams(collective_id=cid, has_side_effects=True, vmem_limit_bytes=58 * 1024 * 1024),
        cost_estimate=pl.CostEstimate(flops=6_000_000_000, bytes_accessed=60_000_000, transcendentals=0),
    )(attn, hidden, w_out, w_up, w_down, *w_next)
    return [t[:rows] for t in out]


def attend(info, counts, qkv, pools_in, unit_srcs, first_unit, prev_pools, state, layer, part, n_slots, layers, page, kvh, q_group, hd):
    sources = list(pools_in) + list(unit_srcs)
    n_pool = len(pools_in)
    prow = page * kvh
    qr = 2 * kvh * q_group
    n_seq = qkv.shape[0]
    scale = hd ** -0.5
    aliased = prev_pools is not None
    carried = state is not None

    def body(info_ref, cnt_ref, qkv_ref, *rest):
        ins, rest = rest[:len(sources)], rest[len(sources):]
        if aliased:
            rest = rest[2:]
        if carried:
            acc_prev, ml_prev = rest[:2]
            rest = rest[2:]
        k_out, v_out, acc_ref, ml_ref, kbuf, vbuf, isem, osem = rest
        lo = cnt_ref[2 * part - 1] if part else 0
        mid = cnt_ref[2 * part]
        hi = cnt_ref[2 * part + 1]

        def load_from(k_page, v_page, i):
            return (pltpu.make_async_copy(k_page, kbuf.at[i], isem.at[0, i]),
                    pltpu.make_async_copy(v_page, vbuf.at[i], isem.at[1, i]))

        def from_pool(i):
            at = info_ref[0, i] * layers + layer
            return load_from(ins[0].at[at], ins[1].at[at], i)

        def loads(i):
            if n_pool:
                return from_pool(i)
            return load_from(ins[0].at[0, pl.ds(0, prow)], ins[0].at[0, pl.ds(prow, prow)], i)

        def start_loads(i):
            at, first = info_ref[3, i], first_unit
            if n_pool and unit_srcs:
                pl.when(at < 0)(lambda: [cp.start() for cp in from_pool(i)] and None)
            elif n_pool:
                for cp in from_pool(i):
                    cp.start()
            for ref in ins[n_pool:]:
                last = first + ref.shape[0]

                @pl.when((at >= first) & (at < last))
                def _():
                    u = at - first
                    for cp in load_from(ref.at[u, pl.ds(0, prow)], ref.at[u, pl.ds(prow, prow)], i):
                        cp.start()

                first = last

        def stores(i):
            slot = info_ref[0, i]
            return (pltpu.make_async_copy(kbuf.at[i], k_out.at[slot * layers + layer], osem.at[0, i]),
                    pltpu.make_async_copy(vbuf.at[i], v_out.at[slot * layers + layer], osem.at[1, i]))

        @pl.loop(lo, hi)
        def _(i):
            start_loads(i)

        if carried:
            acc_ref[...] = acc_prev[...]
            ml_ref[...] = ml_prev[...]
        else:
            acc_ref[...] = jnp.zeros_like(acc_ref)
            ml_ref[0] = jnp.full(ml_ref.shape[1:], NEG, jnp.float32)
            ml_ref[1] = jnp.zeros(ml_ref.shape[1:], jnp.float32)

        col = lax.broadcasted_iota(jnp.int32, (qr, prow), 1)
        row = lax.broadcasted_iota(jnp.int32, (qr, prow), 0)
        late = (row >= kvh * q_group).astype(jnp.int32)
        head_ok = lax.rem(col, kvh) == (row - late * (kvh * q_group)) // q_group
        need = col // kvh - late
        need = jnp.where(head_ok, need, 1 << 20)
        lane = lax.broadcasted_iota(jnp.int32, ml_ref.shape[1:], 1)
        wrow = lax.broadcasted_iota(jnp.int32, (4 * kvh, hd), 0) // kvh

        @pl.loop(0, (mid - lo + UNROLL - 1) // UNROLL)
        def _(g):
            base = lo + g * UNROLL
            idx, seqs, offs = [], [], []
            for u in range(UNROLL):
                i = base + u
                live = i < mid
                j = jnp.minimum(i, mid - 1)
                idx.append(j)
                seqs.append(jnp.where(live, info_ref[1, j], n_seq))
                offs.append(info_ref[2, j])

                @pl.when(live)
                def _():
                    for cp in loads(j):
                        cp.wait()

            for j, seq, off in zip(idx, seqs, offs):
                w = jnp.minimum(off // 2, page // 2 - 2)
                at = pl.ds(pl.multiple_of(w * (2 * kvh), 2 * kvh), 4 * kvh)
                tok = wrow + 2 * w
                seq = jnp.minimum(info_ref[1, j], n_seq - 1)
                for buf, r0 in ((kbuf, qr), (vbuf, qr + 2 * kvh)):
                    new = qkv_ref[seq, r0:r0 + 2 * kvh, :].astype(jnp.float32)
                    first = jnp.concatenate([new[:kvh]] * 4, axis=0)
                    second = jnp.concatenate([new[kvh:]] * 4, axis=0)
                    old = buf[j, at, :].astype(jnp.float32)
                    old = jnp.where(tok == off, first, jnp.where(tok == off + 1, second, old))
                    buf[j, at, :] = old.astype(jnp.bfloat16)

            res = []
            for u in range(UNROLL):
                q = qkv_ref[jnp.minimum(seqs[u], n_seq - 1), :qr, :]
                s = lax.dot_general(q, kbuf[idx[u]], (((1,), (1,)), ((), ())), preferred_element_type=jnp.float32) * scale
                s = jnp.where(need <= offs[u], s, NEG)
                m = jnp.max(s, axis=1, keepdims=True)
                p = jnp.exp(s - m)
                l = jnp.sum(p, axis=1, keepdims=True)
                o = jnp.dot(p.astype(jnp.bfloat16), vbuf[idx[u]], preferred_element_type=jnp.float32)
                res.append((m, l, o))
            for u in range(UNROLL):
                m, l, o = res[u]
                sel = lane == seqs[u]
                m_all, l_all = ml_ref[0], ml_ref[1]
                m_old = jnp.max(jnp.where(sel, m_all, NEG), axis=1, keepdims=True)
                m_new = jnp.maximum(m_old, m)
                alpha = jnp.exp(m_old - m_new)
                beta = jnp.exp(m - m_new)
                acc_ref[seqs[u]] = acc_ref[seqs[u]] * alpha + o * beta
                ml_ref[0] = jnp.where(sel, m_new, m_all)
                ml_ref[1] = jnp.where(sel, l_all * alpha + l * beta, l_all)
            for u in range(UNROLL):
                @pl.when(base + u < mid)
                def _():
                    for cp in stores(base + u):
                        cp.start()

        @pl.loop(mid, hi)
        def _(i):
            for cp in loads(i):
                cp.wait()
            for cp in stores(i):
                cp.start()

        @pl.loop(lo, hi)
        def _(i):
            for cp in stores(i):
                cp.wait()

    any_spec = pl.BlockSpec(memory_space=pl.ANY)
    vmem = pl.BlockSpec(memory_space=pltpu.VMEM)
    smem = pl.BlockSpec(memory_space=pltpu.SMEM)
    operands = [info, counts, qkv, *sources]
    specs = [smem, smem, vmem] + [any_spec] * len(sources)
    alias = {}
    if aliased:
        alias = {len(operands): 0, len(operands) + 1: 1}
        operands += list(prev_pools)
        specs += [any_spec, any_spec]
    if carried:
        operands += list(state)
        specs += [vmem, vmem]
    pool = jax.ShapeDtypeStruct((n_slots * layers, prow, hd), jnp.bfloat16)
    return pl.pallas_call(
        body,
        out_shape=[pool, pool,
                   jax.ShapeDtypeStruct((n_seq + 1, qr, hd), jnp.float32),
                   jax.ShapeDtypeStruct((2, qr, 128), jnp.float32)],
        in_specs=specs,
        out_specs=[any_spec, any_spec, vmem, vmem],
        scratch_shapes=[
            pltpu.VMEM((n_slots, prow, hd), jnp.bfloat16),
            pltpu.VMEM((n_slots, prow, hd), jnp.bfloat16),
            pltpu.SemaphoreType.DMA((2, n_slots)),
            pltpu.SemaphoreType.DMA((2, n_slots)),
        ],
        input_output_aliases=alias,
        cost_estimate=pl.CostEstimate(flops=400_000_000, bytes_accessed=16_000_000, transcendentals=0),
    )(*operands)


def solution(mesh):
    n_rows = mesh.shape['kv2']
    n_cols = mesh.shape['kv']
    dev_axes = ('rep', 'kv2', 'kv')
    seq_spec = P(None, dev_axes, None)
    pool_spec = P(dev_axes, None, None, None, None)
    table_spec = P(dev_axes, None)
    vec_spec = P(dev_axes)
    full_spec = P()

    def per_device(x_embed, w_query, w_key, w_value, w_out, w_up, w_down, k_pool, v_pool, old_table, seq_len, src_slot, dst_slot):
        n_slots, layers, page, kv_heads, head_dim = k_pool.shape
        heads = w_query.shape[2] // head_dim
        q_group = heads // kv_heads
        seq_dev = x_embed.shape[1]
        n_pages = old_table.shape[1]
        n_mig = src_slot.shape[0]
        n_dev = n_rows * n_cols
        row_seqs = seq_dev * n_cols
        prow = page * kv_heads
        width = x_embed.shape[2]
        me_row, me_col = lax.axis_index('kv2'), lax.axis_index('kv')
        me = me_row * n_cols + me_col
        base = me * n_slots

        k_rows = k_pool.reshape(n_slots * layers, prow, head_dim)
        v_rows = v_pool.reshape(n_slots * layers, prow, head_dim)
        pair = [(c, c ^ 1) for c in range(n_cols)]
        over = [(c, c ^ 2) for c in range(n_cols)]
        z_hops = [[(r, (r + s) % n_rows) for r in range(n_rows)] for s in range(1, n_rows)]
        pos = jnp.stack([me_row, me_col]).astype(jnp.int32)
        dev_own = dst_slot // n_slots
        leaving = take_pages((src_slot - base) * layers, k_rows, v_rows, layers)
        units = [[leaving[0], lax.ppermute(leaving[0], 'kv', pair)]]
        dev_pair = lax.ppermute(dev_own, 'kv', pair)

        n_rep = mesh.shape['rep']
        words = [src_slot, dst_slot, dst_slot // n_slots, old_table.reshape(-1), seq_len]
        cuts = [0]
        for w in words:
            cuts.append(cuts[-1] + w.shape[0])
        meta = jnp.pad(jnp.concatenate(words), (0, 128 - cuts[-1])).reshape(1, 128)
        meta_all = share_plan(meta, (n_rep, n_rows, n_cols), 2).reshape(n_rep, n_dev, 128)

        meta_all, pos = lax.optimization_barrier((meta_all, pos))
        z_list = route_z(dev_own, dev_pair, pos)
        hops = pick(z_list, units[0], [Z_CORE] * (n_rows - 1))
        hops, z_list, hidden, meta_all, later = lax.optimization_barrier(
            (hops, z_list, x_embed.reshape(2 * seq_dev, width), meta_all, leaving[1:]))
        units += [[own, lax.ppermute(own, 'kv', pair)] for own in later]

        meta = lax.dynamic_index_in_dim(meta_all, lax.axis_index('rep'), 0, keepdims=False)
        src_all, dst_all, dev_all = (meta[:, cuts[t]:cuts[t + 1]].reshape(-1) for t in range(3))
        row_meta = lax.dynamic_slice_in_dim(meta, me_row * n_cols, n_cols, axis=0)
        row_table = row_meta[:, cuts[3]:cuts[4]].reshape(-1)
        row_len = row_meta[:, cuts[4]:cuts[5]].reshape(-1)

        dev_by = meta_all[:, :, cuts[2]:cuts[3]]
        to_row = dev_by // n_cols
        rows4 = jnp.arange(n_rows, dtype=jnp.int32)
        goes = (to_row[..., None] == rows4).astype(jnp.int32).sum(axis=2)
        per_chip = goes.reshape(n_rep, n_rows, n_cols // 2, 2, n_rows).sum(axis=3)
        leaves = rows4[:, None] != rows4[None, :]
        z_full = ((per_chip > 2 * Z_CORE) & leaves[None, :, None, :]).any()
        side = (jnp.arange(n_dev, dtype=jnp.int32) // 2 % 2)[None, :, None]
        crosses = dev_by // 2 % 2 != side
        per_side = ((to_row[..., None] == rows4) & crosses[..., None]).astype(jnp.int32).sum(axis=2)
        y_full = (per_side.reshape(n_rep, n_rows, n_cols // 2, 2, n_rows).sum(axis=(1, 3)) > 2 * Y_CORE).any()
        full = z_full | y_full

        y_list, unit_of = route(dst_all, dev_all, pos, n_mig, n_slots)

        def along_z(hops):
            got = []
            for h, z in zip(hops, z_hops):
                got.append(lax.ppermute(h, 'kv2', z))
            return got

        def swap(units, got):
            return units + got + [lax.ppermute(g, 'kv', pair) for g in got]

        def along_y(hop):
            got = lax.ppermute(hop, 'kv', over)
            return [got, lax.ppermute(got, 'kv', pair)]

        same = row_table[:, None] == src_all[None, :]
        new_table = jnp.where(same.any(axis=1), jnp.sum(jnp.where(same, dst_all[None, :], 0), axis=1), row_table)
        slots = jnp.arange(n_slots, dtype=jnp.int32)
        cells = jnp.arange(row_seqs * n_pages, dtype=jnp.int32)
        slot_cell = jnp.max(jnp.where(new_table[None, :] == (slots + base)[:, None], cells[None, :], -1), axis=1)
        moves = jnp.arange(n_dev * n_mig, dtype=jnp.int32)
        move_of = jnp.max(jnp.where(dst_all[None, :] == (slots + base)[:, None], moves[None, :], -1), axis=1)
        is_mig = move_of >= 0
        used = slot_cell >= 0
        seq_of = jnp.where(used, slot_cell // n_pages, row_seqs)
        seq_one = seq_of[:, None] == jnp.arange(row_seqs, dtype=jnp.int32)[None, :]
        len_of = jnp.sum(jnp.where(seq_one, row_len[None, :], 0), axis=1)
        off_of = len_of - (slot_cell % n_pages) * page
        off_of = jnp.where(used & (off_of >= 0) & (off_of < page), off_of, 2 * page)
        y_at = 2 * n_mig + 2 * (n_rows - 1) * Z_CORE
        unit = jnp.where(is_mig, jnp.where(full, slots + y_at + 2 * Y_CORE, unit_of[:n_slots]), -1)

        def lists(cls, n_cls):
            key = cls * 2 + (~used).astype(jnp.int32)
            order = key * n_slots + slots
            at = jnp.sum((order[None, :] < order[:, None]).astype(jnp.int32), axis=1)
            place = at[None, :] == jnp.arange(64, dtype=jnp.int32)[:, None]
            info = jnp.stack([jnp.sum(jnp.where(place, t[None, :], 0), axis=1) for t in (slots, seq_of, off_of, unit)])
            counts = jnp.sum((key[None, :] <= jnp.arange(2 * n_cls, dtype=jnp.int32)[:, None]).astype(jnp.int32), axis=1)
            return info, counts

        by_class = lists(is_mig.astype(jnp.int32) + (unit >= y_at).astype(jnp.int32), 3)
        by_use = lists(jnp.zeros_like(slots), 1)

        def all_pages(layer):
            def collect():
                every = lax.all_gather(leaving[layer], ('kv2', 'kv'), tiled=True)
                return pick(jnp.maximum(move_of, 0), [every], [n_slots])[0]

            return lax.cond(full, collect, lambda: uninit((n_slots, 2 * prow, head_dim), jnp.bfloat16))

        pools = None
        got = along_z(hops)
        for layer in range(layers):
            dot = lambda a, w: jnp.dot(a, w[layer], preferred_element_type=jnp.float32)
            if layer == 0:
                parts = [dot(hidden, w).astype(jnp.bfloat16) for w in (w_query, w_key, w_value)]
            else:
                parts = jnp.split(ahead, [heads * head_dim, (heads + kv_heads) * head_dim], axis=1)
            query, k_new, v_new = (t.reshape(2, seq_dev, -1, head_dim) for t in parts)
            per_seq = lambda t: jnp.swapaxes(t, 0, 1).reshape(seq_dev, -1, head_dim)
            qkv = jnp.concatenate([per_seq(query), per_seq(k_new), per_seq(v_new)], axis=1)
            qkv = gather_rows(qkv, 'kv', n_cols, 0).reshape(row_seqs, -1, head_dim)
            dims = dict(layer=layer, n_slots=n_slots, layers=layers, page=page, kvh=kv_heads, q_group=q_group, hd=head_dim)
            if layer == 0:
                *pools, acc, ml = attend(*by_class, qkv, [k_rows, v_rows], [], 0, pools, None, part=0, **dims)
                next_hops = pick(z_list, units[1], [Z_CORE] * (n_rows - 1))
                got, acc, next_hops, by_use = lax.optimization_barrier((got, acc, next_hops, by_use))
                next_got = along_z(next_hops)
                all_units = swap(units[0], got)
                hop, = pick(y_list, all_units, [Y_CORE])
                last = along_y(hop) + [all_pages(0)]
                *pools, acc, ml = attend(*by_class, qkv, [], all_units, 0, pools, (acc, ml), part=1, **dims)
                *pools, acc, ml = attend(*by_class, qkv, [], last, y_at, pools, (acc, ml), part=2, **dims)
            else:
                srcs = all_units + along_y(hop) + [all_pages(layer)]
                *pools, acc, ml = attend(*by_use, qkv, [k_rows, v_rows], srcs, 0, pools, None, part=0, **dims)
            o = combine(acc, ml, 'kv', n_cols, 1)
            if layer + 1 < layers:
                next_got, o = lax.optimization_barrier((next_got, o))
                all_units = swap(units[layer + 1], next_got)
                hop, = pick(y_list, all_units, [Y_CORE])
                hop, o = lax.optimization_barrier((hop, o))
            attn_out = jnp.swapaxes(o.reshape(seq_dev, 2, heads * head_dim), 0, 1).reshape(2 * seq_dev, heads * head_dim)
            w_next = (w_query, w_key, w_value) if layer + 1 < layers else ()
            hidden, *ahead = mlp_pair(attn_out, hidden, w_out, w_up, w_down, w_next, layer, 3 + layer)
            ahead = ahead[0] if ahead else None
        k_out, v_out = (p.reshape(k_pool.shape) for p in pools)
        return hidden.reshape(2, seq_dev, width), k_out, v_out

    return jax.shard_map(per_device, mesh=mesh, in_specs=(seq_spec, full_spec, full_spec, full_spec, full_spec, full_spec, full_spec, pool_spec, pool_spec, table_spec, vec_spec, vec_spec, vec_spec), out_specs=(seq_spec, pool_spec, pool_spec), check_vma=False)
```

```python
import jax
import jax.numpy as jnp
from jax import lax
from jax.experimental import pallas as pl
from jax.experimental.pallas import tpu as pltpu
from jax.sharding import PartitionSpec as P


MESH_ID = pl.DeviceIdType.MESH
NEG = -1e30
UNROLL = 4
Z_CORE = 6
Y_CORE = 10


def cost(flops, size):
    return pl.CostEstimate(flops=flops, bytes_accessed=size, transcendentals=0)


SMALL = cost(100_000_000, 4_000_000)


def around(me):
    sib = me + 1 - 2 * lax.rem(me, 2)
    over = lax.rem(me + 2, 4)
    return sib, over, lax.rem(sib + 2, 4)


def uninit(shape, dtype):
    def body(o_ref):
        pass

    return pl.pallas_call(
        body, out_shape=jax.ShapeDtypeStruct(shape, dtype), out_specs=pl.BlockSpec(memory_space=pl.ANY), name="uninit")()


def take_pages(rows, k_rows, v_rows, layers):
    m = rows.shape[0]
    prow, hd = k_rows.shape[1:]

    def body(rows_ref, k_in, v_in, *rest):
        outs, (buf, isem, osem) = rest[:layers], rest[layers:]
        ins, puts = [], []
        for layer in range(layers):
            for i in range(m):
                for which, ref in enumerate((k_in, v_in)):
                    cp = pltpu.make_async_copy(
                        ref.at[rows_ref[i] + layer], buf.at[layer, i, pl.ds(which * prow, prow)], isem.at[layer, 2 * i + which])
                    cp.start()
                    ins.append(cp)
        for layer in range(layers):
            for cp in ins[layer * 2 * m:(layer + 1) * 2 * m]:
                cp.wait()
            cp = pltpu.make_async_copy(buf.at[layer], outs[layer], osem.at[layer])
            cp.start()
            puts.append(cp)
        for cp in puts:
            cp.wait()

    any_spec = pl.BlockSpec(memory_space=pl.ANY)
    return pl.pallas_call(
        body,
        out_shape=[jax.ShapeDtypeStruct((m, 2 * prow, hd), k_rows.dtype)] * layers,
        in_specs=[pl.BlockSpec(memory_space=pltpu.SMEM), any_spec, any_spec],
        out_specs=[any_spec] * layers,
        scratch_shapes=[pltpu.VMEM((layers, m, 2 * prow, hd), k_rows.dtype),
                        pltpu.SemaphoreType.DMA((layers, 2 * m)), pltpu.SemaphoreType.DMA((layers,))],
        cost_estimate=SMALL,
        name="take_pages",
    )(rows, k_rows, v_rows)


def pick(lists, sources, splits):
    n = sum(splits)
    tail, dtype = sources[0].shape[1:], sources[0].dtype

    def body(idx_ref, *rest):
        ins, outs, (buf, isem, osem) = rest[:len(sources)], rest[len(sources):-3], rest[-3:]

        @pl.loop(0, n)
        def _(i):
            at, lo = idx_ref[i], 0
            for ref in ins:
                hi = lo + ref.shape[0]

                @pl.when((at >= lo) & (at < hi))
                def _():
                    pltpu.make_async_copy(ref.at[at - lo], buf.at[i], isem.at[i]).start()

                lo = hi

        @pl.loop(0, n)
        def _(i):
            pltpu.make_async_copy(ins[0].at[0], buf.at[i], isem.at[i]).wait()

        puts, lo = [], 0
        for j, size in enumerate(splits):
            cp = pltpu.make_async_copy(buf.at[pl.ds(lo, size)], outs[j], osem.at[j])
            cp.start()
            puts.append(cp)
            lo += size
        for cp in puts:
            cp.wait()

    any_spec = pl.BlockSpec(memory_space=pl.ANY)
    return pl.pallas_call(
        body,
        out_shape=[jax.ShapeDtypeStruct((size,) + tail, dtype) for size in splits],
        in_specs=[pl.BlockSpec(memory_space=pltpu.SMEM)] + [any_spec] * len(sources),
        out_specs=[any_spec] * len(splits),
        scratch_shapes=[pltpu.VMEM((n,) + tail, dtype), pltpu.SemaphoreType.DMA((n,)), pltpu.SemaphoreType.DMA((len(splits),))],
        cost_estimate=SMALL,
    )(lists, *sources)


def share_plan(x, mesh_shape, cid):
    nx, ny, nz = mesh_shape
    n = nx * ny * nz

    def body(x_ref, o_ref, send_sem, recv_sem):
        me = (lax.axis_index('rep') * ny + lax.axis_index('kv2')) * nz + lax.axis_index('kv')

        def coords(d):
            p = lax.rem(me + d, n)
            return (p // (ny * nz), lax.rem(p // nz, ny), lax.rem(p, nz))

        barrier = pltpu.get_barrier_semaphore()
        for d in range(1, n):
            pl.semaphore_signal(barrier, inc=1, device_id=coords(d), device_id_type=MESH_ID)
        pl.semaphore_wait(barrier, n - 1)
        copies = []
        for d in range(1, n):
            cp = pltpu.make_async_remote_copy(
                src_ref=x_ref, dst_ref=o_ref.at[me], send_sem=send_sem.at[d], recv_sem=recv_sem.at[d],
                device_id=coords(d), device_id_type=MESH_ID)
            cp.start()
            copies.append(cp)
        o_ref[me] = x_ref[...]
        for cp in copies:
            cp.wait()

    return pl.pallas_call(
        body,
        out_shape=jax.ShapeDtypeStruct((n,) + x.shape, x.dtype),
        in_specs=[pl.BlockSpec(memory_space=pltpu.VMEM)],
        out_specs=pl.BlockSpec(memory_space=pltpu.VMEM),
        scratch_shapes=[pltpu.SemaphoreType.DMA((n,)), pltpu.SemaphoreType.DMA((n,))],
        compiler_params=pltpu.CompilerParams(collective_id=cid, has_side_effects=True),
        name="share_plan",
    )(x)


def route_z(own, pair, pos):
    n_mig = own.shape[0]

    def body(own_ref, pair_ref, pos_ref, z_ref, cnt):
        row, core = pos_ref[0], pos_ref[1] & 1

        @pl.loop(0, 3 * Z_CORE)
        def _(i):
            z_ref[i] = 0

        for i in range(4):
            cnt[i] = 0

        @pl.loop(0, 2 * n_mig)
        def _(i):
            second = (i >= n_mig).astype(jnp.int32)
            e = i - second * n_mig
            mine = second == core
            dd = jnp.where(mine, own_ref[e], pair_ref[e])
            di = dd >> 2
            k = cnt[di]
            cnt[di] = k + 1
            shift = (di - row) & 3

            @pl.when((shift != 0) & ((k & 1) == core) & (k < 2 * Z_CORE))
            def _():
                z_ref[(shift - 1) * Z_CORE + (k >> 1)] = jnp.where(mine, e, n_mig + e)

    smem = pl.BlockSpec(memory_space=pltpu.SMEM)
    return pl.pallas_call(
        body,
        out_shape=jax.ShapeDtypeStruct((64,), jnp.int32),
        in_specs=[smem] * 3,
        out_specs=smem,
        scratch_shapes=[pltpu.SMEM((4,), jnp.int32)],
        name="route_z",
    )(own, pair, pos)


def route(dst, dev, pos, n_mig, n_slots):
    n_dev = dev.shape[0] // n_mig
    z_at, y_at = 2 * n_mig, 2 * n_mig + 2 * 3 * Z_CORE

    def body(dst_ref, dev_ref, pos_ref, y_ref, s_ref, cnt, cnt2):
        row, colm = pos_ref[0], pos_ref[1]
        half, core = colm >> 1, colm & 1
        me = row * 4 + colm

        @pl.loop(0, 64)
        def _(i):
            y_ref[i] = 0
            s_ref[i] = -1
            cnt[i] = 0

        @pl.loop(0, 8)
        def _(i):
            cnt2[i] = 0

        @pl.loop(0, n_dev)
        def _(d):
            si, sy, sc = d >> 2, (d >> 1) & 1, d & 1

            @pl.loop(0, n_mig)
            def _(e):
                dd = dev_ref[d * n_mig + e]
                di, dy = dd >> 2, (dd >> 1) & 1
                c1 = (d >> 1) * 4 + di
                k = cnt[c1]
                cnt[c1] = k + 1
                cross = (dy != sy).astype(jnp.int32)
                c2 = di * 2 + sy
                k2 = cnt2[c2]
                cnt2[c2] = k2 + cross

                @pl.when(di == row)
                def _():
                    shift = (di - si) & 3
                    at = jnp.where(sc == core, e, n_mig + e)
                    z_slot = (shift - 1) * Z_CORE + (k >> 1)
                    here = jnp.where(shift == 0, at, z_at + z_slot + jnp.where((k & 1) == core, 0, 3 * Z_CORE))

                    @pl.when((sy == half) & (cross == 1) & ((k2 & 1) == core) & (k2 < 2 * Y_CORE))
                    def _():
                        y_ref[k2 >> 1] = jnp.minimum(here, y_at - 1)

                    @pl.when(dd == me)
                    def _():
                        by_y = y_at + (k2 >> 1) + jnp.where((k2 & 1) == core, 0, Y_CORE)
                        s_ref[dst_ref[d * n_mig + e] - me * n_slots] = jnp.where(cross == 1, by_y, here)

    smem = pl.BlockSpec(memory_space=pltpu.SMEM)
    return pl.pallas_call(
        body,
        out_shape=[jax.ShapeDtypeStruct((64,), jnp.int32)] * 2,
        in_specs=[smem] * 3,
        out_specs=[smem] * 2,
        scratch_shapes=[pltpu.SMEM((64,), jnp.int32), pltpu.SMEM((8,), jnp.int32)],
        cost_estimate=SMALL,
        name="route",
    )(dst, dev, pos)


def enter(axis, peers):
    barrier = pltpu.get_barrier_semaphore()
    for p in peers:
        pl.semaphore_signal(barrier, inc=1, device_id={axis: p}, device_id_type=MESH_ID)
    pl.semaphore_wait(barrier, len(peers))


def gather_rows(x, axis, n, cid):
    def body(x_ref, o_ref, send_sem, recv_sem):
        me = lax.axis_index(axis)
        sib, over, _ = around(me)
        enter(axis, (sib, over))

        def send(src, at, peer, i):
            return pltpu.make_async_remote_copy(
                src_ref=src, dst_ref=o_ref.at[at], send_sem=send_sem.at[i], recv_sem=recv_sem.at[i],
                device_id={axis: peer}, device_id_type=MESH_ID)

        cross, near = send(x_ref, me, over, 0), send(x_ref, me, sib, 1)
        cross.start()
        near.start()
        o_ref[me] = x_ref[...]
        cross.wait()
        hand = send(o_ref.at[over], over, sib, 2)
        hand.start()
        near.wait()
        hand.wait()

    return pl.pallas_call(
        body,
        out_shape=jax.ShapeDtypeStruct((n,) + x.shape, x.dtype),
        in_specs=[pl.BlockSpec(memory_space=pltpu.VMEM)],
        out_specs=pl.BlockSpec(memory_space=pltpu.VMEM),
        scratch_shapes=[pltpu.SemaphoreType.DMA((3,)), pltpu.SemaphoreType.DMA((3,))],
        compiler_params=pltpu.CompilerParams(collective_id=cid, has_side_effects=True),
        cost_estimate=SMALL,
        name="gather_rows",
    )(x)


def merge_scratch(b, r, hd, ml_shape):
    block, stats = pltpu.VMEM((b, r, hd), jnp.float32), pltpu.VMEM(ml_shape, jnp.float32)
    return [block, block, stats, block, stats, block, stats, pltpu.SemaphoreType.DMA((5,)), pltpu.SemaphoreType.DMA((5,))]


def merge(acc_ref, ml_ref, scratch, axis, b, emit):
    sib_me, sib_over, ml_sib, to_over, ml_to, y_acc, ml_y, send_sem, recv_sem = scratch
    r = acc_ref.shape[1]
    me = lax.axis_index(axis)
    sib, over, diag = around(me)

    def send(src, dst, peer, i):
        return pltpu.make_async_remote_copy(
            src_ref=src, dst_ref=dst, send_sem=send_sem.at[i], recv_sem=recv_sem.at[i],
            device_id={axis: peer}, device_id_type=MESH_ID)

    near = [send(acc_ref.at[pl.ds(diag * b, b)], sib_over, sib, 0), send(ml_ref, ml_sib, sib, 1),
            send(acc_ref.at[pl.ds(sib * b, b)], sib_me, sib, 2)]
    for cp in near:
        cp.start()
    near[0].wait()
    near[1].wait()
    lane = lax.broadcasted_iota(jnp.int32, (r, ml_ref.shape[2]), 1)

    def pick(t, s):
        return jnp.sum(jnp.where(lane == s, t, 0.0), axis=1, keepdims=True)

    top = jnp.maximum(ml_ref[0], ml_sib[0])
    w_own, w_sib = jnp.exp(ml_ref[0] - top), jnp.exp(ml_sib[0] - top)
    tot = w_own * ml_ref[1] + w_sib * ml_sib[1]
    ml_to[0] = top
    ml_to[1] = tot
    for i in range(b):
        s = over * b + i
        to_over[i] = pick(w_own, s) * acc_ref[s] + pick(w_sib, s) * sib_over[i]
    far = [send(to_over, y_acc, over, 3), send(ml_to, ml_y, over, 4)]
    for cp in far:
        cp.start()
    near[2].wait()
    far[1].wait()
    last = jnp.maximum(top, ml_y[0])
    f, g = jnp.exp(top - last), jnp.exp(ml_y[0] - last)
    den = f * tot + g * ml_y[1]
    f, g = f / den, g / den
    w_own, w_sib = f * w_own, f * w_sib
    for i in range(b):
        s = me * b + i
        sib_me[i] = pick(w_own, s) * acc_ref[s] + pick(w_sib, s) * sib_me[i]
    far[0].wait()
    for i in range(b):
        emit(i, sib_me[i] + pick(g, me * b + i) * y_acc[i])


def combine(acc, ml, axis, n, cid):
    rows, r, hd = acc.shape
    b = rows // n

    def body(acc_ref, ml_ref, o_ref, *scratch):
        sib, over, _ = around(lax.axis_index(axis))
        enter(axis, (sib, over))

        def emit(i, val):
            o_ref[i] = val.astype(o_ref.dtype)

        merge(acc_ref, ml_ref, scratch, axis, b, emit)

    return pl.pallas_call(
        body,
        out_shape=jax.ShapeDtypeStruct((b, r, hd), jnp.bfloat16),
        in_specs=[pl.BlockSpec(memory_space=pltpu.VMEM)] * 2,
        out_specs=pl.BlockSpec(memory_space=pltpu.VMEM),
        scratch_shapes=merge_scratch(b, r, hd, ml.shape),
        compiler_params=pltpu.CompilerParams(collective_id=cid, has_side_effects=True),
        cost_estimate=SMALL,
        name="combine",
    )(acc, ml)


def mlp_pair(attn, hidden, w_out, w_up, w_down, w_next, layer, cid):
    rows, d = hidden.shape
    fused = isinstance(attn, tuple)
    ff = w_up.shape[2]
    r = -(-rows // 32) * 32
    tile = 512
    d_half, f_half = d // 2, ff // 2
    n_o, n_f = d_half // tile, f_half // tile
    ring_c, ring_r = 8, 6
    halves = [w.shape[2] // 2 for w in w_next]
    parts = [(w, t * tile) for w, h in enumerate(halves) for t in range(h // tile)]
    n_p, p_half = len(parts), sum(halves)
    pad = lambda t: jnp.pad(t, ((0, r - rows), (0, 0)))
    hidden = pad(hidden)
    first_in = list(attn) if fused else [pad(attn)]
    merge_in = []
    if fused:
        acc_rows, qr, hd = attn[0].shape
        b = acc_rows // 4
        merge_in = [pltpu.VMEM((r, d), jnp.float32), pltpu.VMEM((r, d), jnp.bfloat16)] + merge_scratch(b, qr, hd, attn[1].shape)

    def body(*rest):
        if fused:
            (acc_ref, ml_ref), rest = rest[:2], rest[2:]
        else:
            attn_ref, rest = rest[0], rest[1:]
        hid_ref, wo_ref, wu_ref, wd_ref = rest[:4]
        rest = rest[4:]
        wn_refs, rest = rest[:len(w_next)], rest[len(w_next):]
        o_ref, rest = rest[0], rest[1:]
        if n_p:
            p_ref, p_to, p_in, rest = rest[0], rest[1], rest[2], rest[3:]
        if fused:
            x_f32, attn_ref, scratch, rest = rest[0], rest[1], rest[2:len(merge_in)], rest[len(merge_in):]
        x_all, h_all, hm, act, acc, rx, wc, wr, csem, rsem, ssem, qsem = rest
        me = lax.axis_index('kv')
        core = lax.rem(me, 2)
        peer = me + 1 - 2 * core
        mine, other = pl.ds(core * r, r), pl.ds((1 - core) * r, r)

        def col(c, is_out):
            if is_out:
                src = wo_ref.at[layer, :, pl.ds(pl.multiple_of(core * d_half + c * tile, tile), tile)]
            else:
                src = wu_ref.at[layer, :, pl.ds(pl.multiple_of(core * f_half + (c - n_o) * tile, tile), tile)]
            slot = lax.rem(c, ring_c)
            return pltpu.make_async_copy(src, wc.at[slot], csem.at[slot])

        def proj(p):
            w, lo = parts[p]
            src = wn_refs[w].at[layer + 1, :, pl.ds(pl.multiple_of(core * halves[w] + lo, tile), tile)]
            slot = (n_o + n_f + p) % ring_c
            return pltpu.make_async_copy(src, wc.at[slot], csem.at[slot])

        def row(j):
            slot = lax.rem(j, ring_r)
            src = wd_ref.at[layer, pl.ds(pl.multiple_of(core * f_half + j * tile, tile), tile), :]
            return pltpu.make_async_copy(src, wr.at[slot], rsem.at[slot])

        for c in range(ring_c):
            col(c, c < n_o).start()

        enter('kv', (peer, around(me)[1]) if fused else (peer,))
        if fused:
            x_f32[...] = jnp.zeros_like(x_f32)

            def emit(i, val):
                for t in range(2):
                    for h in range(d // hd):
                        k = t * (d // hd) + h
                        x_f32[t * b + i:t * b + i + 1, h * hd:(h + 1) * hd] = val[k:k + 1]

            merge(acc_ref, ml_ref, scratch, 'kv', b, emit)
            attn_ref[...] = x_f32[...].astype(attn_ref.dtype)

        def send(src, dst, i):
            return pltpu.make_async_remote_copy(
                src_ref=src, dst_ref=dst, send_sem=ssem.at[i], recv_sem=qsem.at[i],
                device_id={'kv': peer}, device_id_type=MESH_ID)

        swaps = [send(attn_ref, x_all.at[mine], 0), send(hid_ref, h_all.at[mine], 1)]
        for cp in swaps:
            cp.start()
        x_all[mine] = attn_ref[...]
        h_all[mine] = hid_ref[...]
        for cp in swaps:
            cp.wait()

        @pl.loop(0, n_o)
        def _(c):
            col(c, True).wait()
            at = pl.ds(pl.multiple_of(core * d_half + c * tile, tile), tile)
            part = jnp.dot(x_all[...], wc[lax.rem(c, ring_c)], preferred_element_type=jnp.float32)
            hm[:, at] = (h_all[:, at].astype(jnp.float32) + part).astype(jnp.bfloat16)

            @pl.when(c + ring_c < n_o + n_f)
            def _():
                col(c + ring_c, False).start()

        own_cols = pl.ds(pl.multiple_of(core * d_half, tile), d_half)
        cp = send(hm.at[:, own_cols], hm.at[:, own_cols], 2)
        cp.start()
        acc[...] = jnp.zeros_like(acc)
        cp.wait()

        @pl.loop(0, n_f)
        def _(j):
            c = j + n_o
            col(c, False).wait()
            up = jnp.dot(hm[...], wc[lax.rem(c, ring_c)], preferred_element_type=jnp.float32)
            act[:, pl.ds(pl.multiple_of(j * tile, tile), tile)] = jax.nn.gelu(up).astype(jnp.bfloat16)

            @pl.when(c + ring_c < n_o + n_f)
            def _():
                col(c + ring_c, False).start()

            for p in range(n_p):
                @pl.when(c + ring_c == n_o + n_f + p)
                def _():
                    proj(p).start()

            @pl.when(j < ring_r)
            def _():
                row(j).start()

        @pl.loop(0, n_f)
        def _(j):
            row(j).wait()
            acc[...] += jnp.dot(act[:, pl.ds(pl.multiple_of(j * tile, tile), tile)], wr[lax.rem(j, ring_r)],
                                preferred_element_type=jnp.float32)

            @pl.when(j + ring_r < n_f)
            def _():
                row(j + ring_r).start()

        cp = send(acc.at[other], rx, 3)
        cp.start()
        cp.wait()
        o_ref[...] = (hm[mine].astype(jnp.float32) + (acc[mine] + rx[...])).astype(o_ref.dtype)
        if not n_p:
            return
        cp = send(o_ref, x_all.at[mine], 4)
        cp.start()
        x_all[mine] = o_ref[...]
        cp.wait()
        at = 0
        for p in range(n_p):
            w, lo = parts[p]
            proj(p).wait()
            res = jnp.dot(x_all[...], wc[(n_o + n_f + p) % ring_c], preferred_element_type=jnp.float32).astype(jnp.bfloat16)
            first = 2 * sum(halves[:w])
            acc_at = pl.ds(pl.multiple_of(first + core * halves[w] + lo, tile), tile)

            @pl.when(core == 0)
            def _():
                p_ref[:, acc_at] = res[:r]
                p_to[:, at:at + tile] = res[r:]

            @pl.when(core == 1)
            def _():
                p_ref[:, acc_at] = res[r:]
                p_to[:, at:at + tile] = res[:r]

            at += tile
        cp = send(p_to, p_in, 5)
        cp.start()
        cp.wait()
        at = 0
        for w, lo in parts:
            first = 2 * sum(halves[:w])
            p_ref[:, pl.ds(pl.multiple_of(first + (1 - core) * halves[w] + lo, tile), tile)] = p_in[:, at:at + tile]
            at += tile

    vmem, any_spec = pl.BlockSpec(memory_space=pltpu.VMEM), pl.BlockSpec(memory_space=pl.ANY)
    out_shape = [jax.ShapeDtypeStruct((r, d), jnp.bfloat16)]
    extra = []
    if n_p:
        out_shape.append(jax.ShapeDtypeStruct((r, 2 * p_half), jnp.bfloat16))
        extra = [pltpu.VMEM((r, p_half), jnp.bfloat16)] * 2
    out = pl.pallas_call(
        body,
        out_shape=out_shape,
        in_specs=[vmem] * (len(first_in) + 1) + [any_spec] * (3 + len(w_next)),
        out_specs=[vmem] * len(out_shape),
        scratch_shapes=extra + merge_in + [
            pltpu.VMEM((2 * r, d), jnp.bfloat16), pltpu.VMEM((2 * r, d), jnp.bfloat16), pltpu.VMEM((2 * r, d), jnp.bfloat16),
            pltpu.VMEM((2 * r, f_half), jnp.bfloat16), pltpu.VMEM((2 * r, d), jnp.float32), pltpu.VMEM((r, d), jnp.float32),
            pltpu.VMEM((ring_c, d, tile), jnp.bfloat16), pltpu.VMEM((ring_r, tile, d), jnp.bfloat16),
            pltpu.SemaphoreType.DMA((ring_c,)), pltpu.SemaphoreType.DMA((ring_r,)),
            pltpu.SemaphoreType.DMA((6,)), pltpu.SemaphoreType.DMA((6,)),
        ],
        compiler_params=pltpu.CompilerParams(collective_id=cid, has_side_effects=True, vmem_limit_bytes=58 * 1024 * 1024),
        cost_estimate=cost(6_000_000_000, 60_000_000),
    )(*first_in, hidden, w_out, w_up, w_down, *w_next)
    return [t[:rows] for t in out]


def attend(info, counts, qkv, pools_in, unit_srcs, first_unit, prev_pools, state, layer, part, n_slots, layers, page, kvh, q_group, hd):
    sources = list(pools_in) + list(unit_srcs)
    n_pool = len(pools_in)
    prow = page * kvh
    qr = 2 * kvh * q_group
    n_seq = qkv.shape[0]
    scale = hd ** -0.5
    aliased = prev_pools is not None
    carried = state is not None

    def body(info_ref, cnt_ref, qkv_ref, *rest):
        ins, rest = rest[:len(sources)], rest[len(sources):]
        if aliased:
            rest = rest[2:]
        if carried:
            acc_prev, ml_prev = rest[:2]
            rest = rest[2:]
        k_out, v_out, acc_ref, ml_ref, kbuf, vbuf, isem, osem = rest
        lo = cnt_ref[2 * part - 1] if part else 0
        mid = cnt_ref[2 * part]
        hi = cnt_ref[2 * part + 1]

        def load_from(k_page, v_page, i):
            return (pltpu.make_async_copy(k_page, kbuf.at[i], isem.at[0, i]),
                    pltpu.make_async_copy(v_page, vbuf.at[i], isem.at[1, i]))

        def from_pool(i):
            at = info_ref[0, i] * layers + layer
            return load_from(ins[0].at[at], ins[1].at[at], i)

        def loads(i):
            if n_pool:
                return from_pool(i)
            return load_from(ins[0].at[0, pl.ds(0, prow)], ins[0].at[0, pl.ds(prow, prow)], i)

        def start_loads(i):
            at, first = info_ref[3, i], first_unit
            if n_pool and unit_srcs:
                pl.when(at < 0)(lambda: [cp.start() for cp in from_pool(i)] and None)
            elif n_pool:
                for cp in from_pool(i):
                    cp.start()
            for ref in ins[n_pool:]:
                last = first + ref.shape[0]

                @pl.when((at >= first) & (at < last))
                def _():
                    u = at - first
                    for cp in load_from(ref.at[u, pl.ds(0, prow)], ref.at[u, pl.ds(prow, prow)], i):
                        cp.start()

                first = last

        def stores(i):
            slot = info_ref[0, i]
            return (pltpu.make_async_copy(kbuf.at[i], k_out.at[slot * layers + layer], osem.at[0, i]),
                    pltpu.make_async_copy(vbuf.at[i], v_out.at[slot * layers + layer], osem.at[1, i]))

        @pl.loop(lo, hi)
        def _(i):
            start_loads(i)

        if carried:
            acc_ref[...] = acc_prev[...]
            ml_ref[...] = ml_prev[...]
        else:
            acc_ref[...] = jnp.zeros_like(acc_ref)
            ml_ref[0] = jnp.full(ml_ref.shape[1:], NEG, jnp.float32)
            ml_ref[1] = jnp.zeros(ml_ref.shape[1:], jnp.float32)

        col = lax.broadcasted_iota(jnp.int32, (qr, prow), 1)
        row = lax.broadcasted_iota(jnp.int32, (qr, prow), 0)
        late = (row >= kvh * q_group).astype(jnp.int32)
        head_ok = lax.rem(col, kvh) == (row - late * (kvh * q_group)) // q_group
        need = col // kvh - late
        need = jnp.where(head_ok, need, 1 << 20)
        lane = lax.broadcasted_iota(jnp.int32, ml_ref.shape[1:], 1)
        wrow = lax.broadcasted_iota(jnp.int32, (4 * kvh, hd), 0) // kvh

        @pl.loop(0, (mid - lo + UNROLL - 1) // UNROLL)
        def _(g):
            base = lo + g * UNROLL
            idx, seqs, offs = [], [], []
            for u in range(UNROLL):
                i = base + u
                live = i < mid
                j = jnp.minimum(i, mid - 1)
                idx.append(j)
                seqs.append(jnp.where(live, info_ref[1, j], n_seq))
                offs.append(info_ref[2, j])

                @pl.when(live)
                def _():
                    for cp in loads(j):
                        cp.wait()

            for j, seq, off in zip(idx, seqs, offs):
                w = jnp.minimum(off // 2, page // 2 - 2)
                at = pl.ds(pl.multiple_of(w * (2 * kvh), 2 * kvh), 4 * kvh)
                tok = wrow + 2 * w
                seq = jnp.minimum(info_ref[1, j], n_seq - 1)
                for buf, r0 in ((kbuf, qr), (vbuf, qr + 2 * kvh)):
                    new = qkv_ref[seq, r0:r0 + 2 * kvh, :].astype(jnp.float32)
                    first = jnp.concatenate([new[:kvh]] * 4, axis=0)
                    second = jnp.concatenate([new[kvh:]] * 4, axis=0)
                    old = buf[j, at, :].astype(jnp.float32)
                    old = jnp.where(tok == off, first, jnp.where(tok == off + 1, second, old))
                    buf[j, at, :] = old.astype(jnp.bfloat16)

            res = []
            for u in range(UNROLL):
                q = qkv_ref[jnp.minimum(seqs[u], n_seq - 1), :qr, :]
                s = lax.dot_general(q, kbuf[idx[u]], (((1,), (1,)), ((), ())), preferred_element_type=jnp.float32) * scale
                s = jnp.where(need <= offs[u], s, NEG)
                m = jnp.max(s, axis=1, keepdims=True)
                p = jnp.exp(s - m)
                l = jnp.sum(p, axis=1, keepdims=True)
                o = jnp.dot(p.astype(jnp.bfloat16), vbuf[idx[u]], preferred_element_type=jnp.float32)
                res.append((m, l, o))
            for u in range(UNROLL):
                m, l, o = res[u]
                sel = lane == seqs[u]
                m_all, l_all = ml_ref[0], ml_ref[1]
                m_old = jnp.max(jnp.where(sel, m_all, NEG), axis=1, keepdims=True)
                m_new = jnp.maximum(m_old, m)
                alpha = jnp.exp(m_old - m_new)
                beta = jnp.exp(m - m_new)
                acc_ref[seqs[u]] = acc_ref[seqs[u]] * alpha + o * beta
                ml_ref[0] = jnp.where(sel, m_new, m_all)
                ml_ref[1] = jnp.where(sel, l_all * alpha + l * beta, l_all)
            for u in range(UNROLL):
                @pl.when(base + u < mid)
                def _():
                    for cp in stores(base + u):
                        cp.start()

        @pl.loop(mid, hi)
        def _(i):
            for cp in loads(i):
                cp.wait()
            for cp in stores(i):
                cp.start()

        @pl.loop(lo, hi)
        def _(i):
            for cp in stores(i):
                cp.wait()

    any_spec = pl.BlockSpec(memory_space=pl.ANY)
    vmem = pl.BlockSpec(memory_space=pltpu.VMEM)
    smem = pl.BlockSpec(memory_space=pltpu.SMEM)
    operands = [info, counts, qkv, *sources]
    specs = [smem, smem, vmem] + [any_spec] * len(sources)
    alias = {}
    if aliased:
        alias = {len(operands): 0, len(operands) + 1: 1}
        operands += list(prev_pools)
        specs += [any_spec, any_spec]
    if carried:
        operands += list(state)
        specs += [vmem, vmem]
    pool = jax.ShapeDtypeStruct((n_slots * layers, prow, hd), jnp.bfloat16)
    return pl.pallas_call(
        body,
        out_shape=[pool, pool,
                   jax.ShapeDtypeStruct((n_seq + 1, qr, hd), jnp.float32),
                   jax.ShapeDtypeStruct((2, qr, 128), jnp.float32)],
        in_specs=specs,
        out_specs=[any_spec, any_spec, vmem, vmem],
        scratch_shapes=[
            pltpu.VMEM((n_slots, prow, hd), jnp.bfloat16),
            pltpu.VMEM((n_slots, prow, hd), jnp.bfloat16),
            pltpu.SemaphoreType.DMA((2, n_slots)),
            pltpu.SemaphoreType.DMA((2, n_slots)),
        ],
        input_output_aliases=alias,
        cost_estimate=cost(400_000_000, 16_000_000),
    )(*operands)


def solution(mesh):
    n_rows = mesh.shape['kv2']
    n_cols = mesh.shape['kv']
    dev_axes = ('rep', 'kv2', 'kv')
    seq_spec = P(None, dev_axes, None)
    pool_spec = P(dev_axes, None, None, None, None)
    table_spec = P(dev_axes, None)
    vec_spec = P(dev_axes)
    full_spec = P()

    def per_device(x_embed, w_query, w_key, w_value, w_out, w_up, w_down, k_pool, v_pool, old_table, seq_len, src_slot, dst_slot):
        n_slots, layers, page, kv_heads, head_dim = k_pool.shape
        heads = w_query.shape[2] // head_dim
        q_group = heads // kv_heads
        seq_dev = x_embed.shape[1]
        n_pages = old_table.shape[1]
        n_mig = src_slot.shape[0]
        n_dev = n_rows * n_cols
        row_seqs = seq_dev * n_cols
        prow = page * kv_heads
        width = x_embed.shape[2]
        me_row, me_col = lax.axis_index('kv2'), lax.axis_index('kv')
        me = me_row * n_cols + me_col
        base = me * n_slots

        k_rows = k_pool.reshape(n_slots * layers, prow, head_dim)
        v_rows = v_pool.reshape(n_slots * layers, prow, head_dim)
        pair = [(c, c ^ 1) for c in range(n_cols)]
        over = [(c, c ^ 2) for c in range(n_cols)]
        z_hops = [[(r, (r + s) % n_rows) for r in range(n_rows)] for s in range(1, n_rows)]
        pos = jnp.stack([me_row, me_col]).astype(jnp.int32)
        dev_own = dst_slot // n_slots
        leaving = take_pages((src_slot - base) * layers, k_rows, v_rows, layers)
        units = [[leaving[0], lax.ppermute(leaving[0], 'kv', pair)]]
        dev_pair = lax.ppermute(dev_own, 'kv', pair)

        n_rep = mesh.shape['rep']
        words = [src_slot, dst_slot, dst_slot // n_slots, old_table.reshape(-1), seq_len]
        cuts = [0]
        for w in words:
            cuts.append(cuts[-1] + w.shape[0])
        meta = jnp.pad(jnp.concatenate(words), (0, 128 - cuts[-1])).reshape(1, 128)
        meta_all = share_plan(meta, (n_rep, n_rows, n_cols), 2).reshape(n_rep, n_dev, 128)

        meta_all, pos = lax.optimization_barrier((meta_all, pos))
        z_list = route_z(dev_own, dev_pair, pos)
        hops = pick(z_list, units[0], [Z_CORE] * (n_rows - 1))
        hops, z_list, hidden, meta_all, later = lax.optimization_barrier(
            (hops, z_list, x_embed.reshape(2 * seq_dev, width), meta_all, leaving[1:]))
        units += [[own, lax.ppermute(own, 'kv', pair)] for own in later]

        meta = lax.dynamic_index_in_dim(meta_all, lax.axis_index('rep'), 0, keepdims=False)
        src_all, dst_all, dev_all = (meta[:, cuts[t]:cuts[t + 1]].reshape(-1) for t in range(3))
        row_meta = lax.dynamic_slice_in_dim(meta, me_row * n_cols, n_cols, axis=0)
        row_table = row_meta[:, cuts[3]:cuts[4]].reshape(-1)
        row_len = row_meta[:, cuts[4]:cuts[5]].reshape(-1)

        dev_by = meta_all[:, :, cuts[2]:cuts[3]]
        to_row = dev_by // n_cols
        rows4 = jnp.arange(n_rows, dtype=jnp.int32)
        goes = (to_row[..., None] == rows4).astype(jnp.int32).sum(axis=2)
        per_chip = goes.reshape(n_rep, n_rows, n_cols // 2, 2, n_rows).sum(axis=3)
        leaves = rows4[:, None] != rows4[None, :]
        z_full = ((per_chip > 2 * Z_CORE) & leaves[None, :, None, :]).any()
        side = (jnp.arange(n_dev, dtype=jnp.int32) // 2 % 2)[None, :, None]
        crosses = dev_by // 2 % 2 != side
        per_side = ((to_row[..., None] == rows4) & crosses[..., None]).astype(jnp.int32).sum(axis=2)
        y_full = (per_side.reshape(n_rep, n_rows, n_cols // 2, 2, n_rows).sum(axis=(1, 3)) > 2 * Y_CORE).any()
        full = z_full | y_full

        y_list, unit_of = route(dst_all, dev_all, pos, n_mig, n_slots)

        def along_z(hops):
            got = []
            for h, z in zip(hops, z_hops):
                got.append(lax.ppermute(h, 'kv2', z))
            return got

        def swap(units, got):
            return units + got + [lax.ppermute(g, 'kv', pair) for g in got]

        def along_y(hop):
            got = lax.ppermute(hop, 'kv', over)
            return [got, lax.ppermute(got, 'kv', pair)]

        same = row_table[:, None] == src_all[None, :]
        new_table = jnp.where(same.any(axis=1), jnp.sum(jnp.where(same, dst_all[None, :], 0), axis=1), row_table)
        slots = jnp.arange(n_slots, dtype=jnp.int32)
        cells = jnp.arange(row_seqs * n_pages, dtype=jnp.int32)
        slot_cell = jnp.max(jnp.where(new_table[None, :] == (slots + base)[:, None], cells[None, :], -1), axis=1)
        moves = jnp.arange(n_dev * n_mig, dtype=jnp.int32)
        move_of = jnp.max(jnp.where(dst_all[None, :] == (slots + base)[:, None], moves[None, :], -1), axis=1)
        is_mig = move_of >= 0
        used = slot_cell >= 0
        seq_of = jnp.where(used, slot_cell // n_pages, row_seqs)
        seq_one = seq_of[:, None] == jnp.arange(row_seqs, dtype=jnp.int32)[None, :]
        len_of = jnp.sum(jnp.where(seq_one, row_len[None, :], 0), axis=1)
        off_of = len_of - (slot_cell % n_pages) * page
        off_of = jnp.where(used & (off_of >= 0) & (off_of < page), off_of, 2 * page)
        y_at = 2 * n_mig + 2 * (n_rows - 1) * Z_CORE
        unit = jnp.where(is_mig, jnp.where(full, slots + y_at + 2 * Y_CORE, unit_of[:n_slots]), -1)

        def lists(cls, n_cls):
            key = cls * 2 + (~used).astype(jnp.int32)
            order = key * n_slots + slots
            at = jnp.sum((order[None, :] < order[:, None]).astype(jnp.int32), axis=1)
            place = at[None, :] == jnp.arange(64, dtype=jnp.int32)[:, None]
            info = jnp.stack([jnp.sum(jnp.where(place, t[None, :], 0), axis=1) for t in (slots, seq_of, off_of, unit)])
            counts = jnp.sum((key[None, :] <= jnp.arange(2 * n_cls, dtype=jnp.int32)[:, None]).astype(jnp.int32), axis=1)
            return info, counts

        by_class = lists(is_mig.astype(jnp.int32) + (unit >= y_at).astype(jnp.int32), 3)
        by_use = lists(jnp.zeros_like(slots), 1)

        def all_pages(layer):
            def collect():
                every = lax.all_gather(leaving[layer], ('kv2', 'kv'), tiled=True)
                return pick(jnp.maximum(move_of, 0), [every], [n_slots])[0]

            return lax.cond(full, collect, lambda: uninit((n_slots, 2 * prow, head_dim), jnp.bfloat16))

        pools = None
        got = along_z(hops)
        for layer in range(layers):
            dot = lambda a, w: jnp.dot(a, w[layer], preferred_element_type=jnp.float32)
            if layer == 0:
                parts = [dot(hidden, w).astype(jnp.bfloat16) for w in (w_query, w_key, w_value)]
            else:
                parts = jnp.split(ahead, [heads * head_dim, (heads + kv_heads) * head_dim], axis=1)
            query, k_new, v_new = (t.reshape(2, seq_dev, -1, head_dim) for t in parts)
            per_seq = lambda t: jnp.swapaxes(t, 0, 1).reshape(seq_dev, -1, head_dim)
            qkv = jnp.concatenate([per_seq(query), per_seq(k_new), per_seq(v_new)], axis=1)
            qkv = gather_rows(qkv, 'kv', n_cols, 0).reshape(row_seqs, -1, head_dim)
            dims = dict(layer=layer, n_slots=n_slots, layers=layers, page=page, kvh=kv_heads, q_group=q_group, hd=head_dim)
            if layer == 0:
                *pools, acc, ml = attend(*by_class, qkv, [k_rows, v_rows], [], 0, pools, None, part=0, **dims)
                next_hops = pick(z_list, units[1], [Z_CORE] * (n_rows - 1))
                got, acc, next_hops, by_use = lax.optimization_barrier((got, acc, next_hops, by_use))
                next_got = along_z(next_hops)
                all_units = swap(units[0], got)
                hop, = pick(y_list, all_units, [Y_CORE])
                last = along_y(hop) + [all_pages(0)]
                *pools, acc, ml = attend(*by_class, qkv, [], all_units, 0, pools, (acc, ml), part=1, **dims)
                *pools, acc, ml = attend(*by_class, qkv, [], last, y_at, pools, (acc, ml), part=2, **dims)
            else:
                srcs = all_units + along_y(hop) + [all_pages(layer)]
                *pools, acc, ml = attend(*by_use, qkv, [k_rows, v_rows], srcs, 0, pools, None, part=0, **dims)
            if layer + 1 < layers:
                o = combine(acc, ml, 'kv', n_cols, 1)
                next_got, o = lax.optimization_barrier((next_got, o))
                all_units = swap(units[layer + 1], next_got)
                hop, = pick(y_list, all_units, [Y_CORE])
                hop, o = lax.optimization_barrier((hop, o))
                attn_out = jnp.swapaxes(o.reshape(seq_dev, 2, heads * head_dim), 0, 1).reshape(2 * seq_dev, heads * head_dim)
            else:
                attn_out = (acc, ml)
            w_next = (w_query, w_key, w_value) if layer + 1 < layers else ()
            hidden, *ahead = mlp_pair(attn_out, hidden, w_out, w_up, w_down, w_next, layer, 3 + layer)
            ahead = ahead[0] if ahead else None
        k_out, v_out = (p.reshape(k_pool.shape) for p in pools)
        return hidden.reshape(2, seq_dev, width), k_out, v_out

    return jax.shard_map(per_device, mesh=mesh, in_specs=(seq_spec, full_spec, full_spec, full_spec, full_spec, full_spec, full_spec, pool_spec, pool_spec, table_spec, vec_spec, vec_spec, vec_spec), out_specs=(seq_spec, pool_spec, pool_spec), check_vma=False)
```
